32 devices in a mesh: groups: 2 (over x), mp: 16 (over z, y, core).
Axes of the slice: x: 2, y: 2, z: 4, core: 2. Of those that a mesh axis runs over, the one named last changes fastest.
Arguments:
- hidden: bfloat16 [1024, 4096], P(('groups', 'mp')), parts along dimension 0, may hold values from -6 to 6
- norm_gain_attn: float32 [4096], replicated, may hold values from 0.5 to 1.5
- w_query: bfloat16 [4096, 1024], P(None, 'mp'), may hold values from -0.09375 to 0.09375
- entering_kv: bfloat16 [16, 2048, 2048], P('groups', 'mp'), parts along dimension 0, may hold values from -60 to 60
- cached_kv: bfloat16 [16, 2048, 2048], P('groups', None, 'mp'), parts along dimension 0, may hold values from -60 to 60
- enc_lengths: int32 [2, 16], P(None, 'groups'), parts along dimension 1, may hold values from 128 to 2048
- w_out: bfloat16 [1024, 4096], P('mp'), may hold values from -0.1875 to 0.1875
- norm_gain_ffn: float32 [4096], replicated, may hold values from 0.5 to 1.5
- w_gate: bfloat16 [4096, 10240], P(None, 'mp'), may hold values from -0.09375 to 0.09375
- w_up: bfloat16 [4096, 10240], P(None, 'mp'), may hold values from -0.09375 to 0.09375
- w_down: bfloat16 [10240, 4096], P('mp'), may hold values from -0.0625 to 0.0625
Outputs:
- output: bfloat16 [1024, 4096], P(('groups', 'mp')), parts along dimension 0
The draws below stay inside these ranges and needn't reach their ends.
There are 2 independent parts, one for each index of `groups`. The reference program is written for one: setup_inputs(seed, part) draws one part's arguments, and reference() takes and returns one part's arrays. A program takes and returns all parts, laid end to end along the dimension named above; an argument that names none is the same for every part. Nothing has to cross between parts.
All inputs are finite; a program needn't handle non-finite values.
Results may differ from the reference program's by a relative error of at most 0.0095.
The reference program's roundings to bfloat16 on the way (of `normed_in`, `query`, `weights`, `context`, `residual`, `normed_ffn` and `activated`) count: a program that leaves them out, or rounds other values in their place, can miss the bound.
Values may be sent and summed in bfloat16 or wider, within the bound.
A program may use at most 128 MiB of HBM per device.

```python
import jax
import jax.numpy as jnp
from jax import lax

D = 4096
DH = 64
FF = 10240
H = 16
S = 2048
QLEN = 32
REQ = 8
TOK = 512


def kv_block(seed_key):
    width = 2 * H * DH
    base = jnp.clip(jax.random.normal(seed_key, (REQ, S, width), jnp.float32), -4.5, 4.5)
    return base.astype(jnp.bfloat16)


def draw_entering_kv(key, part):
    return kv_block(jax.random.fold_in(key, 11))


def draw_cached_kv(key, part):
    return kv_block(jax.random.fold_in(key, 23))


def place_ends(result, stream_key, smallest, top_value):
    longest = result.shape.index(max(result.shape))
    spots = []
    for shift in (0, 1):
        where = [jax.random.randint(jax.random.fold_in(stream_key, axis), (), 0, length) for axis, length in enumerate(result.shape)]
        where[longest] = (where[longest] + shift) % result.shape[longest]
        spots.append(tuple(where))
    return result.at[spots[0]].set(smallest).at[spots[1]].set(top_value)


def steps_of(own_key, extent, split, least, high):
    def one(dim, blocks):
        heights = jax.random.uniform(jax.random.fold_in(jax.random.fold_in(own_key, 6), dim), (blocks,), jnp.float32, least / len(split), high / len(split))
        return jnp.repeat(jnp.exp(heights), extent[dim] // blocks).reshape((-1,) + (1,) * (len(extent) - dim - 1))

    factor_of = one(*split[0])
    for cut in split[1:]:
        factor_of = factor_of * one(*cut)
    return factor_of


def gaussian(own_key, extent, scale, limit, pieces=(), kind=jnp.bfloat16):
    entries = jax.random.normal(own_key, extent, jnp.float32) * scale
    if len(pieces) > 0:
        entries = steps_of(own_key, extent, pieces, -0.22, 0.18) * entries
    return jnp.clip(entries, min=-limit, max=limit).astype(kind)


def setup_inputs(seed: int = 0, part: int = 0) -> dict:
    key_of = jax.random.split(jax.random.key(seed), 12)
    part_keys = jax.random.split(jax.random.fold_in(key_of[11], part), 12)
    hidden = gaussian(part_keys[0], (TOK, D), 1.0, 6.0, ((0, 16),))
    norm_gain_attn = jnp.clip(1.0 + 0.1 * jax.random.normal(key_of[1], (D,), jnp.float32), 0.5, 1.5)
    w_query = gaussian(key_of[2], (D, H * DH), D ** -0.5, 0.09375, ((1, 16),))
    entering_kv = draw_entering_kv(jax.random.fold_in(jax.random.fold_in(key_of[11], part), 71), part)
    cached_kv = draw_cached_kv(jax.random.fold_in(jax.random.fold_in(key_of[11], part), 71), part)
    enc_lengths = place_ends(jax.random.randint(part_keys[5], (2, REQ), S // 16, S + 1), jax.random.fold_in(part_keys[5], 1), S // 16, S).astype(jnp.int32)
    w_out = gaussian(key_of[6], (H * DH, D), (H * DH) ** -0.5, 0.1875, ((0, 16),))
    norm_gain_ffn = jnp.clip(1.0 + 0.1 * jax.random.normal(key_of[7], (D,), jnp.float32), 0.5, 1.5)
    w_gate = gaussian(key_of[8], (D, FF), D ** -0.5, 0.09375, ((1, 16),))
    w_up = gaussian(key_of[9], (D, FF), D ** -0.5, 0.09375, ((1, 16),))
    w_down = gaussian(key_of[10], (FF, D), FF ** -0.5, 0.0625, ((0, 16),))
    return {"hidden": hidden, "norm_gain_attn": norm_gain_attn, "w_query": w_query, "entering_kv": entering_kv, "cached_kv": cached_kv, "enc_lengths": enc_lengths, "w_out": w_out, "norm_gain_ffn": norm_gain_ffn, "w_gate": w_gate, "w_up": w_up, "w_down": w_down}


epsilon = 0.1

def normalize(matrix, gain_row):
    values = matrix.astype(jnp.float32)
    mean_square = lax.optimization_barrier(jnp.mean(values * values, axis=-1, keepdims=True))
    return (values * lax.rsqrt(mean_square + epsilon) * gain_row).astype(jnp.bfloat16)

def attend(query, key_value, lengths):
    requests = lengths.shape[0]
    head_count = key_value.shape[2] // (2 * DH)
    query_heads = query.reshape(requests, QLEN, head_count, DH).astype(jnp.float32)
    paired = key_value.reshape(requests, S, head_count, 2, DH).astype(jnp.float32)
    key_part = paired[:, :, :, 0, :]
    value_part = paired[:, :, :, 1, :]
    scores = jnp.einsum('rqhd,rshd->rhqs', query_heads, key_part)
    usable = (jnp.arange(S, dtype=jnp.int32)[None, :] < lengths[:, None].astype(jnp.int32))[:, None, None, :]
    masked = jnp.where(usable, scores, -1e+30)
    largest = lax.optimization_barrier(jnp.max(masked, axis=-1, keepdims=True))
    exponent = jnp.where(usable, jnp.exp(masked - largest), 0.0)
    weights = (exponent / lax.optimization_barrier(jnp.sum(exponent, axis=-1, keepdims=True))).astype(jnp.bfloat16)
    context = jnp.einsum('rhqs,rshd->rqhd', weights.astype(jnp.float32), value_part)
    return context.astype(jnp.bfloat16).reshape(requests * QLEN, head_count * DH)

def reference(hidden, norm_gain_attn, w_query, entering_kv, cached_kv, enc_lengths, w_out, norm_gain_ffn, w_gate, w_up, w_down):
    normed_in = normalize(hidden, norm_gain_attn)
    query = jnp.dot(normed_in, w_query, preferred_element_type=jnp.float32).astype(jnp.bfloat16)
    split_row = REQ * QLEN
    context = jnp.concatenate([attend(query[:split_row], entering_kv, enc_lengths[0]), attend(query[split_row:], cached_kv, enc_lengths[1])], axis=0)
    attention = jnp.dot(context, w_out, preferred_element_type=jnp.float32)
    residual = (hidden.astype(jnp.float32) + attention).astype(jnp.bfloat16)
    normed_ffn = normalize(residual, norm_gain_ffn)
    gate = jnp.dot(normed_ffn, w_gate, preferred_element_type=jnp.float32)
    upward = jnp.dot(normed_ffn, w_up, preferred_element_type=jnp.float32)
    activated = (jax.nn.gelu(gate, approximate=True) * upward).astype(jnp.bfloat16)
    return (residual.astype(jnp.float32) + jnp.dot(activated, w_down, preferred_element_type=jnp.float32)).astype(jnp.bfloat16)
```

```python
import functools

import jax
import jax.numpy as jnp
from jax import lax
from jax.experimental import pallas as pl
from jax.experimental.pallas import tpu as pltpu
from jax.sharding import PartitionSpec as P

DH = 64
QLEN = 32
PAD = 2 * DH
MESH = pl.DeviceIdType.MESH
VM = pltpu.VMEM
DMA = pltpu.SemaphoreType.DMA

epsilon = 0.1


def normalize(matrix, gain_row):
    values = matrix.astype(jnp.float32)
    mean_square = jnp.mean(values * values, axis=-1, keepdims=True)
    return (values * lax.rsqrt(mean_square + epsilon) * gain_row).astype(jnp.bfloat16)


def place(n):
    me = lax.axis_index("mp")
    return me, me // 4, (me // 2) % 2, me % 2


def index_of(a, b, c):
    return (a * 2 + b) * 2 + c


def remote(src, dst, send, recv, to):
    return pltpu.make_async_remote_copy(
        src_ref=src, dst_ref=dst, send_sem=send, recv_sem=recv, device_id={"mp": to}, device_id_type=MESH
    )


def greet(to):
    pl.semaphore_signal(pltpu.get_barrier_semaphore(), inc=1, device_id={"mp": to}, device_id_type=MESH)


def gather_kernel(n, x_ref, out_ref, zs, zr, ys, yr, cs, cr):
    A = n // 4
    me, a, b, c = place(n)
    across, pair = index_of(a, 1 - b, c), index_of(a, b, 1 - c)
    right, left = me + 4, me - 4
    has = {1: a < A - 1, -1: a > 0}
    toward = {1: right, -1: left}
    for d in (1, -1):

        @pl.when(has[d])
        def _():
            greet(toward[d])

    greet(across)
    greet(pair)
    pl.semaphore_wait(
        pltpu.get_barrier_semaphore(), 2 + has[1].astype(jnp.int32) + has[-1].astype(jnp.int32)
    )

    def z_copy(src, k, s, d):
        row = 0 if d == 1 else A
        return remote(src, out_ref.at[index_of(k, b, c)], zs.at[row + s], zr.at[k], toward[d])

    def y_copy(src, k, bb):
        return remote(src, out_ref.at[index_of(k, bb, c)], ys.at[k], yr.at[k], across)

    def c_copy(src, k, bb, cc):
        return remote(src, out_ref.at[index_of(k, bb, cc)], cs.at[bb * A + k], cr.at[bb * A + k], pair)

    for d in (1, -1):

        @pl.when(has[d])
        def _():
            z_copy(x_ref, a, 0, d).start()

    y_copy(x_ref, a, b).start()
    c_copy(x_ref, a, b, c).start()
    out_ref[me] = x_ref[...]

    def pass_on(s):
        for d in (1, -1) if s else (1,):
            k = a - s * d

            @pl.when((k >= 0) & (k < A))
            def _():
                y_copy(x_ref, k, 1 - b).wait_recv()
                c_copy(out_ref.at[index_of(k, 1 - b, c)], k, 1 - b, c).start()

    for s in range(1, A):
        for d in (1, -1):
            k = a - s * d

            @pl.when((k >= 0) & (k < A))
            def _():
                block = out_ref.at[index_of(k, b, c)]
                remote(x_ref, block, zs.at[0], zr.at[k], toward[-d]).wait_recv()

                @pl.when(has[d])
                def _():
                    z_copy(block, k, s, d).start()

                y_copy(block, k, b).start()
                c_copy(block, k, b, c).start()

        pass_on(s - 1)
    pass_on(A - 1)
    for bb in range(2):
        for k in range(A):
            c_copy(x_ref, k, bb, 1 - c).wait_recv()
    for s in range(A):
        for d in (1, -1):
            k = a - s * d

            @pl.when((k >= 0) & (k < A) & has[d])
            def _():
                z_copy(x_ref, k, s, d).wait_send()

    for k in range(A):
        y_copy(x_ref, k, b).wait_send()
        for bb in range(2):
            c_copy(x_ref, k, bb, c).wait_send()


def params(number):
    return pltpu.CompilerParams(collective_id=number, has_side_effects=True, vmem_limit_bytes=56 * 2**20)


def gather(x, n, number):
    A = n // 4
    return pl.pallas_call(
        functools.partial(gather_kernel, n),
        out_shape=jax.ShapeDtypeStruct((n,) + x.shape, x.dtype),
        in_specs=[pl.BlockSpec(memory_space=VM)],
        out_specs=pl.BlockSpec(memory_space=VM),
        scratch_shapes=[DMA((2 * A,)), DMA((A,)), DMA((A,)), DMA((A,)), DMA((2 * A,)), DMA((2 * A,))],
        compiler_params=params(number),
        name=f"gather_{number}",
    )(x)


def scatter_kernel(
    n, left_ref, w_ref, out_ref, part, cbuf, ysend, yrecv, zsend, zright, zleft, cs, cr, ys, yr, zs, zr
):
    A = n // 4
    me, a, b, c = place(n)
    across, pair = index_of(a, 1 - b, c), index_of(a, b, 1 - c)
    has = {1: a < A - 1, -1: a > 0}
    toward = {1: me + 4, -1: me - 4}
    landing = {1: zright, -1: zleft}
    rows, width = out_ref.shape
    for d in (1, -1):

        @pl.when(has[d])
        def _():
            greet(toward[d])

    greet(across)
    greet(pair)
    pl.semaphore_wait(
        pltpu.get_barrier_semaphore(), 2 + has[1].astype(jnp.int32) + has[-1].astype(jnp.int32)
    )

    def near_last(visit):
        for s in range(A - 1, -1, -1):
            for d in (1, -1) if s else (1,):
                k = a + s * d

                @pl.when((k >= 0) & (k < A))
                def _():
                    visit(s, d, k)

    def multiply(group, bb, cc):
        left = jnp.concatenate([left_ref[index_of(k, bb, cc)] for k in range(A)], axis=0)
        tile = min(width, 1024)

        def columns(t, carry):
            at = pl.ds(pl.multiple_of(t * tile, tile), tile)
            found = jnp.dot(left, w_ref[:, at], preferred_element_type=jnp.float32)
            part[group, :, :, at] = found.reshape(A, rows, tile)
            return carry

        lax.fori_loop(0, width // tile, columns, 0)

    def c_copy(group, k, bb):
        slot = bb * A + k
        return remote(part.at[group, k], cbuf.at[slot], cs.at[slot], cr.at[slot], pair)

    def y_copy(k):
        return remote(ysend.at[k], yrecv.at[k], ys.at[k], yr.at[k], across)

    def z_copy(k, d):
        row = 0 if d == 1 else A
        return remote(zsend.at[k], landing[d].at[k], zs.at[k], zr.at[row + k], toward[d])

    def z_arrival(k, d):
        row = 0 if d == 1 else A
        return remote(zsend.at[k], landing[d].at[k], zs.at[k], zr.at[row + k], toward[-d])

    multiply(0, 1 - b, 1 - c)
    near_last(lambda s, d, k: c_copy(0, k, 1 - b).start())
    multiply(1, 1 - b, c)

    def send_across(s, d, k):
        c_copy(0, k, 1 - b).wait_recv()
        ysend[k] = (part[1, k] + cbuf[(1 - b) * A + k]).astype(jnp.bfloat16)
        y_copy(k).start()

    near_last(send_across)
    multiply(2, b, 1 - c)
    near_last(lambda s, d, k: c_copy(2, k, b).start())
    multiply(3, b, c)

    def pass_on(s, d, k):
        c_copy(2, k, b).wait_recv()
        y_copy(k).wait_recv()
        part[3, k] = part[3, k] + cbuf[b * A + k] + yrecv[k].astype(jnp.float32)
        for came in (d,) if s else (1, -1):

            @pl.when(has[-came])
            def _():
                z_arrival(k, came).wait_recv()
                part[3, k] = part[3, k] + landing[came][k].astype(jnp.float32)

        if s:
            zsend[k] = part[3, k].astype(jnp.bfloat16)
            z_copy(k, d).start()
        else:
            out_ref[...] = part[3, k]

    near_last(pass_on)

    def finish(s, d, k):
        y_copy(k).wait_send()
        if s:
            z_copy(k, d).wait_send()
        c_copy(0, k, 1 - b).wait_send()
        c_copy(2, k, b).wait_send()

    near_last(finish)


def scatter(left, w, n, number):
    A = n // 4
    rows, depth = left.shape[0] // n, left.shape[1]
    block = (rows, w.shape[1])
    half = jnp.bfloat16
    return pl.pallas_call(
        functools.partial(scatter_kernel, n),
        out_shape=jax.ShapeDtypeStruct(block, jnp.float32),
        in_specs=[pl.BlockSpec(memory_space=VM)] * 2,
        out_specs=pl.BlockSpec(memory_space=VM),
        scratch_shapes=[VM((4, A) + block, jnp.float32), VM((2 * A,) + block, jnp.float32)]
        + [VM((A,) + block, half)] * 5
        + [DMA((2 * A,)), DMA((2 * A,)), DMA((A,)), DMA((A,)), DMA((A,)), DMA((2 * A,))],
        compiler_params=params(number),
        name=f"scatter_{number}",
    )(left.reshape(n, rows, depth), w)


def pieces_of(n, width):
    return max(1, min(4, 16 // (n // 4), width // 128))


def neighbours(n):
    A = n // 4
    me, a, b, c = place(n)
    has = {1: a < A - 1, -1: a > 0}
    toward = {1: me + 4, -1: me - 4}
    return has, toward


def greet_along(has, toward):
    for d in (1, -1):

        @pl.when(has[d])
        def _():
            greet(toward[d])


def await_greetings(has, others):
    pl.semaphore_wait(
        pltpu.get_barrier_semaphore(), others + has[1].astype(jnp.int32) + has[-1].astype(jnp.int32)
    )


def query_kernel(
    n, x_ref, gain_ref, wq_ref, wo_ref, q_ref, plane_ref,
    xs, w2, q_send, q_recv, local, zs, zr, cs, cr, ws, wr, ps, pr,
):
    A = n // 4
    me, a, b, c = place(n)
    across, pair = index_of(a, 1 - b, c), index_of(a, b, 1 - c)
    has, toward = neighbours(n)
    P, W = xs.shape[0], xs.shape[-1]
    rows = x_ref.shape[0]
    greet_along(has, toward)
    greet(across)
    greet(pair)
    load_w = pltpu.make_async_copy(wq_ref, w2.at[0], local.at[0])
    load_w.start()
    values = x_ref[...].astype(jnp.float32)
    scale = lax.rsqrt(jnp.mean(values * values, axis=-1, keepdims=True) + epsilon)
    for p in range(P):
        part = slice(p * W, (p + 1) * W)
        xs[p, a, c] = (values[:, part] * scale * gain_ref[:, part]).astype(jnp.bfloat16)
    await_greetings(has, 2)

    def z_copy(k, p, s, d):
        row = 0 if d == 1 else A
        return remote(xs.at[p, k, c], xs.at[p, k, c], zs.at[row + s, p], zr.at[k, p], toward[d])

    def c_copy(k, p, cc):
        return remote(xs.at[p, k, cc], xs.at[p, k, cc], cs.at[k, p], cr.at[k, p], pair)

    wq_copy = remote(wq_ref, w2.at[1], ws.at[0], wr.at[0], across)
    q_copy = remote(q_send, q_recv, ws.at[1], wr.at[1], across)
    plane_pair = remote(wo_ref, plane_ref.at[0], ps.at[0], pr.at[0], pair)
    plane_across = remote(wo_ref, plane_ref.at[1], ps.at[1], pr.at[1], across)
    plane_diagonal = remote(plane_ref.at[1], plane_ref.at[2], ps.at[2], pr.at[2], pair)
    for p in range(P):
        for d in (1, -1):

            @pl.when(has[d])
            def _():
                z_copy(a, p, 0, d).start()

    wq_copy.start()
    plane_across.start()
    for p in range(P):
        c_copy(a, p, c).start()
    plane_pair.start()
    for s in range(1, A):
        for p in range(P):
            for d in (1, -1):
                k = a - s * d

                @pl.when((k >= 0) & (k < A))
                def _():
                    remote(xs.at[p, k, c], xs.at[p, k, c], zs.at[0, p], zr.at[k, p], toward[-d]).wait_recv()

                    @pl.when(has[d])
                    def _():
                        z_copy(k, p, s, d).start()

                    c_copy(k, p, c).start()

    load_w.wait()
    wq_copy.wait_recv()
    for k in range(A):
        for p in range(P):
            c_copy(k, p, 1 - c).wait_recv()
    total = jnp.zeros((2 * A * rows, PAD), jnp.float32)
    for p in range(P):
        total = total + lax.dot_general(
            xs[p].reshape(2 * A * rows, W), w2[:, :, p * W : (p + 1) * W].reshape(PAD, W),
            (((1,), (1,)), ((), ())), preferred_element_type=jnp.float32,
        )
    q_send[...] = total.astype(jnp.bfloat16)
    low = lax.broadcasted_iota(jnp.int32, (2 * A * rows, PAD), 1) < DH
    own = jnp.where(low, total, 0.0).astype(jnp.bfloat16).reshape(2 * A, rows, PAD)
    for k in range(A):
        for cc in range(2):
            q_ref[index_of(k, b, cc)] = own[2 * k + cc]
    q_copy.start()
    plane_across.wait_recv()
    plane_diagonal.start()
    for s in range(A):
        for d in (1, -1):
            k = a - s * d

            @pl.when((k >= 0) & (k < A) & has[d])
            def _():
                for p in range(P):
                    z_copy(k, p, s, d).wait_send()

    for k in range(A):
        for p in range(P):
            c_copy(k, p, c).wait_send()
    q_copy.wait_recv()
    came = pltpu.roll(q_recv[...].astype(jnp.float32), DH, 1)
    came = jnp.where(low, came, 0.0).astype(jnp.bfloat16).reshape(2 * A, rows, PAD)
    for k in range(A):
        for cc in range(2):
            q_ref[index_of(k, 1 - b, cc)] = came[2 * k + cc]
    wq_copy.wait_send()
    q_copy.wait_send()
    plane_across.wait_send()
    plane_pair.wait()
    plane_diagonal.wait()


def make_query(hidden, gain, w_query, w_out, n, number):
    A = n // 4
    rows, width = hidden.shape
    P = pieces_of(n, width)
    W = width // P
    half = jnp.bfloat16
    return pl.pallas_call(
        functools.partial(query_kernel, n),
        out_shape=[
            jax.ShapeDtypeStruct((n, rows, PAD), half),
            jax.ShapeDtypeStruct((3,) + w_out.shape, half),
        ],
        in_specs=[pl.BlockSpec(memory_space=m) for m in (VM, VM, pl.ANY, pl.ANY)],
        out_specs=[pl.BlockSpec(memory_space=VM), pl.BlockSpec(memory_space=pl.ANY)],
        scratch_shapes=[
            VM((P, A, 2, rows, W), half),
            VM((2, DH, width), half),
            VM((2 * A * rows, PAD), half),
            VM((2 * A * rows, PAD), half),
            DMA((1,)), DMA((2 * A, P)), DMA((A, P)), DMA((A, P)), DMA((A, P)),
            DMA((2,)), DMA((2,)), DMA((3,)), DMA((3,)),
        ],
        compiler_params=params(number),
        name=f"query_{number}",
    )(hidden, gain[None, :], w_query.T, w_out)


def project_kernel(
    n, context_ref, hidden_ref, wo_ref, plane_ref, out_ref,
    w4, c_send, c_recv, part, zsend, zright, zleft, local, cs, cr, zs, zr,
):
    A = n // 4
    me, a, b, c = place(n)
    peers = (index_of(a, b, 1 - c), index_of(a, 1 - b, c), index_of(a, 1 - b, 1 - c))
    has, toward = neighbours(n)
    landing = {1: zright, -1: zleft}
    P, _, rows, W = part.shape
    depth = wo_ref.shape[0]
    greet_along(has, toward)
    for peer in peers:
        greet(peer)
    load_own = pltpu.make_async_copy(wo_ref, w4.at[0], local.at[0])
    load_plane = pltpu.make_async_copy(plane_ref, w4.at[pl.ds(1, 3)], local.at[1])
    load_own.start()
    load_plane.start()
    for i, (bb, cc) in enumerate(((b, 1 - c), (1 - b, c), (1 - b, 1 - c))):
        for k in range(A):
            c_send[i, k] = context_ref[index_of(k, bb, cc)]
    for k in range(A):
        c_recv[0, k] = context_ref[index_of(k, b, c)]
    await_greetings(has, 3)
    swaps = [remote(c_send.at[i], c_recv.at[i + 1], cs.at[i], cr.at[i], peers[i]) for i in range(3)]
    for i in (2, 1, 0):
        swaps[i].start()
    load_own.wait()
    load_plane.wait()
    for swap in swaps:
        swap.wait_recv()
    low = lax.broadcasted_iota(jnp.int32, (A * rows, PAD), 1) < DH

    def beside(i):
        first = c_recv[i].reshape(A * rows, PAD).astype(jnp.float32)
        second = c_recv[i + 1].reshape(A * rows, PAD).astype(jnp.float32)
        return jnp.where(low, pltpu.roll(first, DH, 1), second).astype(jnp.bfloat16)

    left = jnp.concatenate([beside(0), beside(2)], axis=1)

    def z_copy(k, p, d):
        return remote(zsend.at[p, k], landing[d].at[p, k], zs.at[k, p], zr.at[(0 if d == 1 else A) + k, p], toward[d])

    def z_arrival(k, p, d):
        return remote(zsend.at[p, k], landing[d].at[p, k], zs.at[k, p], zr.at[(0 if d == 1 else A) + k, p], toward[-d])

    for s in range(A - 1, -1, -1):
        for p in range(P):
            if s == A - 1:
                w = w4[:, :, p * W : (p + 1) * W].reshape(4 * depth, W)
                found = jnp.dot(left, w, preferred_element_type=jnp.float32)
                part[p] = found.reshape(A, rows, W)
            for d in (1, -1) if s else (1,):
                k = a + s * d

                @pl.when((k >= 0) & (k < A))
                def _():
                    for came in (d,) if s else (1, -1):

                        @pl.when(has[-came])
                        def _():
                            z_arrival(k, p, came).wait_recv()
                            part[p, k] = part[p, k] + landing[came][p, k].astype(jnp.float32)

                    if s:
                        zsend[p, k] = part[p, k].astype(jnp.bfloat16)
                        z_copy(k, p, d).start()
                    else:
                        at = slice(p * W, (p + 1) * W)
                        out_ref[:, at] = (hidden_ref[:, at].astype(jnp.float32) + part[p, k]).astype(jnp.bfloat16)

    for s in range(A - 1, 0, -1):
        for d in (1, -1):
            k = a + s * d

            @pl.when((k >= 0) & (k < A))
            def _():
                for p in range(P):
                    z_copy(k, p, d).wait_send()

    for swap in swaps:
        swap.wait_send()


def project(context, hidden, w_out, plane, n, number):
    A = n // 4
    rows, width = hidden.shape
    P = pieces_of(n, width)
    W = width // P
    half = jnp.bfloat16
    return pl.pallas_call(
        functools.partial(project_kernel, n),
        out_shape=jax.ShapeDtypeStruct((rows, width), half),
        in_specs=[pl.BlockSpec(memory_space=m) for m in (VM, VM, pl.ANY, pl.ANY)],
        out_specs=pl.BlockSpec(memory_space=VM),
        scratch_shapes=[
            VM((4,) + w_out.shape, half),
            VM((3, A, rows, PAD), half),
            VM((4, A, rows, PAD), half),
            VM((P, A, rows, W), jnp.float32),
        ]
        + [VM((P, A, rows, W), half)] * 3
        + [DMA((2,)), DMA((3,)), DMA((3,)), DMA((A, P)), DMA((2 * A, P))],
        compiler_params=params(number),
        name=f"project_{number}",
    )(context, hidden, w_out, plane)


def attend_kernel(
    n, own_ref, kv_ref, cached_ref, mask_ref, cached_mask_ref, out_ref,
    q_ref, q_all, kv, cached, scores, chances, o_send, o_recv, st_send, st_recv, local, qs, qr, os, orr, ss, sr,
):
    me = lax.axis_index("mp")
    requests, positions, width = kv.shape
    pairs, heads = requests // 2, width // PAD
    load_cached = pltpu.make_async_copy(cached_ref, cached, local.at[0])
    load_kv = pltpu.make_async_copy(kv_ref, kv, local.at[1])
    load_cached.start()
    load_kv.start()
    order = sorted(range(1, n), key=lambda s: -min(s, n - s))
    others = [lax.rem(me + s, n) for s in order]
    for other in others:
        greet(other)
    for step in range(pairs):
        even, odd = (
            own_ref[(2 * step + i) * QLEN : (2 * step + i + 1) * QLEN, :].astype(jnp.float32) for i in range(2)
        )
        q_ref[step * QLEN : (step + 1) * QLEN, :] = (even + pltpu.roll(odd, DH, 1)).astype(jnp.bfloat16)
    pl.semaphore_wait(pltpu.get_barrier_semaphore(), n - 1)

    def q_copy(other, spot):
        return remote(q_ref, q_all.at[spot], qs.at[other], qr.at[spot], other)

    def o_copy(other, spot, step):
        rows = pl.ds(pl.multiple_of(step * QLEN, QLEN), QLEN)
        return remote(
            o_send.at[other, rows], o_recv.at[spot, rows], os.at[step, other], orr.at[step, spot], other
        )

    def st_copy(other, spot):
        return remote(st_send.at[other], st_recv.at[spot], ss.at[other], sr.at[spot], other)

    for other in others:
        q_copy(other, me).start()
    q_all[me] = q_ref[...]
    lane = lax.broadcasted_iota(jnp.int32, (QLEN, PAD), 1)
    load_cached.wait()

    def cached_request(r, carry):
        to = pl.ds(pl.multiple_of((requests + r) * QLEN, QLEN), QLEN)
        block = cached[r]
        found = lax.dot_general(
            own_ref[to, :], block, (((1,), (1,)), ((), ())), preferred_element_type=jnp.float32
        )
        usable = cached_mask_ref[r] > 0.5
        masked = jnp.where(usable, found, -1e30)
        exponent = jnp.where(usable, jnp.exp(masked - jnp.max(masked, axis=-1, keepdims=True)), 0.0)
        weights = (exponent / jnp.sum(exponent, axis=-1, keepdims=True)).astype(jnp.bfloat16)
        out_ref[to, :] = jnp.dot(weights, block, preferred_element_type=jnp.float32).astype(jnp.bfloat16)
        return carry

    lax.fori_loop(0, requests, cached_request, 0)
    st_send[...] = jnp.zeros_like(st_send)
    load_kv.wait()
    for other in others:
        q_copy(other, other).wait_recv()

    def pair_step(step, carry):
        rows = pl.ds(pl.multiple_of(step * QLEN, QLEN), QLEN)
        low = lane < DH
        nothing = jnp.zeros((QLEN, PAD), jnp.bfloat16)
        for i in range(2):
            for g in range(heads // 2):
                two = []
                for h in (2 * g, 2 * g + 1):
                    packed = q_all[h, rows, :].astype(jnp.float32)
                    packed = packed if i == 0 else pltpu.roll(packed, DH, 1)
                    two.append(jnp.where(low, packed, 0.0).astype(jnp.bfloat16))
                spread = jnp.concatenate(
                    [
                        jnp.concatenate([two[0], nothing], axis=1),
                        jnp.concatenate([nothing, two[1]], axis=1),
                    ],
                    axis=0,
                )
                scores[i, g] = lax.dot_general(
                    spread, kv[step * 2 + i, :, g * 2 * PAD : (g + 1) * 2 * PAD], (((1,), (1,)), ((), ())),
                    preferred_element_type=jnp.float32,
                )
        for i in range(2):
            r = step * 2 + i
            usable = mask_ref[r] > 0.5
            masked = jnp.where(usable, scores[i], -1e30)
            largest = jnp.max(masked, axis=-1, keepdims=True)
            exponent = jnp.where(usable, jnp.exp(masked - largest), 0.0)
            total = jnp.sum(exponent, axis=-1, keepdims=True)
            chances[i] = exponent.astype(jnp.bfloat16)
            st_send[...] = jnp.where(
                lane == r,
                largest.reshape(heads, QLEN, 1),
                jnp.where(lane == r + DH, total.reshape(heads, QLEN, 1), st_send[...]),
            )
        for g in range(heads // 2):
            found = [
                jnp.dot(
                    chances[i, g], kv[step * 2 + i, :, g * 2 * PAD : (g + 1) * 2 * PAD],
                    preferred_element_type=jnp.float32,
                )
                for i in range(2)
            ]
            for e in range(2):
                even, odd = (f[e * QLEN : (e + 1) * QLEN, e * PAD : (e + 1) * PAD] for f in found)
                o_send[2 * g + e, rows, :] = jnp.where(low, pltpu.roll(odd, DH, 1), even).astype(jnp.bfloat16)
        for other in others:
            o_copy(other, me, step).start()
        return carry

    lax.fori_loop(0, pairs, pair_step, 0)
    for other in others:
        st_copy(other, me).start()
    o_recv[me] = o_send[me]
    st_recv[me] = st_send[me]
    for other in others:
        st_copy(other, other).wait_recv()
    largest = st_recv[...]
    scale = jnp.exp(largest - jnp.max(largest, axis=0, keepdims=True))
    total = jnp.sum(
        scale * pltpu.roll(largest.reshape(n * QLEN, PAD), DH, 1).reshape(n, QLEN, PAD), axis=0, keepdims=True
    )
    st_recv[...] = scale / jnp.where(total > 0.0, total, 1.0)
    for step in range(pairs):
        for other in others:
            o_copy(other, other, step).wait_recv()
        mixed = jnp.zeros((QLEN, PAD), jnp.float32)
        for d in range(n):
            share = st_recv[d]
            share = jnp.where(
                lane < DH, share[:, 2 * step + 1 : 2 * step + 2], share[:, 2 * step : 2 * step + 1]
            )
            mixed = mixed + share * o_recv[d, step * QLEN : (step + 1) * QLEN, :].astype(jnp.float32)
        out_ref[2 * step * QLEN : (2 * step + 1) * QLEN, :] = mixed.astype(jnp.bfloat16)
        out_ref[(2 * step + 1) * QLEN : (2 * step + 2) * QLEN, :] = pltpu.roll(mixed, DH, 1).astype(jnp.bfloat16)
    for other in others:
        q_copy(other, me).wait_send()
        st_copy(other, me).wait_send()
        for step in range(pairs):
            o_copy(other, me, step).wait_send()


def attend(query, entering_kv, cached_kv, lengths, n, number):
    requests, positions, width = entering_kv.shape
    length = cached_kv.shape[1]
    pairs, heads = requests // 2, width // PAD
    start = lax.axis_index("mp") * positions
    usable = (start + jnp.arange(positions, dtype=jnp.int32))[None, :] < lengths[0][:, None]
    cached_usable = jnp.arange(length, dtype=jnp.int32)[None, :] < lengths[1][:, None]
    half_type = jnp.bfloat16
    context = pl.pallas_call(
        functools.partial(attend_kernel, n),
        out_shape=jax.ShapeDtypeStruct((2 * requests * QLEN, PAD), half_type),
        in_specs=[pl.BlockSpec(memory_space=m) for m in (VM, pl.ANY, pl.ANY, VM, VM)],
        out_specs=pl.BlockSpec(memory_space=VM),
        scratch_shapes=[
            VM((pairs * QLEN, PAD), half_type),
            VM((n, pairs * QLEN, PAD), half_type),
            VM(entering_kv.shape, half_type),
            VM(cached_kv.shape, half_type),
            VM((2, heads // 2, 2 * QLEN, positions), jnp.float32),
            VM((2, heads // 2, 2 * QLEN, positions), half_type),
            VM((n, pairs * QLEN, PAD), half_type),
            VM((n, pairs * QLEN, PAD), half_type),
            VM((n, QLEN, PAD), jnp.float32),
            VM((n, QLEN, PAD), jnp.float32),
            DMA((2,)), DMA((n,)), DMA((n,)), DMA((pairs, n)), DMA((pairs, n)), DMA((n,)), DMA((n,)),
        ],
        compiler_params=params(number),
        name=f"attend_{number}",
    )(
        query, entering_kv, cached_kv,
        usable.astype(jnp.float32)[:, None, :], cached_usable.astype(jnp.float32)[:, None, :],
    )
    return context


def per_device(
    n,
    hidden,
    norm_gain_attn,
    w_query,
    entering_kv,
    cached_kv,
    enc_lengths,
    w_out,
    norm_gain_ffn,
    w_gate,
    w_up,
    w_down,
):
    rows, width = hidden.shape
    query, plane = make_query(hidden, norm_gain_attn, w_query, w_out, n, 0)
    context = attend(query.reshape(-1, PAD), entering_kv, cached_kv, enc_lengths, n, 1)
    residual = project(context.reshape(n, rows, PAD), hidden, w_out, plane, n, 3)
    portion = gather(normalize(residual, norm_gain_ffn), n, 4).reshape(-1, width)
    gate = jnp.dot(portion, w_gate, preferred_element_type=jnp.float32)
    upward = jnp.dot(portion, w_up, preferred_element_type=jnp.float32)
    activated = (jax.nn.gelu(gate, approximate=True) * upward).astype(jnp.bfloat16)
    feed_out = scatter(activated, w_down, n, 5)
    return (residual.astype(jnp.float32) + feed_out).astype(jnp.bfloat16)


def solution(mesh):
    placed = (
        P(("groups", "mp"), None),
        P(),
        P(None, "mp"),
        P("groups", "mp", None),
        P("groups", None, "mp"),
        P(None, "groups"),
        P("mp", None),
        P(),
        P(None, "mp"),
        P(None, "mp"),
        P("mp", None),
    )
    return jax.shard_map(
        functools.partial(per_device, mesh.shape["mp"]),
        mesh=mesh,
        in_specs=placed,
        out_specs=P(("groups", "mp"), None),
        check_vma=False,
    )
```

```python
import functools

import jax
import jax.numpy as jnp
from jax import lax
from jax.experimental import pallas as pl
from jax.experimental.pallas import tpu as pltpu
from jax.sharding import PartitionSpec as P

DH = 64
QLEN = 32
PAD = 2 * DH
MESH = pl.DeviceIdType.MESH
VM = pltpu.VMEM
DMA = pltpu.SemaphoreType.DMA

epsilon = 0.1


def place(n):
    me = lax.axis_index("mp")
    return me, me // 4, (me // 2) % 2, me % 2


def index_of(a, b, c):
    return (a * 2 + b) * 2 + c


def remote(src, dst, send, recv, to):
    return pltpu.make_async_remote_copy(
        src_ref=src, dst_ref=dst, send_sem=send, recv_sem=recv, device_id={"mp": to}, device_id_type=MESH
    )


def greet(to):
    pl.semaphore_signal(pltpu.get_barrier_semaphore(), inc=1, device_id={"mp": to}, device_id_type=MESH)


def params(number):
    return pltpu.CompilerParams(collective_id=number, has_side_effects=True, vmem_limit_bytes=56 * 2**20)


def pieces_of(n, width):
    return max(1, min(4, 16 // (n // 4), width // 128))


def neighbours(n):
    A = n // 4
    me, a, b, c = place(n)
    has = {1: a < A - 1, -1: a > 0}
    toward = {1: me + 4, -1: me - 4}
    return has, toward


def greet_along(has, toward):
    for d in (1, -1):

        @pl.when(has[d])
        def _():
            greet(toward[d])


def await_greetings(has, others):
    pl.semaphore_wait(
        pltpu.get_barrier_semaphore(), others + has[1].astype(jnp.int32) + has[-1].astype(jnp.int32)
    )


def query_kernel(
    n, x_ref, gain_ref, wq_ref, wo_ref, q_ref, plane_ref,
    xs, w2, q_send, q_recv, local, zs, zr, cs, cr, ws, wr, ps, pr,
):
    A = n // 4
    me, a, b, c = place(n)
    across, pair = index_of(a, 1 - b, c), index_of(a, b, 1 - c)
    has, toward = neighbours(n)
    P, W = xs.shape[0], xs.shape[-1]
    rows = x_ref.shape[0]
    greet_along(has, toward)
    greet(across)
    greet(pair)
    load_w = pltpu.make_async_copy(wq_ref, w2.at[0], local.at[0])
    load_w.start()
    values = x_ref[...].astype(jnp.float32)
    scale = lax.rsqrt(jnp.mean(values * values, axis=-1, keepdims=True) + epsilon)
    for p in range(P):
        part = slice(p * W, (p + 1) * W)
        xs[p, a, c] = (values[:, part] * scale * gain_ref[:, part]).astype(jnp.bfloat16)
    await_greetings(has, 2)

    def z_copy(k, p, s, d):
        row = 0 if d == 1 else A
        return remote(xs.at[p, k, c], xs.at[p, k, c], zs.at[row + s, p], zr.at[k, p], toward[d])

    def c_copy(k, p, cc):
        return remote(xs.at[p, k, cc], xs.at[p, k, cc], cs.at[k, p], cr.at[k, p], pair)

    wq_copy = remote(wq_ref, w2.at[1], ws.at[0], wr.at[0], across)
    q_copy = remote(q_send, q_recv, ws.at[1], wr.at[1], across)
    plane_pair = remote(wo_ref, plane_ref.at[0], ps.at[0], pr.at[0], pair)
    plane_across = remote(wo_ref, plane_ref.at[1], ps.at[1], pr.at[1], across)
    plane_diagonal = remote(plane_ref.at[1], plane_ref.at[2], ps.at[2], pr.at[2], pair)
    for p in range(P):
        for d in (1, -1):

            @pl.when(has[d])
            def _():
                z_copy(a, p, 0, d).start()

    wq_copy.start()
    plane_across.start()
    for p in range(P):
        c_copy(a, p, c).start()
    plane_pair.start()
    for s in range(1, A):
        for p in range(P):
            for d in (1, -1):
                k = a - s * d

                @pl.when((k >= 0) & (k < A))
                def _():
                    remote(xs.at[p, k, c], xs.at[p, k, c], zs.at[0, p], zr.at[k, p], toward[-d]).wait_recv()

                    @pl.when(has[d])
                    def _():
                        z_copy(k, p, s, d).start()

                    c_copy(k, p, c).start()

    load_w.wait()
    wq_copy.wait_recv()
    for k in range(A):
        for p in range(P):
            c_copy(k, p, 1 - c).wait_recv()
    total = jnp.zeros((2 * A * rows, PAD), jnp.float32)
    for p in range(P):
        total = total + lax.dot_general(
            xs[p].reshape(2 * A * rows, W), w2[:, :, p * W : (p + 1) * W].reshape(PAD, W),
            (((1,), (1,)), ((), ())), preferred_element_type=jnp.float32,
        )
    q_send[...] = total.astype(jnp.bfloat16)
    low = lax.broadcasted_iota(jnp.int32, (2 * A * rows, PAD), 1) < DH
    own = jnp.where(low, total, 0.0).astype(jnp.bfloat16).reshape(2 * A, rows, PAD)
    for k in range(A):
        for cc in range(2):
            q_ref[index_of(k, b, cc)] = own[2 * k + cc]
    q_copy.start()
    plane_across.wait_recv()
    plane_diagonal.start()
    for s in range(A):
        for d in (1, -1):
            k = a - s * d

            @pl.when((k >= 0) & (k < A) & has[d])
            def _():
                for p in range(P):
                    z_copy(k, p, s, d).wait_send()

    for k in range(A):
        for p in range(P):
            c_copy(k, p, c).wait_send()
    q_copy.wait_recv()
    came = pltpu.roll(q_recv[...].astype(jnp.float32), DH, 1)
    came = jnp.where(low, came, 0.0).astype(jnp.bfloat16).reshape(2 * A, rows, PAD)
    for k in range(A):
        for cc in range(2):
            q_ref[index_of(k, 1 - b, cc)] = came[2 * k + cc]
    wq_copy.wait_send()
    q_copy.wait_send()
    plane_across.wait_send()
    plane_pair.wait()
    plane_diagonal.wait()


def make_query(hidden, gain, w_query, w_out, n, number):
    A = n // 4
    rows, width = hidden.shape
    P = pieces_of(n, width)
    W = width // P
    half = jnp.bfloat16
    return pl.pallas_call(
        functools.partial(query_kernel, n),
        out_shape=[
            jax.ShapeDtypeStruct((n, rows, PAD), half),
            jax.ShapeDtypeStruct((3,) + w_out.shape, half),
        ],
        in_specs=[pl.BlockSpec(memory_space=m) for m in (VM, VM, pl.ANY, pl.ANY)],
        out_specs=[pl.BlockSpec(memory_space=VM), pl.BlockSpec(memory_space=pl.ANY)],
        scratch_shapes=[
            VM((P, A, 2, rows, W), half),
            VM((2, DH, width), half),
            VM((2 * A * rows, PAD), half),
            VM((2 * A * rows, PAD), half),
            DMA((1,)), DMA((2 * A, P)), DMA((A, P)), DMA((A, P)), DMA((A, P)),
            DMA((2,)), DMA((2,)), DMA((3,)), DMA((3,)),
        ],
        compiler_params=params(number),
        name=f"query_{number}",
    )(hidden, gain[None, :], w_query.T, w_out)


def project_kernel(
    n, context_ref, hidden_ref, wo_ref, plane_ref, out_ref,
    w4, c_send, c_recv, part, zsend, zright, zleft, local, cs, cr, zs, zr,
):
    A = n // 4
    me, a, b, c = place(n)
    peers = (index_of(a, b, 1 - c), index_of(a, 1 - b, c), index_of(a, 1 - b, 1 - c))
    has, toward = neighbours(n)
    landing = {1: zright, -1: zleft}
    P, _, rows, W = part.shape
    depth = wo_ref.shape[0]
    greet_along(has, toward)
    for peer in peers:
        greet(peer)
    load_own = pltpu.make_async_copy(wo_ref, w4.at[0], local.at[0])
    load_plane = pltpu.make_async_copy(plane_ref, w4.at[pl.ds(1, 3)], local.at[1])
    load_own.start()
    load_plane.start()
    for i, (bb, cc) in enumerate(((b, 1 - c), (1 - b, c), (1 - b, 1 - c))):
        for k in range(A):
            c_send[i, k] = context_ref[index_of(k, bb, cc)]
    for k in range(A):
        c_recv[0, k] = context_ref[index_of(k, b, c)]
    await_greetings(has, 3)
    swaps = [remote(c_send.at[i], c_recv.at[i + 1], cs.at[i], cr.at[i], peers[i]) for i in range(3)]
    for i in (2, 1, 0):
        swaps[i].start()
    load_own.wait()
    load_plane.wait()
    for swap in swaps:
        swap.wait_recv()
    low = lax.broadcasted_iota(jnp.int32, (A * rows, PAD), 1) < DH

    def beside(i):
        first = c_recv[i].reshape(A * rows, PAD).astype(jnp.float32)
        second = c_recv[i + 1].reshape(A * rows, PAD).astype(jnp.float32)
        return jnp.where(low, pltpu.roll(first, DH, 1), second).astype(jnp.bfloat16)

    left = jnp.concatenate([beside(0), beside(2)], axis=1)

    def z_copy(k, p, d):
        return remote(zsend.at[p, k], landing[d].at[p, k], zs.at[k, p], zr.at[(0 if d == 1 else A) + k, p], toward[d])

    def z_arrival(k, p, d):
        return remote(zsend.at[p, k], landing[d].at[p, k], zs.at[k, p], zr.at[(0 if d == 1 else A) + k, p], toward[-d])

    for s in range(A - 1, -1, -1):
        for p in range(P):
            if s == A - 1:
                w = w4[:, :, p * W : (p + 1) * W].reshape(4 * depth, W)
                found = jnp.dot(left, w, preferred_element_type=jnp.float32)
                part[p] = found.reshape(A, rows, W)
            for d in (1, -1) if s else (1,):
                k = a + s * d

                @pl.when((k >= 0) & (k < A))
                def _():
                    for came in (d,) if s else (1, -1):

                        @pl.when(has[-came])
                        def _():
                            z_arrival(k, p, came).wait_recv()
                            part[p, k] = part[p, k] + landing[came][p, k].astype(jnp.float32)

                    if s:
                        zsend[p, k] = part[p, k].astype(jnp.bfloat16)
                        z_copy(k, p, d).start()
                    else:
                        at = slice(p * W, (p + 1) * W)
                        out_ref[:, at] = (hidden_ref[:, at].astype(jnp.float32) + part[p, k]).astype(jnp.bfloat16)

    for s in range(A - 1, 0, -1):
        for d in (1, -1):
            k = a + s * d

            @pl.when((k >= 0) & (k < A))
            def _():
                for p in range(P):
                    z_copy(k, p, d).wait_send()

    for swap in swaps:
        swap.wait_send()


def project(context, hidden, w_out, plane, n, number):
    A = n // 4
    rows, width = hidden.shape
    P = pieces_of(n, width)
    W = width // P
    half = jnp.bfloat16
    return pl.pallas_call(
        functools.partial(project_kernel, n),
        out_shape=jax.ShapeDtypeStruct((rows, width), half),
        in_specs=[pl.BlockSpec(memory_space=m) for m in (VM, VM, pl.ANY, pl.ANY)],
        out_specs=pl.BlockSpec(memory_space=VM),
        scratch_shapes=[
            VM((4,) + w_out.shape, half),
            VM((3, A, rows, PAD), half),
            VM((4, A, rows, PAD), half),
            VM((P, A, rows, W), jnp.float32),
        ]
        + [VM((P, A, rows, W), half)] * 3
        + [DMA((2,)), DMA((3,)), DMA((3,)), DMA((A, P)), DMA((2 * A, P))],
        compiler_params=params(number),
        name=f"project_{number}",
    )(context, hidden, w_out, plane)


def attend_kernel(
    n, own_ref, kv_ref, cached_ref, mask_ref, cached_mask_ref, out_ref,
    q_ref, q_all, kv, cached, scores, chances, o_send, o_recv, st_send, st_recv, local, qs, qr, os, orr, ss, sr,
):
    me = lax.axis_index("mp")
    requests, positions, width = kv.shape
    pairs, heads = requests // 2, width // PAD
    load_cached = pltpu.make_async_copy(cached_ref, cached, local.at[0])
    load_kv = pltpu.make_async_copy(kv_ref, kv, local.at[1])
    load_cached.start()
    load_kv.start()
    order = sorted(range(1, n), key=lambda s: -min(s, n - s))
    others = [lax.rem(me + s, n) for s in order]
    for other in others:
        greet(other)
    for step in range(pairs):
        even, odd = (
            own_ref[(2 * step + i) * QLEN : (2 * step + i + 1) * QLEN, :].astype(jnp.float32) for i in range(2)
        )
        q_ref[step * QLEN : (step + 1) * QLEN, :] = (even + pltpu.roll(odd, DH, 1)).astype(jnp.bfloat16)
    pl.semaphore_wait(pltpu.get_barrier_semaphore(), n - 1)

    def q_copy(other, spot):
        return remote(q_ref, q_all.at[spot], qs.at[other], qr.at[spot], other)

    def o_copy(other, spot, step):
        rows = pl.ds(pl.multiple_of(step * QLEN, QLEN), QLEN)
        return remote(
            o_send.at[other, rows], o_recv.at[spot, rows], os.at[step, other], orr.at[step, spot], other
        )

    def st_copy(other, spot):
        return remote(st_send.at[other], st_recv.at[spot], ss.at[other], sr.at[spot], other)

    for other in others:
        q_copy(other, me).start()
    q_all[me] = q_ref[...]
    lane = lax.broadcasted_iota(jnp.int32, (QLEN, PAD), 1)
    load_cached.wait()

    def cached_request(r, carry):
        to = pl.ds(pl.multiple_of((requests + r) * QLEN, QLEN), QLEN)
        block = cached[r]
        found = lax.dot_general(
            own_ref[to, :], block, (((1,), (1,)), ((), ())), preferred_element_type=jnp.float32
        )
        usable = cached_mask_ref[r] > 0.5
        masked = jnp.where(usable, found, -1e30)
        exponent = jnp.where(usable, jnp.exp(masked - jnp.max(masked, axis=-1, keepdims=True)), 0.0)
        weights = (exponent / jnp.sum(exponent, axis=-1, keepdims=True)).astype(jnp.bfloat16)
        out_ref[to, :] = jnp.dot(weights, block, preferred_element_type=jnp.float32).astype(jnp.bfloat16)
        return carry

    lax.fori_loop(0, requests, cached_request, 0)
    st_send[...] = jnp.zeros_like(st_send)
    load_kv.wait()
    for other in others:
        q_copy(other, other).wait_recv()

    def pair_step(step, carry):
        rows = pl.ds(pl.multiple_of(step * QLEN, QLEN), QLEN)
        low = lane < DH
        nothing = jnp.zeros((QLEN, PAD), jnp.bfloat16)
        for i in range(2):
            for g in range(heads // 2):
                two = []
                for h in (2 * g, 2 * g + 1):
                    packed = q_all[h, rows, :].astype(jnp.float32)
                    packed = packed if i == 0 else pltpu.roll(packed, DH, 1)
                    two.append(jnp.where(low, packed, 0.0).astype(jnp.bfloat16))
                spread = jnp.concatenate(
                    [
                        jnp.concatenate([two[0], nothing], axis=1),
                        jnp.concatenate([nothing, two[1]], axis=1),
                    ],
                    axis=0,
                )
                scores[i, g] = lax.dot_general(
                    spread, kv[step * 2 + i, :, g * 2 * PAD : (g + 1) * 2 * PAD], (((1,), (1,)), ((), ())),
                    preferred_element_type=jnp.float32,
                )
        for i in range(2):
            r = step * 2 + i
            usable = mask_ref[r] > 0.5
            masked = jnp.where(usable, scores[i], -1e30)
            largest = jnp.max(masked, axis=-1, keepdims=True)
            exponent = jnp.where(usable, jnp.exp(masked - largest), 0.0)
            total = jnp.sum(exponent, axis=-1, keepdims=True)
            chances[i] = exponent.astype(jnp.bfloat16)
            st_send[...] = jnp.where(
                lane == r,
                largest.reshape(heads, QLEN, 1),
                jnp.where(lane == r + DH, total.reshape(heads, QLEN, 1), st_send[...]),
            )
        for g in range(heads // 2):
            found = [
                jnp.dot(
                    chances[i, g], kv[step * 2 + i, :, g * 2 * PAD : (g + 1) * 2 * PAD],
                    preferred_element_type=jnp.float32,
                )
                for i in range(2)
            ]
            for e in range(2):
                even, odd = (f[e * QLEN : (e + 1) * QLEN, e * PAD : (e + 1) * PAD] for f in found)
                o_send[2 * g + e, rows, :] = jnp.where(low, pltpu.roll(odd, DH, 1), even).astype(jnp.bfloat16)
        for other in others:
            o_copy(other, me, step).start()
        return carry

    lax.fori_loop(0, pairs, pair_step, 0)
    for other in others:
        st_copy(other, me).start()
    o_recv[me] = o_send[me]
    st_recv[me] = st_send[me]
    for other in others:
        st_copy(other, other).wait_recv()
    largest = st_recv[...]
    scale = jnp.exp(largest - jnp.max(largest, axis=0, keepdims=True))
    total = jnp.sum(
        scale * pltpu.roll(largest.reshape(n * QLEN, PAD), DH, 1).reshape(n, QLEN, PAD), axis=0, keepdims=True
    )
    st_recv[...] = scale / jnp.where(total > 0.0, total, 1.0)
    for step in range(pairs):
        for other in others:
            o_copy(other, other, step).wait_recv()
        mixed = jnp.zeros((QLEN, PAD), jnp.float32)
        for d in range(n):
            share = st_recv[d]
            share = jnp.where(
                lane < DH, share[:, 2 * step + 1 : 2 * step + 2], share[:, 2 * step : 2 * step + 1]
            )
            mixed = mixed + share * o_recv[d, step * QLEN : (step + 1) * QLEN, :].astype(jnp.float32)
        out_ref[2 * step * QLEN : (2 * step + 1) * QLEN, :] = mixed.astype(jnp.bfloat16)
        out_ref[(2 * step + 1) * QLEN : (2 * step + 2) * QLEN, :] = pltpu.roll(mixed, DH, 1).astype(jnp.bfloat16)
    for other in others:
        q_copy(other, me).wait_send()
        st_copy(other, me).wait_send()
        for step in range(pairs):
            o_copy(other, me, step).wait_send()


def attend(query, entering_kv, cached_kv, lengths, n, number):
    requests, positions, width = entering_kv.shape
    length = cached_kv.shape[1]
    pairs, heads = requests // 2, width // PAD
    start = lax.axis_index("mp") * positions
    usable = (start + jnp.arange(positions, dtype=jnp.int32))[None, :] < lengths[0][:, None]
    cached_usable = jnp.arange(length, dtype=jnp.int32)[None, :] < lengths[1][:, None]
    half_type = jnp.bfloat16
    context = pl.pallas_call(
        functools.partial(attend_kernel, n),
        out_shape=jax.ShapeDtypeStruct((2 * requests * QLEN, PAD), half_type),
        in_specs=[pl.BlockSpec(memory_space=m) for m in (VM, pl.ANY, pl.ANY, VM, VM)],
        out_specs=pl.BlockSpec(memory_space=VM),
        scratch_shapes=[
            VM((pairs * QLEN, PAD), half_type),
            VM((n, pairs * QLEN, PAD), half_type),
            VM(entering_kv.shape, half_type),
            VM(cached_kv.shape, half_type),
            VM((2, heads // 2, 2 * QLEN, positions), jnp.float32),
            VM((2, heads // 2, 2 * QLEN, positions), half_type),
            VM((n, pairs * QLEN, PAD), half_type),
            VM((n, pairs * QLEN, PAD), half_type),
            VM((n, QLEN, PAD), jnp.float32),
            VM((n, QLEN, PAD), jnp.float32),
            DMA((2,)), DMA((n,)), DMA((n,)), DMA((pairs, n)), DMA((pairs, n)), DMA((n,)), DMA((n,)),
        ],
        compiler_params=params(number),
        name=f"attend_{number}",
    )(
        query, entering_kv, cached_kv,
        usable.astype(jnp.float32)[:, None, :], cached_usable.astype(jnp.float32)[:, None, :],
    )
    return context


def far_first(A, a):
    low, high = 0, A - 1
    found = []
    for _ in range(A):
        left = (a - low > high - a).astype(jnp.int32)
        found.append(high + left * (low - high))
        low, high = low + left, high - 1 + left
    return found


def feed_kernel(
    n, x_ref, gain_ref, gate_ref, up_ref, down_ref, out_ref,
    xs, w_gate, w_up, w_down, gates, ups, act, part, cbuf, ysend, yrecv, zsend, zland,
    local, zs, zr, ys, yr, cs, cr, gs, gr, hs, hr, ts, tr,
):
    A = n // 4
    me, a, b, c = place(n)
    across, pair = index_of(a, 1 - b, c), index_of(a, b, 1 - c)
    has, toward = neighbours(n)
    P, W = xs.shape[0], xs.shape[-1]
    rows = x_ref.shape[0]
    greet_along(has, toward)
    greet(across)
    greet(pair)
    loads = [
        pltpu.make_async_copy(src, dst, local.at[i])
        for i, (src, dst) in enumerate(((gate_ref, w_gate), (up_ref, w_up), (down_ref, w_down)))
    ]
    for load in loads:
        load.start()
    values = x_ref[...].astype(jnp.float32)
    scale = lax.rsqrt(jnp.mean(values * values, axis=-1, keepdims=True) + epsilon)
    for p in range(P):
        at = slice(p * W, (p + 1) * W)
        xs[p, b, c, a] = (values[:, at] * scale * gain_ref[:, at]).astype(jnp.bfloat16)
    await_greetings(has, 2)

    def z_copy(k, p, s, d):
        block = xs.at[p, b, c, k]
        return remote(block, block, zs.at[(0 if d == 1 else A) + s, p], zr.at[k, p], toward[d])

    def y_copy(k, p, bb):
        block = xs.at[p, bb, c, k]
        return remote(block, block, ys.at[k, p], yr.at[k, p], across)

    def c_copy(k, p, bb, cc):
        block = xs.at[p, bb, cc, k]
        return remote(block, block, cs.at[bb * A + k, p], cr.at[bb * A + k, p], pair)

    for p in range(P):
        for d in (1, -1):

            @pl.when(has[d])
            def _():
                z_copy(a, p, 0, d).start()

        y_copy(a, p, b).start()
    for p in range(P):
        c_copy(a, p, b, c).start()

    def pass_on(s, p):
        for d in (1, -1) if s else (1,):
            k = a - s * d

            @pl.when((k >= 0) & (k < A))
            def _():
                y_copy(k, p, 1 - b).wait_recv()
                c_copy(k, p, 1 - b, c).start()

    for s in range(1, A):
        for p in range(P):
            for d in (1, -1):
                k = a - s * d

                @pl.when((k >= 0) & (k < A))
                def _():
                    block = xs.at[p, b, c, k]
                    remote(block, block, zs.at[0, p], zr.at[k, p], toward[-d]).wait_recv()

                    @pl.when(has[d])
                    def _():
                        z_copy(k, p, s, d).start()

                    y_copy(k, p, b).start()
                    c_copy(k, p, b, c).start()

            if s > 1:
                pass_on(s - 2, p)
    for p in range(P):
        pass_on(A - 2, p)
    for load in loads:
        load.wait()

    def contract(p):
        for bb in range(2):
            for k in range(A):
                c_copy(k, p, bb, 1 - c).wait_recv()
        left = xs[p].reshape(n * rows, W)
        for w, sums in ((w_gate, gates), (w_up, ups)):
            found = jnp.dot(left, w[p * W : (p + 1) * W, :], preferred_element_type=jnp.float32)
            sums[...] = found if p == 0 else sums[...] + found

    for p in range(P):
        pass_on(A - 1, p)
        if p:
            contract(p - 1)
    contract(P - 1)
    for p in range(P):
        for s in range(A):
            for d in (1, -1):
                k = a - s * d

                @pl.when((k >= 0) & (k < A) & has[d])
                def _():
                    z_copy(k, p, s, d).wait_send()

        for k in range(A):
            y_copy(k, p, b).wait_send()
            for bb in range(2):
                c_copy(k, p, bb, c).wait_send()

    tall = A * rows
    for group in range(4):
        at = slice(group * tall, (group + 1) * tall)
        act[group] = (jax.nn.gelu(gates[at, :], approximate=True) * ups[at, :]).astype(jnp.bfloat16)

    def multiply(i, p, bb, cc):
        found = jnp.dot(act[2 * bb + cc], w_down[:, p * W : (p + 1) * W], preferred_element_type=jnp.float32)
        part[i, p] = found.reshape(A, rows, W)

    def g_copy(side, p):
        return remote(part.at[2 * side, p], cbuf.at[side, p], gs.at[side, p], gr.at[side, p], pair)

    def h_copy(k, p):
        return remote(ysend.at[p, k], yrecv.at[p, k], hs.at[k, p], hr.at[k, p], across)

    def t_copy(k, p, right):
        return remote(
            zsend.at[p, k], zland.at[right, p, k], ts.at[k, p], tr.at[right, k, p], me + 8 * right - 4
        )

    def t_arrival(k, p, right):
        return remote(
            zsend.at[p, k], zland.at[right, p, k], ts.at[k, p], tr.at[right, k, p], me - 8 * right + 4
        )

    order = far_first(A, a)
    for t, k in enumerate(order):
        for p in range(P):
            if t == 0:
                if p == 0:
                    multiply(0, p, 1 - b, 1 - c)
                    g_copy(0, p).start()
                    multiply(1, p, 1 - b, c)
                if p + 1 < P:
                    multiply(0, p + 1, 1 - b, 1 - c)
                    g_copy(0, p + 1).start()
                g_copy(0, p).wait_recv()
            ysend[p, k] = (part[1, p, k] + cbuf[0, p, k]).astype(jnp.bfloat16)
            h_copy(k, p).start()
            if t == 0 and p + 1 < P:
                multiply(1, p + 1, 1 - b, c)
    for p in range(P):
        multiply(2, p, b, 1 - c)
        g_copy(1, p).start()
    for p in range(P):
        multiply(3, p, b, c)
    for t, k in enumerate(order):
        right = (k > a).astype(jnp.int32)
        for p in range(P):
            if t == 0:
                g_copy(1, p).wait_recv()
            h_copy(k, p).wait_recv()
            part[3, p, k] = part[3, p, k] + cbuf[1, p, k] + yrecv[p, k].astype(jnp.float32)
            if t < A - 1:
                comes = ((right == 1) & (a > 0)) | ((right == 0) & (a < A - 1))

                @pl.when(comes)
                def _():
                    t_arrival(k, p, right).wait_recv()
                    part[3, p, k] = part[3, p, k] + zland[right, p, k].astype(jnp.float32)

                zsend[p, k] = part[3, p, k].astype(jnp.bfloat16)
                t_copy(k, p, right).start()
            else:
                for came in (1, -1):

                    @pl.when(has[-came])
                    def _():
                        side = (came + 1) // 2
                        t_arrival(k, p, side).wait_recv()
                        part[3, p, k] = part[3, p, k] + zland[side, p, k].astype(jnp.float32)

                at = slice(p * W, (p + 1) * W)
                out_ref[:, at] = (x_ref[:, at].astype(jnp.float32) + part[3, p, k]).astype(jnp.bfloat16)

    for t, k in enumerate(order):
        right = (k > a).astype(jnp.int32)
        for p in range(P):
            h_copy(k, p).wait_send()
            if t < A - 1:
                t_copy(k, p, right).wait_send()
    for p in range(P):
        g_copy(0, p).wait_send()
        g_copy(1, p).wait_send()


def feed(residual, gain, w_gate, w_up, w_down, n, number):
    A = n // 4
    rows, width = residual.shape
    hidden_units = w_gate.shape[1]
    P = pieces_of(n, width)
    W = width // P
    half, full = jnp.bfloat16, jnp.float32
    return pl.pallas_call(
        functools.partial(feed_kernel, n),
        out_shape=jax.ShapeDtypeStruct((rows, width), half),
        in_specs=[pl.BlockSpec(memory_space=m) for m in (VM, VM, pl.ANY, pl.ANY, pl.ANY)],
        out_specs=pl.BlockSpec(memory_space=VM),
        scratch_shapes=[
            VM((P, 2, 2, A, rows, W), half),
            VM(w_gate.shape, half),
            VM(w_up.shape, half),
            VM(w_down.shape, half),
            VM((n * rows, hidden_units), full),
            VM((n * rows, hidden_units), full),
            VM((4, A * rows, hidden_units), half),
            VM((4, P, A, rows, W), full),
            VM((2, P, A, rows, W), full),
        ]
        + [VM((P, A, rows, W), half)] * 3
        + [VM((2, P, A, rows, W), half)]
        + [
            DMA((3,)), DMA((2 * A, P)), DMA((A, P)), DMA((A, P)), DMA((A, P)), DMA((2 * A, P)), DMA((2 * A, P)),
            DMA((2, P)), DMA((2, P)), DMA((A, P)), DMA((A, P)), DMA((A, P)), DMA((2, A, P)),
        ],
        compiler_params=params(number),
        name=f"feed_{number}",
    )(residual, gain[None, :], w_gate, w_up, w_down)


def per_device(
    n,
    hidden,
    norm_gain_attn,
    w_query,
    entering_kv,
    cached_kv,
    enc_lengths,
    w_out,
    norm_gain_ffn,
    w_gate,
    w_up,
    w_down,
):
    rows, width = hidden.shape
    query, plane = make_query(hidden, norm_gain_attn, w_query, w_out, n, 0)
    context = attend(query.reshape(-1, PAD), entering_kv, cached_kv, enc_lengths, n, 1)
    residual = project(context.reshape(n, rows, PAD), hidden, w_out, plane, n, 3)
    return feed(residual, norm_gain_ffn, w_gate, w_up, w_down, n, 4)


def solution(mesh):
    placed = (
        P(("groups", "mp"), None),
        P(),
        P(None, "mp"),
        P("groups", "mp", None),
        P("groups", None, "mp"),
        P(None, "groups"),
        P("mp", None),
        P(),
        P(None, "mp"),
        P(None, "mp"),
        P("mp", None),
    )
    return jax.shard_map(
        functools.partial(per_device, mesh.shape["mp"]),
        mesh=mesh,
        in_specs=placed,
        out_specs=P(("groups", "mp"), None),
        check_vma=False,
    )
```

```python
import functools

import jax
import jax.numpy as jnp
from jax import lax
from jax.experimental import pallas as pl
from jax.experimental.pallas import tpu as pltpu
from jax.sharding import PartitionSpec as P

DH = 64
QLEN = 32
PAD = 2 * DH
MESH = pl.DeviceIdType.MESH
VM = pltpu.VMEM
DMA = pltpu.SemaphoreType.DMA

epsilon = 0.1


def place(n):
    me = lax.axis_index("mp")
    return me, me // 4, (me // 2) % 2, me % 2


def index_of(a, b, c):
    return (a * 2 + b) * 2 + c


def remote(src, dst, send, recv, to):
    return pltpu.make_async_remote_copy(
        src_ref=src, dst_ref=dst, send_sem=send, recv_sem=recv, device_id={"mp": to}, device_id_type=MESH
    )


def greet(to):
    pl.semaphore_signal(pltpu.get_barrier_semaphore(), inc=1, device_id={"mp": to}, device_id_type=MESH)


def params(number):
    return pltpu.CompilerParams(collective_id=number, has_side_effects=True, vmem_limit_bytes=56 * 2**20)


def pieces_of(n, width):
    return max(1, min(4, 16 // (n // 4), width // 128))


def neighbours(n):
    A = n // 4
    me, a, b, c = place(n)
    has = {1: a < A - 1, -1: a > 0}
    toward = {1: me + 4, -1: me - 4}
    return has, toward


def greet_along(has, toward):
    for d in (1, -1):

        @pl.when(has[d])
        def _():
            greet(toward[d])


def await_greetings(has, others):
    pl.semaphore_wait(
        pltpu.get_barrier_semaphore(), others + has[1].astype(jnp.int32) + has[-1].astype(jnp.int32)
    )


def query_kernel(
    n, groups, x_ref, gain_ref, wq_ref, wo_ref, q_ref, plane_ref,
    xs, w2, local, zs, zr, cs, cr, ys, yr, gs, gr, ps, pr,
):
    A = n // 4
    me, a, b, c = place(n)
    mine = lax.axis_index("groups")
    across, pair = index_of(a, 1 - b, c), index_of(a, b, 1 - c)
    has, toward = neighbours(n)
    P, W = xs.shape[0], xs.shape[-1]
    rows = x_ref.shape[0]
    share = DH // groups
    twins = [lax.rem(mine + i, groups) for i in range(1, groups)]
    greet_along(has, toward)
    greet(across)
    greet(pair)
    for twin in twins:
        pl.semaphore_signal(
            pltpu.get_barrier_semaphore(), inc=1, device_id={"groups": twin, "mp": me}, device_id_type=MESH
        )
    load_w = pltpu.make_async_copy(wq_ref, w2.at[b], local.at[0])
    load_w.start()
    values = x_ref[...].astype(jnp.float32)
    scale = lax.rsqrt(jnp.mean(values * values, axis=-1, keepdims=True) + epsilon)
    for p in range(P):
        part = slice(p * W, (p + 1) * W)
        xs[p, a, c] = (values[:, part] * scale * gain_ref[:, part]).astype(jnp.bfloat16)
    await_greetings(has, 1 + groups)

    def z_copy(k, p, s, d):
        row = 0 if d == 1 else A
        return remote(xs.at[p, k, c], xs.at[p, k, c], zs.at[row + s, p], zr.at[k, p], toward[d])

    def c_copy(k, p, cc):
        return remote(xs.at[p, k, cc], xs.at[p, k, cc], cs.at[k, p], cr.at[k, p], pair)

    def strip(part):
        return pl.ds(pl.multiple_of(part * share, share), share)

    def landing(which, bb, part):
        return w2.at[bb, strip(part)] if which == 0 else plane_ref.at[1, strip(part)]

    def y_copy(which):
        source = (wq_ref, wo_ref)[which].at[strip(mine)]
        return remote(source, landing(which, b, mine), ys.at[which], yr.at[which], across)

    def y_arrival(which):
        spot = landing(which, 1 - b, mine)
        return remote(spot, spot, ys.at[which], yr.at[which], across)

    def g_copy(which, part, to):
        spot = landing(which, 1 - b, part)
        return pltpu.make_async_remote_copy(
            src_ref=spot, dst_ref=spot, send_sem=gs.at[which, to], recv_sem=gr.at[which, part],
            device_id={"groups": to, "mp": me}, device_id_type=MESH,
        )

    plane_pair = remote(wo_ref, plane_ref.at[0], ps.at[0], pr.at[0], pair)
    plane_diagonal = remote(plane_ref.at[1], plane_ref.at[2], ps.at[1], pr.at[1], pair)
    for p in range(P):
        for d in (1, -1):

            @pl.when(has[d])
            def _():
                z_copy(a, p, 0, d).start()

    for which in range(2):
        y_copy(which).start()
    for p in range(P):
        c_copy(a, p, c).start()
    plane_pair.start()
    for s in range(1, A):
        for p in range(P):
            for d in (1, -1):
                k = a - s * d

                @pl.when((k >= 0) & (k < A))
                def _():
                    remote(xs.at[p, k, c], xs.at[p, k, c], zs.at[0, p], zr.at[k, p], toward[-d]).wait_recv()

                    @pl.when(has[d])
                    def _():
                        z_copy(k, p, s, d).start()

                    c_copy(k, p, c).start()

        if s < 3:
            y_arrival(s - 1).wait_recv()
            for twin in twins:
                g_copy(s - 1, mine, twin).start()
    for which in range(2):
        for twin in twins:
            g_copy(which, twin, mine).wait_recv()
    plane_diagonal.start()
    load_w.wait()
    total = jnp.zeros((2 * A * rows, PAD), jnp.float32)
    for p in range(P):
        for k in range(A):
            c_copy(k, p, 1 - c).wait_recv()
        total = total + lax.dot_general(
            xs[p].reshape(2 * A * rows, W), w2[:, :, p * W : (p + 1) * W].reshape(PAD, W),
            (((1,), (1,)), ((), ())), preferred_element_type=jnp.float32,
        )
    q_ref[...] = total.astype(jnp.bfloat16).reshape(2 * A, rows, PAD)
    for s in range(A):
        for d in (1, -1):
            k = a - s * d

            @pl.when((k >= 0) & (k < A) & has[d])
            def _():
                for p in range(P):
                    z_copy(k, p, s, d).wait_send()

    for k in range(A):
        for p in range(P):
            c_copy(k, p, c).wait_send()
    for which in range(2):
        y_copy(which).wait_send()
        for twin in twins:
            g_copy(which, mine, twin).wait_send()
    plane_pair.wait()
    plane_diagonal.wait()


def make_query(hidden, gain, w_query, w_out, n, groups, number):
    A = n // 4
    assert A > 2 and DH % groups == 0
    rows, width = hidden.shape
    P = pieces_of(n, width)
    W = width // P
    half = jnp.bfloat16
    return pl.pallas_call(
        functools.partial(query_kernel, n, groups),
        out_shape=[
            jax.ShapeDtypeStruct((2 * A, rows, PAD), half),
            jax.ShapeDtypeStruct((3,) + w_out.shape, half),
        ],
        in_specs=[pl.BlockSpec(memory_space=m) for m in (VM, VM, pl.ANY, pl.ANY)],
        out_specs=[pl.BlockSpec(memory_space=VM), pl.BlockSpec(memory_space=pl.ANY)],
        scratch_shapes=[
            VM((P, A, 2, rows, W), half),
            VM((2, DH, width), half),
            DMA((1,)), DMA((2 * A, P)), DMA((A, P)), DMA((A, P)), DMA((A, P)),
            DMA((2,)), DMA((2,)), DMA((2, groups)), DMA((2, groups)), DMA((2,)), DMA((2,)),
        ],
        compiler_params=params(number),
        name=f"query_{number}",
    )(hidden, gain[None, :], w_query.T, w_out)


def project_kernel(
    n, context_ref, hidden_ref, wo_ref, plane_ref, out_ref,
    w4, c_send, c_recv, part, zsend, zright, zleft, local, cs, cr, zs, zr,
):
    A = n // 4
    me, a, b, c = place(n)
    peers = (index_of(a, b, 1 - c), index_of(a, 1 - b, c), index_of(a, 1 - b, 1 - c))
    has, toward = neighbours(n)
    landing = {1: zright, -1: zleft}
    P, _, rows, W = part.shape
    depth = wo_ref.shape[0]
    greet_along(has, toward)
    for peer in peers:
        greet(peer)
    load_own = pltpu.make_async_copy(wo_ref, w4.at[0], local.at[0])
    load_plane = pltpu.make_async_copy(plane_ref, w4.at[pl.ds(1, 3)], local.at[1])
    load_own.start()
    load_plane.start()
    for i, (bb, cc) in enumerate(((b, 1 - c), (1 - b, c), (1 - b, 1 - c))):
        for k in range(A):
            c_send[i, k] = context_ref[index_of(k, bb, cc)]
    for k in range(A):
        c_recv[0, k] = context_ref[index_of(k, b, c)]
    await_greetings(has, 3)
    swaps = [remote(c_send.at[i], c_recv.at[i + 1], cs.at[i], cr.at[i], peers[i]) for i in range(3)]
    for i in (2, 1, 0):
        swaps[i].start()
    load_own.wait()
    load_plane.wait()
    for swap in swaps:
        swap.wait_recv()
    low = lax.broadcasted_iota(jnp.int32, (A * rows, PAD), 1) < DH

    def beside(i):
        first = c_recv[i].reshape(A * rows, PAD).astype(jnp.float32)
        second = c_recv[i + 1].reshape(A * rows, PAD).astype(jnp.float32)
        return jnp.where(low, pltpu.roll(first, DH, 1), second).astype(jnp.bfloat16)

    left = jnp.concatenate([beside(0), beside(2)], axis=1)

    def z_copy(k, p, d):
        return remote(zsend.at[p, k], landing[d].at[p, k], zs.at[k, p], zr.at[(0 if d == 1 else A) + k, p], toward[d])

    def z_arrival(k, p, d):
        return remote(zsend.at[p, k], landing[d].at[p, k], zs.at[k, p], zr.at[(0 if d == 1 else A) + k, p], toward[-d])

    for s in range(A - 1, -1, -1):
        for p in range(P):
            if s == A - 1:
                w = w4[:, :, p * W : (p + 1) * W].reshape(4 * depth, W)
                found = jnp.dot(left, w, preferred_element_type=jnp.float32)
                part[p] = found.reshape(A, rows, W)
            for d in (1, -1) if s else (1,):
                k = a + s * d

                @pl.when((k >= 0) & (k < A))
                def _():
                    for came in (d,) if s else (1, -1):

                        @pl.when(has[-came])
                        def _():
                            z_arrival(k, p, came).wait_recv()
                            part[p, k] = part[p, k] + landing[came][p, k].astype(jnp.float32)

                    if s:
                        zsend[p, k] = part[p, k].astype(jnp.bfloat16)
                        z_copy(k, p, d).start()
                    else:
                        at = slice(p * W, (p + 1) * W)
                        out_ref[:, at] = (hidden_ref[:, at].astype(jnp.float32) + part[p, k]).astype(jnp.bfloat16)

    for s in range(A - 1, 0, -1):
        for d in (1, -1):
            k = a + s * d

            @pl.when((k >= 0) & (k < A))
            def _():
                for p in range(P):
                    z_copy(k, p, d).wait_send()

    for swap in swaps:
        swap.wait_send()


def project(context, hidden, w_out, plane, n, number):
    A = n // 4
    rows, width = hidden.shape
    P = pieces_of(n, width)
    W = width // P
    half = jnp.bfloat16
    return pl.pallas_call(
        functools.partial(project_kernel, n),
        out_shape=jax.ShapeDtypeStruct((rows, width), half),
        in_specs=[pl.BlockSpec(memory_space=m) for m in (VM, VM, pl.ANY, pl.ANY)],
        out_specs=pl.BlockSpec(memory_space=VM),
        scratch_shapes=[
            VM((4,) + w_out.shape, half),
            VM((3, A, rows, PAD), half),
            VM((4, A, rows, PAD), half),
            VM((P, A, rows, W), jnp.float32),
        ]
        + [VM((P, A, rows, W), half)] * 3
        + [DMA((2,)), DMA((3,)), DMA((3,)), DMA((A, P)), DMA((2 * A, P))],
        compiler_params=params(number),
        name=f"project_{number}",
    )(context, hidden, w_out, plane)


def attend_kernel(
    n, lengths_ref, q_ref, kv_ref, cached_ref, out_ref,
    q_all, q_cached, kv, cached, scores, chances, o_send, o_recv, stats, st_send, st_recv,
    local, qzs, qzr, qys, qyr, qcs, qcr, os, orr, ss, sr,
):
    A = n // 4
    me, a, b, c = place(n)
    across, pair = index_of(a, 1 - b, c), index_of(a, b, 1 - c)
    requests, positions, width = kv.shape
    pairs, heads = requests // 2, width // PAD
    rows = q_ref.shape[1]
    length = cached.shape[1]
    load_cached = pltpu.make_async_copy(cached_ref, cached, local.at[0])
    load_kv = pltpu.make_async_copy(kv_ref, kv, local.at[1])
    load_cached.start()
    load_kv.start()
    order = sorted(range(1, n), key=lambda s: -min(s, n - s))
    others = [lax.rem(me + s, n) for s in order]
    for other in others:
        greet(other)
    columns = [lax.rem(a + s, A) for s in range(1, A)]
    entering, flying = pl.ds(0, A), pl.ds(A, A)
    q_all[a, c, b] = q_ref[:A]
    q_cached[b] = q_ref[A:]
    stats[...] = jnp.zeros_like(stats)
    pl.semaphore_wait(pltpu.get_barrier_semaphore(), n - 1)

    def qz_copy(to, k):
        return remote(q_ref.at[entering], q_all.at[k, c, b], qzs.at[to], qzr.at[k], index_of(to, b, c))

    def qy_copy(k, bb, src=None):
        spot = q_all.at[k, c, bb]
        return remote(spot if src is None else src, spot, qys.at[k], qyr.at[k], across)

    def qc_copy(k, bb, cc, src=None):
        spot = q_all.at[k, cc, bb]
        return remote(spot if src is None else src, spot, qcs.at[bb * A + k], qcr.at[bb * A + k], pair)

    def cached_copy(bb):
        return remote(q_ref.at[flying], q_cached.at[bb], qys.at[A], qyr.at[A], across)

    def o_copy(other, spot, step):
        at = pl.ds(pl.multiple_of(step * QLEN, QLEN), QLEN)
        return remote(
            o_send.at[other, at], o_recv.at[spot, at], os.at[step, other], orr.at[step, spot], other
        )

    def st_copy(other, spot):
        return remote(st_send.at[other], st_recv.at[spot], ss.at[other], sr.at[spot], other)

    for k in columns:
        qz_copy(k, a).start()
    qy_copy(a, b, q_ref.at[entering]).start()
    cached_copy(b).start()
    qc_copy(a, b, c, q_ref.at[entering]).start()
    lane = lax.broadcasted_iota(jnp.int32, (QLEN, PAD), 1)
    low = lane < DH

    def request_of(r, block):
        per = QLEN // rows
        parts = []
        for i in range(per):
            spot = r * per + i
            parts.append(block((spot // 2) % 2, (spot // 4) * 2 + spot % 2))
        return parts[0] if per == 1 else jnp.concatenate(parts, axis=0)

    def cached_request(r):
        to = pl.ds(pl.multiple_of((requests + r) * QLEN, QLEN), QLEN)
        block = cached[r]
        query = request_of(r, lambda bb, spot: q_cached[bb, spot]).astype(jnp.float32)
        query = jnp.where(b == 0, query, pltpu.roll(query, DH, 1))
        found = lax.dot_general(
            jnp.where(low, query, 0.0).astype(jnp.bfloat16), block, (((1,), (1,)), ((), ())),
            preferred_element_type=jnp.float32,
        )
        usable = lax.broadcasted_iota(jnp.int32, (1, length), 1) < lengths_ref[1, r]
        masked = jnp.where(usable, found, -1e30)
        exponent = jnp.exp(masked - jnp.max(masked, axis=-1, keepdims=True))
        inverse = 1.0 / jnp.sum(exponent, axis=-1, keepdims=True)
        weights = (exponent * inverse).astype(jnp.bfloat16)
        out_ref[to, :] = jnp.dot(weights, block, preferred_element_type=jnp.float32).astype(jnp.bfloat16)

    def cached_requests(start, stop):
        def two(i, carry):
            cached_request(start + 2 * i)
            cached_request(start + 2 * i + 1)
            return carry

        lax.fori_loop(0, (stop - start) // 2, two, 0)
        if (stop - start) % 2:
            cached_request(stop - 1)

    for k in columns:
        qz_copy(k, k).wait_recv()
        qy_copy(k, b).start()
        qc_copy(k, b, c).start()
    cached_copy(1 - b).wait_recv()
    load_cached.wait()
    first, second = requests // 4, requests // 2
    cached_requests(0, first)
    qy_copy(a, 1 - b).wait_recv()
    qc_copy(a, 1 - b, c).start()
    for k in columns:
        qy_copy(k, 1 - b).wait_recv()
        qc_copy(k, 1 - b, c).start()
    cached_requests(first, second)
    load_kv.wait()
    for k in range(A):
        for bb in range(2):
            qc_copy(k, bb, 1 - c).wait_recv()
    at_position = me * positions + lax.broadcasted_iota(jnp.int32, (1, positions), 1)

    def pair_step(step, carry):
        at = pl.ds(pl.multiple_of(step * QLEN, QLEN), QLEN)
        nothing = jnp.zeros((QLEN, PAD), jnp.bfloat16)
        for i in range(2):
            for g in range(heads // 2):
                two = []
                for cc in range(2):
                    packed = request_of(
                        step * 2 + i, lambda bb, spot: q_all[g // 2, cc, bb, spot]
                    ).astype(jnp.float32)
                    packed = packed if g % 2 == 0 else pltpu.roll(packed, DH, 1)
                    two.append(jnp.where(low, packed, 0.0).astype(jnp.bfloat16))
                spread = jnp.concatenate(
                    [
                        jnp.concatenate([two[0], nothing], axis=1),
                        jnp.concatenate([nothing, two[1]], axis=1),
                    ],
                    axis=0,
                )
                scores[i, g] = lax.dot_general(
                    spread, kv[step * 2 + i, :, g * 2 * PAD : (g + 1) * 2 * PAD], (((1,), (1,)), ((), ())),
                    preferred_element_type=jnp.float32,
                )
        for i in range(2):
            r = step * 2 + i
            masked = jnp.where(at_position < lengths_ref[0, r], scores[i], -1e30)
            largest = jnp.max(masked, axis=-1, keepdims=True)
            exponent = jnp.exp(masked - largest)
            total = jnp.sum(exponent, axis=-1, keepdims=True)
            chances[i] = exponent.astype(jnp.bfloat16)
            stats[...] = jnp.where(
                lane == r,
                largest.reshape(heads, QLEN, 1),
                jnp.where(lane == r + requests, total.reshape(heads, QLEN, 1), stats[...]),
            )
        for g in range(heads // 2):
            found = [
                jnp.dot(
                    chances[i, g], kv[step * 2 + i, :, g * 2 * PAD : (g + 1) * 2 * PAD],
                    preferred_element_type=jnp.float32,
                )
                for i in range(2)
            ]
            for e in range(2):
                even, odd = (f[e * QLEN : (e + 1) * QLEN, e * PAD : (e + 1) * PAD] for f in found)
                o_send[2 * g + e, at, :] = jnp.where(low, pltpu.roll(odd, DH, 1), even).astype(jnp.bfloat16)
        for other in others:
            o_copy(other, me, step).start()
        return carry

    lax.fori_loop(0, pairs, pair_step, 0)
    parts = QLEN // 8
    gap = PAD // parts
    folded = stats[:, :8, :].reshape(heads * 8, PAD)
    for g in range(1, parts):
        folded = folded + pltpu.roll(stats[:, 8 * g : 8 * g + 8, :].reshape(heads * 8, PAD), g * gap, 1)
    st_send[...] = folded.reshape(heads, 8, PAD)
    for other in others:
        st_copy(other, me).start()
    o_recv[me] = o_send[me]
    st_recv[me] = st_send[me]
    cached_requests(second, requests)
    for other in others:
        st_copy(other, other).wait_recv()
    largest = st_recv[...]
    scale = jnp.exp(largest - jnp.max(largest, axis=0, keepdims=True))
    total = jnp.sum(
        scale * pltpu.roll(largest.reshape(n * 8, PAD), PAD - requests, 1).reshape(n, 8, PAD), axis=0, keepdims=True
    )
    st_recv[...] = scale / jnp.where(total > 0.0, total, 1.0)
    short = low[:8]
    for step in range(pairs):
        for other in others:
            o_copy(other, other, step).wait_recv()
        mixed = jnp.zeros((QLEN, PAD), jnp.float32)
        for d in range(n):
            known = st_recv[d]
            share = []
            for g in range(parts):
                lone = g * gap + 2 * step
                share.append(jnp.where(short, known[:, lone + 1 : lone + 2], known[:, lone : lone + 1]))
            share = jnp.concatenate(share, axis=0)
            mixed = mixed + share * o_recv[d, step * QLEN : (step + 1) * QLEN, :].astype(jnp.float32)
        out_ref[2 * step * QLEN : (2 * step + 1) * QLEN, :] = mixed.astype(jnp.bfloat16)
        out_ref[(2 * step + 1) * QLEN : (2 * step + 2) * QLEN, :] = pltpu.roll(mixed, DH, 1).astype(jnp.bfloat16)
    for k in columns:
        qz_copy(k, a).wait_send()
    cached_copy(b).wait_send()
    for k in range(A):
        qy_copy(k, b).wait_send()
        for bb in range(2):
            qc_copy(k, bb, c).wait_send()
    for other in others:
        st_copy(other, me).wait_send()
        for step in range(pairs):
            o_copy(other, me, step).wait_send()


def attend(query, entering_kv, cached_kv, lengths, n, number):
    A = n // 4
    requests, positions, width = entering_kv.shape
    pairs, heads = requests // 2, width // PAD
    rows = query.shape[1]
    assert heads == n and QLEN % rows == 0 and 8 * requests <= PAD
    half, full = jnp.bfloat16, jnp.float32
    return pl.pallas_call(
        functools.partial(attend_kernel, n),
        out_shape=jax.ShapeDtypeStruct((2 * requests * QLEN, PAD), half),
        in_specs=[pl.BlockSpec(memory_space=m) for m in (pltpu.SMEM, VM, pl.ANY, pl.ANY)],
        out_specs=pl.BlockSpec(memory_space=VM),
        scratch_shapes=[
            VM((A, 2, 2, A, rows, PAD), half),
            VM((2, A, rows, PAD), half),
            VM(entering_kv.shape, half),
            VM(cached_kv.shape, half),
            VM((2, heads // 2, 2 * QLEN, positions), full),
            VM((2, heads // 2, 2 * QLEN, positions), half),
            VM((n, pairs * QLEN, PAD), half),
            VM((n, pairs * QLEN, PAD), half),
            VM((n, QLEN, PAD), full),
            VM((n, 8, PAD), full),
            VM((n, 8, PAD), full),
            DMA((2,)), DMA((A,)), DMA((A,)), DMA((A + 1,)), DMA((A + 1,)), DMA((2 * A,)), DMA((2 * A,)),
            DMA((pairs, n)), DMA((pairs, n)), DMA((n,)), DMA((n,)),
        ],
        compiler_params=params(number),
        name=f"attend_{number}",
    )(lengths, query, entering_kv, cached_kv)


def far_first(A, a):
    low, high = 0, A - 1
    found = []
    for _ in range(A):
        left = (a - low > high - a).astype(jnp.int32)
        found.append(high + left * (low - high))
        low, high = low + left, high - 1 + left
    return found


def feed_kernel(
    n, x_ref, gain_ref, gate_ref, up_ref, down_ref, out_ref,
    xs, w_gate, w_up, w_down, gates, ups, act, part, cbuf, ysend, yrecv, zsend, zland,
    local, zs, zr, ys, yr, cs, cr, gs, gr, hs, hr, ts, tr,
):
    A = n // 4
    me, a, b, c = place(n)
    across, pair = index_of(a, 1 - b, c), index_of(a, b, 1 - c)
    has, toward = neighbours(n)
    P, W = xs.shape[0], xs.shape[-1]
    rows = x_ref.shape[0]
    greet_along(has, toward)
    greet(across)
    greet(pair)
    loads = [
        pltpu.make_async_copy(src, dst, local.at[i])
        for i, (src, dst) in enumerate(((gate_ref, w_gate), (up_ref, w_up), (down_ref, w_down)))
    ]
    for load in loads:
        load.start()
    values = x_ref[...].astype(jnp.float32)
    scale = lax.rsqrt(jnp.mean(values * values, axis=-1, keepdims=True) + epsilon)
    for p in range(P):
        at = slice(p * W, (p + 1) * W)
        xs[p, b, c, a] = (values[:, at] * scale * gain_ref[:, at]).astype(jnp.bfloat16)
    await_greetings(has, 2)

    def z_copy(k, p, s, d):
        block = xs.at[p, b, c, k]
        return remote(block, block, zs.at[(0 if d == 1 else A) + s, p], zr.at[k, p], toward[d])

    def y_copy(k, p, bb):
        block = xs.at[p, bb, c, k]
        return remote(block, block, ys.at[k, p], yr.at[k, p], across)

    def c_copy(k, p, bb, cc):
        block = xs.at[p, bb, cc, k]
        return remote(block, block, cs.at[bb * A + k, p], cr.at[bb * A + k, p], pair)

    for p in range(P):
        for d in (1, -1):

            @pl.when(has[d])
            def _():
                z_copy(a, p, 0, d).start()

        y_copy(a, p, b).start()
    for p in range(P):
        c_copy(a, p, b, c).start()

    def pass_on(s, p):
        for d in (1, -1) if s else (1,):
            k = a - s * d

            @pl.when((k >= 0) & (k < A))
            def _():
                y_copy(k, p, 1 - b).wait_recv()
                c_copy(k, p, 1 - b, c).start()

    for s in range(1, A):
        for p in range(P):
            for d in (1, -1):
                k = a - s * d

                @pl.when((k >= 0) & (k < A))
                def _():
                    block = xs.at[p, b, c, k]
                    remote(block, block, zs.at[0, p], zr.at[k, p], toward[-d]).wait_recv()

                    @pl.when(has[d])
                    def _():
                        z_copy(k, p, s, d).start()

                    y_copy(k, p, b).start()
                    c_copy(k, p, b, c).start()

            if s > 1:
                pass_on(s - 2, p)
    for p in range(P):
        pass_on(A - 2, p)
    for load in loads:
        load.wait()

    def contract(p):
        for bb in range(2):
            for k in range(A):
                c_copy(k, p, bb, 1 - c).wait_recv()
        left = xs[p].reshape(n * rows, W)
        for w, sums in ((w_gate, gates), (w_up, ups)):
            found = jnp.dot(left, w[p * W : (p + 1) * W, :], preferred_element_type=jnp.float32)
            sums[...] = found if p == 0 else sums[...] + found

    for p in range(P):
        pass_on(A - 1, p)
        if p:
            contract(p - 1)
    contract(P - 1)
    for p in range(P):
        for s in range(A):
            for d in (1, -1):
                k = a - s * d

                @pl.when((k >= 0) & (k < A) & has[d])
                def _():
                    z_copy(k, p, s, d).wait_send()

        for k in range(A):
            y_copy(k, p, b).wait_send()
            for bb in range(2):
                c_copy(k, p, bb, c).wait_send()

    tall = A * rows
    for group in range(4):
        at = slice(group * tall, (group + 1) * tall)
        act[group] = (jax.nn.gelu(gates[at, :], approximate=True) * ups[at, :]).astype(jnp.bfloat16)

    def multiply(i, p, bb, cc):
        found = jnp.dot(act[2 * bb + cc], w_down[:, p * W : (p + 1) * W], preferred_element_type=jnp.float32)
        part[i, p] = found.reshape(A, rows, W)

    def g_copy(side, p):
        return remote(part.at[2 * side, p], cbuf.at[side, p], gs.at[side, p], gr.at[side, p], pair)

    def h_copy(k, p):
        return remote(ysend.at[p, k], yrecv.at[p, k], hs.at[k, p], hr.at[k, p], across)

    def t_copy(k, p, right):
        return remote(
            zsend.at[p, k], zland.at[right, p, k], ts.at[k, p], tr.at[right, k, p], me + 8 * right - 4
        )

    def t_arrival(k, p, right):
        return remote(
            zsend.at[p, k], zland.at[right, p, k], ts.at[k, p], tr.at[right, k, p], me - 8 * right + 4
        )

    order = far_first(A, a)
    for t, k in enumerate(order):
        for p in range(P):
            if t == 0:
                if p == 0:
                    multiply(0, p, 1 - b, 1 - c)
                    g_copy(0, p).start()
                    multiply(1, p, 1 - b, c)
                if p + 1 < P:
                    multiply(0, p + 1, 1 - b, 1 - c)
                    g_copy(0, p + 1).start()
                g_copy(0, p).wait_recv()
            ysend[p, k] = (part[1, p, k] + cbuf[0, p, k]).astype(jnp.bfloat16)
            h_copy(k, p).start()
            if t == 0 and p + 1 < P:
                multiply(1, p + 1, 1 - b, c)
    for p in range(P):
        multiply(2, p, b, 1 - c)
        g_copy(1, p).start()
    for p in range(P):
        multiply(3, p, b, c)
    for t, k in enumerate(order):
        right = (k > a).astype(jnp.int32)
        for p in range(P):
            if t == 0:
                g_copy(1, p).wait_recv()
            h_copy(k, p).wait_recv()
            part[3, p, k] = part[3, p, k] + cbuf[1, p, k] + yrecv[p, k].astype(jnp.float32)
            if t < A - 1:
                comes = ((right == 1) & (a > 0)) | ((right == 0) & (a < A - 1))

                @pl.when(comes)
                def _():
                    t_arrival(k, p, right).wait_recv()
                    part[3, p, k] = part[3, p, k] + zland[right, p, k].astype(jnp.float32)

                zsend[p, k] = part[3, p, k].astype(jnp.bfloat16)
                t_copy(k, p, right).start()
            else:
                for came in (1, -1):

                    @pl.when(has[-came])
                    def _():
                        side = (came + 1) // 2
                        t_arrival(k, p, side).wait_recv()
                        part[3, p, k] = part[3, p, k] + zland[side, p, k].astype(jnp.float32)

                at = slice(p * W, (p + 1) * W)
                out_ref[:, at] = (x_ref[:, at].astype(jnp.float32) + part[3, p, k]).astype(jnp.bfloat16)

    for t, k in enumerate(order):
        right = (k > a).astype(jnp.int32)
        for p in range(P):
            h_copy(k, p).wait_send()
            if t < A - 1:
                t_copy(k, p, right).wait_send()
    for p in range(P):
        g_copy(0, p).wait_send()
        g_copy(1, p).wait_send()


def feed(residual, gain, w_gate, w_up, w_down, n, number):
    A = n // 4
    rows, width = residual.shape
    hidden_units = w_gate.shape[1]
    P = pieces_of(n, width)
    W = width // P
    half, full = jnp.bfloat16, jnp.float32
    return pl.pallas_call(
        functools.partial(feed_kernel, n),
        out_shape=jax.ShapeDtypeStruct((rows, width), half),
        in_specs=[pl.BlockSpec(memory_space=m) for m in (VM, VM, pl.ANY, pl.ANY, pl.ANY)],
        out_specs=pl.BlockSpec(memory_space=VM),
        scratch_shapes=[
            VM((P, 2, 2, A, rows, W), half),
            VM(w_gate.shape, half),
            VM(w_up.shape, half),
            VM(w_down.shape, half),
            VM((n * rows, hidden_units), full),
            VM((n * rows, hidden_units), full),
            VM((4, A * rows, hidden_units), half),
            VM((4, P, A, rows, W), full),
            VM((2, P, A, rows, W), full),
        ]
        + [VM((P, A, rows, W), half)] * 3
        + [VM((2, P, A, rows, W), half)]
        + [
            DMA((3,)), DMA((2 * A, P)), DMA((A, P)), DMA((A, P)), DMA((A, P)), DMA((2 * A, P)), DMA((2 * A, P)),
            DMA((2, P)), DMA((2, P)), DMA((A, P)), DMA((A, P)), DMA((A, P)), DMA((2, A, P)),
        ],
        compiler_params=params(number),
        name=f"feed_{number}",
    )(residual, gain[None, :], w_gate, w_up, w_down)


def per_device(
    n,
    groups,
    hidden,
    norm_gain_attn,
    w_query,
    entering_kv,
    cached_kv,
    enc_lengths,
    w_out,
    norm_gain_ffn,
    w_gate,
    w_up,
    w_down,
):
    rows, width = hidden.shape
    query, plane = make_query(hidden, norm_gain_attn, w_query, w_out, n, groups, 0)
    context = attend(query, entering_kv, cached_kv, enc_lengths, n, 1)
    residual = project(context.reshape(n, rows, PAD), hidden, w_out, plane, n, 3)
    return feed(residual, norm_gain_ffn, w_gate, w_up, w_down, n, 4)


def solution(mesh):
    placed = (
        P(("groups", "mp"), None),
        P(),
        P(None, "mp"),
        P("groups", "mp", None),
        P("groups", None, "mp"),
        P(None, "groups"),
        P("mp", None),
        P(),
        P(None, "mp"),
        P(None, "mp"),
        P("mp", None),
    )
    return jax.shard_map(
        functools.partial(per_device, mesh.shape["mp"], mesh.shape["groups"]),
        mesh=mesh,
        in_specs=placed,
        out_specs=P(("groups", "mp"), None),
        check_vma=False,
    )
```

```python
import functools

import jax
import jax.numpy as jnp
from jax import lax
from jax.experimental import pallas as pl
from jax.experimental.pallas import tpu as pltpu
from jax.sharding import PartitionSpec as P

DH = 64
QLEN = 32
PAD = 2 * DH
MESH = pl.DeviceIdType.MESH
VM = pltpu.VMEM
DMA = pltpu.SemaphoreType.DMA

epsilon = 0.1


def place(n):
    me = lax.axis_index("mp")
    return me, me // 4, (me // 2) % 2, me % 2


def index_of(a, b, c):
    return (a * 2 + b) * 2 + c


def remote(src, dst, send, recv, to):
    return pltpu.make_async_remote_copy(
        src_ref=src, dst_ref=dst, send_sem=send, recv_sem=recv, device_id={"mp": to}, device_id_type=MESH
    )


def greet(to):
    pl.semaphore_signal(pltpu.get_barrier_semaphore(), inc=1, device_id={"mp": to}, device_id_type=MESH)


def pieces_of(n, width):
    return max(1, min(4, 16 // (n // 4), width // 128))


def neighbours(n):
    A = n // 4
    me, a, b, c = place(n)
    has = {1: a < A - 1, -1: a > 0}
    toward = {1: me + 4, -1: me - 4}
    return has, toward


def query_phase(
    n, groups, x_ref, gain_ref, wq_ref, wo_ref, q_ref, w4, xs, w2, local, zs, zr, cs, cr, ys, yr, gs, gr, ps, pr
):
    A = n // 4
    me, a, b, c = place(n)
    mine = lax.axis_index("groups")
    across, pair = index_of(a, 1 - b, c), index_of(a, b, 1 - c)
    has, toward = neighbours(n)
    P, W = xs.shape[0], xs.shape[-1]
    rows = x_ref.shape[0]
    share = DH // groups
    twins = [lax.rem(mine + i, groups) for i in range(1, groups)]
    for other in range(1, n):
        greet(lax.rem(me + other, n))
    for twin in twins:
        pl.semaphore_signal(
            pltpu.get_barrier_semaphore(), inc=1, device_id={"groups": twin, "mp": me}, device_id_type=MESH
        )
    load_w = pltpu.make_async_copy(wq_ref, w2.at[b], local.at[0])
    load_w.start()
    load_own = pltpu.make_async_copy(wo_ref, w4.at[0], local.at[1])
    load_own.start()
    values = x_ref[...].astype(jnp.float32)
    scale = lax.rsqrt(jnp.mean(values * values, axis=-1, keepdims=True) + epsilon)
    for p in range(P):
        part = slice(p * W, (p + 1) * W)
        xs[p, a, c] = (values[:, part] * scale * gain_ref[:, part]).astype(jnp.bfloat16)
    pl.semaphore_wait(pltpu.get_barrier_semaphore(), n + groups - 2)

    def z_copy(k, p, s, d):
        row = 0 if d == 1 else A
        return remote(xs.at[p, k, c], xs.at[p, k, c], zs.at[row + s, p], zr.at[k, p], toward[d])

    def c_copy(k, p, cc):
        return remote(xs.at[p, k, cc], xs.at[p, k, cc], cs.at[k, p], cr.at[k, p], pair)

    def strip(part):
        return pl.ds(pl.multiple_of(part * share, share), share)

    def landing(which, bb, part):
        return w2.at[bb, strip(part)] if which == 0 else w4.at[2, strip(part)]

    def y_copy(which):
        source = (wq_ref, wo_ref)[which].at[strip(mine)]
        return remote(source, landing(which, b, mine), ys.at[which], yr.at[which], across)

    def y_arrival(which):
        spot = landing(which, 1 - b, mine)
        return remote(spot, spot, ys.at[which], yr.at[which], across)

    def g_copy(which, part, to):
        spot = landing(which, 1 - b, part)
        return pltpu.make_async_remote_copy(
            src_ref=spot, dst_ref=spot, send_sem=gs.at[which, to], recv_sem=gr.at[which, part],
            device_id={"groups": to, "mp": me}, device_id_type=MESH,
        )

    plane_pair = remote(wo_ref, w4.at[1], ps.at[0], pr.at[0], pair)
    plane_diagonal = remote(w4.at[2], w4.at[3], ps.at[1], pr.at[1], pair)
    for p in range(P):
        for d in (1, -1):

            @pl.when(has[d])
            def _():
                z_copy(a, p, 0, d).start()

    for which in range(2):
        y_copy(which).start()
    for p in range(P):
        c_copy(a, p, c).start()
    plane_pair.start()
    for s in range(1, A):
        for p in range(P):
            for d in (1, -1):
                k = a - s * d

                @pl.when((k >= 0) & (k < A))
                def _():
                    remote(xs.at[p, k, c], xs.at[p, k, c], zs.at[0, p], zr.at[k, p], toward[-d]).wait_recv()

                    @pl.when(has[d])
                    def _():
                        z_copy(k, p, s, d).start()

                    c_copy(k, p, c).start()

        if s < 3:
            y_arrival(s - 1).wait_recv()
            for twin in twins:
                g_copy(s - 1, mine, twin).start()
    for twin in twins:
        g_copy(0, twin, mine).wait_recv()
    load_w.wait()
    total = jnp.zeros((2 * A * rows, PAD), jnp.float32)
    for p in range(P):
        for k in range(A):
            c_copy(k, p, 1 - c).wait_recv()
        total = total + lax.dot_general(
            xs[p].reshape(2 * A * rows, W), w2[:, :, p * W : (p + 1) * W].reshape(PAD, W),
            (((1,), (1,)), ((), ())), preferred_element_type=jnp.float32,
        )
    q_ref[...] = total.astype(jnp.bfloat16).reshape(2 * A, rows, PAD)

    def share_diagonal():
        for twin in twins:
            g_copy(1, twin, mine).wait_recv()
        plane_diagonal.start()

    def share_arrived():
        load_own.wait()
        plane_pair.wait_recv()
        plane_diagonal.wait_recv()

    def finish():
        for s in range(A):
            for d in (1, -1):
                k = a - s * d

                @pl.when((k >= 0) & (k < A) & has[d])
                def _():
                    for p in range(P):
                        z_copy(k, p, s, d).wait_send()

        for k in range(A):
            for p in range(P):
                c_copy(k, p, c).wait_send()
        for which in range(2):
            y_copy(which).wait_send()
            for twin in twins:
                g_copy(which, mine, twin).wait_send()
        plane_pair.wait_send()
        plane_diagonal.wait_send()

    return share_diagonal, share_arrived, finish


def attend_phase(
    n, between, lengths_ref, q_ref, kv_ref, cached_ref, context_ref,
    kv, cached, scores, chances, stats,
    q_all, q_cached, o_send, o_recv, st_send, st_recv,
    local, qzs, qzr, qys, qyr, qcs, qcr, os, orr, ss, sr,
):
    A = n // 4
    me, a, b, c = place(n)
    across, pair = index_of(a, 1 - b, c), index_of(a, b, 1 - c)
    requests, positions, width = kv.shape
    pairs, heads = requests // 2, width // PAD
    rows = q_ref.shape[1]
    length = cached.shape[1]
    load_cached = pltpu.make_async_copy(cached_ref, cached, local.at[0])
    load_kv = pltpu.make_async_copy(kv_ref, kv, local.at[1])
    load_cached.start()
    load_kv.start()
    order = sorted(range(1, n), key=lambda s: -min(s, n - s))
    others = [lax.rem(me + s, n) for s in order]
    columns = [lax.rem(a + s, A) for s in range(1, A)]
    entering, flying = pl.ds(0, A), pl.ds(A, A)
    q_all[a, c, b] = q_ref[:A]
    q_cached[b] = q_ref[A:]
    stats[...] = jnp.zeros_like(stats)

    def qz_copy(to, k):
        return remote(q_ref.at[entering], q_all.at[k, c, b], qzs.at[to], qzr.at[k], index_of(to, b, c))

    def qy_copy(k, bb, src=None):
        spot = q_all.at[k, c, bb]
        return remote(spot if src is None else src, spot, qys.at[k], qyr.at[k], across)

    def qc_copy(k, bb, cc, src=None):
        spot = q_all.at[k, cc, bb]
        return remote(spot if src is None else src, spot, qcs.at[bb * A + k], qcr.at[bb * A + k], pair)

    def cached_copy(bb):
        return remote(q_ref.at[flying], q_cached.at[bb], qys.at[A], qyr.at[A], across)

    def o_copy(other, spot, step):
        at = pl.ds(pl.multiple_of(step * QLEN, QLEN), QLEN)
        return remote(
            o_send.at[other, at], o_recv.at[spot, at], os.at[step, other], orr.at[step, spot], other
        )

    def st_copy(other, spot):
        return remote(st_send.at[other], st_recv.at[spot], ss.at[other], sr.at[spot], other)

    for k in columns:
        qz_copy(k, a).start()
    qy_copy(a, b, q_ref.at[entering]).start()
    cached_copy(b).start()
    qc_copy(a, b, c, q_ref.at[entering]).start()
    lane = lax.broadcasted_iota(jnp.int32, (QLEN, PAD), 1)
    low = lane < DH

    def request_of(r, block):
        per = QLEN // rows
        parts = []
        for i in range(per):
            spot = r * per + i
            parts.append(block((spot // 2) % 2, (spot // 4) * 2 + spot % 2))
        return parts[0] if per == 1 else jnp.concatenate(parts, axis=0)

    def put(r, value):
        per = QLEN // rows
        for i in range(per):
            context_ref[r * per + i] = value[i * rows : (i + 1) * rows].astype(jnp.bfloat16)

    def cached_request(r):
        block = cached[r]
        query = request_of(r, lambda bb, spot: q_cached[bb, spot]).astype(jnp.float32)
        query = jnp.where(b == 0, query, pltpu.roll(query, DH, 1))
        found = lax.dot_general(
            jnp.where(low, query, 0.0).astype(jnp.bfloat16), block, (((1,), (1,)), ((), ())),
            preferred_element_type=jnp.float32,
        )
        usable = lax.broadcasted_iota(jnp.int32, (1, length), 1) < lengths_ref[1, r]
        masked = jnp.where(usable, found, -1e30)
        exponent = jnp.exp(masked - jnp.max(masked, axis=-1, keepdims=True))
        inverse = 1.0 / jnp.sum(exponent, axis=-1, keepdims=True)
        weights = (exponent * inverse).astype(jnp.bfloat16)
        put(requests + r, jnp.dot(weights, block, preferred_element_type=jnp.float32))

    def cached_requests(start, stop):
        def two(i, carry):
            cached_request(start + 2 * i)
            cached_request(start + 2 * i + 1)
            return carry

        lax.fori_loop(0, (stop - start) // 2, two, 0)
        if (stop - start) % 2:
            cached_request(stop - 1)

    at_position = me * positions + lax.broadcasted_iota(jnp.int32, (1, positions), 1)

    def pair_step(step, carry):
        at = pl.ds(pl.multiple_of(step * QLEN, QLEN), QLEN)
        nothing = jnp.zeros((QLEN, PAD), jnp.bfloat16)
        for i in range(2):
            for g in range(heads // 2):
                two = []
                for cc in range(2):
                    packed = request_of(
                        step * 2 + i, lambda bb, spot: q_all[g // 2, cc, bb, spot]
                    ).astype(jnp.float32)
                    packed = packed if g % 2 == 0 else pltpu.roll(packed, DH, 1)
                    two.append(jnp.where(low, packed, 0.0).astype(jnp.bfloat16))
                spread = jnp.concatenate(
                    [
                        jnp.concatenate([two[0], nothing], axis=1),
                        jnp.concatenate([nothing, two[1]], axis=1),
                    ],
                    axis=0,
                )
                scores[i, g] = lax.dot_general(
                    spread, kv[step * 2 + i, :, g * 2 * PAD : (g + 1) * 2 * PAD], (((1,), (1,)), ((), ())),
                    preferred_element_type=jnp.float32,
                )
        for i in range(2):
            r = step * 2 + i
            masked = jnp.where(at_position < lengths_ref[0, r], scores[i], -1e30)
            largest = jnp.max(masked, axis=-1, keepdims=True)
            exponent = jnp.exp(masked - largest)
            total = jnp.sum(exponent, axis=-1, keepdims=True)
            chances[i] = exponent.astype(jnp.bfloat16)
            stats[...] = jnp.where(
                lane == r,
                largest.reshape(heads, QLEN, 1),
                jnp.where(lane == r + requests, total.reshape(heads, QLEN, 1), stats[...]),
            )
        for g in range(heads // 2):
            found = [
                jnp.dot(
                    chances[i, g], kv[step * 2 + i, :, g * 2 * PAD : (g + 1) * 2 * PAD],
                    preferred_element_type=jnp.float32,
                )
                for i in range(2)
            ]
            for e in range(2):
                even, odd = (f[e * QLEN : (e + 1) * QLEN, e * PAD : (e + 1) * PAD] for f in found)
                o_send[2 * g + e, at, :] = jnp.where(low, pltpu.roll(odd, DH, 1), even).astype(jnp.bfloat16)
        for other in others:
            o_copy(other, me, step).start()
        return carry

    def steps(column):
        def one(i, carry):
            return pair_step(2 * i + column, carry)

        lax.fori_loop(0, pairs // 2, one, 0)

    def second_column():
        qy_copy(a, 1 - b).wait_recv()
        qc_copy(a, 1 - b, c).start()
        for k in columns:
            qy_copy(k, 1 - b).wait_recv()
            qc_copy(k, 1 - b, c).start()

    def arrived(bb):
        for k in range(A):
            qc_copy(k, bb, 1 - c).wait_recv()

    for k in columns:
        qz_copy(k, k).wait_recv()
        qy_copy(k, b).start()
        qc_copy(k, b, c).start()
    between()
    cached_copy(1 - b).wait_recv()
    load_cached.wait()
    first, second = requests // 4, requests // 2
    cached_requests(0, first)
    load_kv.wait()
    if rows == QLEN:
        arrived(b)
        steps(b)
        second_column()
    else:
        second_column()
        arrived(b)
        arrived(1 - b)
        steps(b)
    cached_requests(first, second)
    if rows == QLEN:
        arrived(1 - b)
    steps(1 - b)
    parts = QLEN // 8
    gap = PAD // parts
    folded = stats[:, :8, :].reshape(heads * 8, PAD)
    for g in range(1, parts):
        folded = folded + pltpu.roll(stats[:, 8 * g : 8 * g + 8, :].reshape(heads * 8, PAD), g * gap, 1)
    st_send[...] = folded.reshape(heads, 8, PAD)
    for other in others:
        st_copy(other, me).start()
    o_recv[me] = o_send[me]
    st_recv[me] = st_send[me]
    cached_requests(second, requests)
    for other in others:
        st_copy(other, other).wait_recv()
    largest = st_recv[...]
    scale = jnp.exp(largest - jnp.max(largest, axis=0, keepdims=True))
    total = jnp.sum(
        scale * pltpu.roll(largest.reshape(n * 8, PAD), PAD - requests, 1).reshape(n, 8, PAD), axis=0, keepdims=True
    )
    st_recv[...] = scale / jnp.where(total > 0.0, total, 1.0)
    short = low[:8]
    for step in range(pairs):
        for other in others:
            o_copy(other, other, step).wait_recv()
        mixed = jnp.zeros((QLEN, PAD), jnp.float32)
        for d in range(n):
            known = st_recv[d]
            share = []
            for g in range(parts):
                lone = g * gap + 2 * step
                share.append(jnp.where(short, known[:, lone + 1 : lone + 2], known[:, lone : lone + 1]))
            share = jnp.concatenate(share, axis=0)
            mixed = mixed + share * o_recv[d, step * QLEN : (step + 1) * QLEN, :].astype(jnp.float32)
        put(2 * step, mixed)
        put(2 * step + 1, pltpu.roll(mixed, DH, 1))

    def finish():
        for k in columns:
            qz_copy(k, a).wait_send()
        cached_copy(b).wait_send()
        for k in range(A):
            qy_copy(k, b).wait_send()
            for bb in range(2):
                qc_copy(k, bb, c).wait_send()
        for other in others:
            st_copy(other, me).wait_send()
            for step in range(pairs):
                o_copy(other, me, step).wait_send()

    return finish


def project_phase(
    n, arrived, context_ref, hidden_ref, out_ref, w4, part, c_send, c_recv, zsend, zright, zleft, cs, cr, zs, zr
):
    A = n // 4
    me, a, b, c = place(n)
    peers = (index_of(a, b, 1 - c), index_of(a, 1 - b, c), index_of(a, 1 - b, 1 - c))
    has, toward = neighbours(n)
    landing = {1: zright, -1: zleft}
    P, _, rows, W = part.shape
    depth = w4.shape[1]
    for i, (bb, cc) in enumerate(((b, 1 - c), (1 - b, c), (1 - b, 1 - c))):
        for k in range(A):
            c_send[i, k] = context_ref[index_of(k, bb, cc)]
    for k in range(A):
        c_recv[0, k] = context_ref[index_of(k, b, c)]
    swaps = [remote(c_send.at[i], c_recv.at[i + 1], cs.at[i], cr.at[i], peers[i]) for i in range(3)]
    for i in (2, 1, 0):
        swaps[i].start()
    arrived()
    for swap in swaps:
        swap.wait_recv()
    low = lax.broadcasted_iota(jnp.int32, (A * rows, PAD), 1) < DH

    def beside(i):
        first = c_recv[i].reshape(A * rows, PAD).astype(jnp.float32)
        second = c_recv[i + 1].reshape(A * rows, PAD).astype(jnp.float32)
        return jnp.where(low, pltpu.roll(first, DH, 1), second).astype(jnp.bfloat16)

    left = jnp.concatenate([beside(0), beside(2)], axis=1)

    def z_copy(k, p, d):
        return remote(zsend.at[p, k], landing[d].at[p, k], zs.at[k, p], zr.at[(0 if d == 1 else A) + k, p], toward[d])

    def z_arrival(k, p, d):
        return remote(zsend.at[p, k], landing[d].at[p, k], zs.at[k, p], zr.at[(0 if d == 1 else A) + k, p], toward[-d])

    for s in range(A - 1, -1, -1):
        for p in range(P):
            if s == A - 1:
                w = w4[:, :, p * W : (p + 1) * W].reshape(4 * depth, W)
                found = jnp.dot(left, w, preferred_element_type=jnp.float32)
                part[p] = found.reshape(A, rows, W)
            for d in (1, -1) if s else (1,):
                k = a + s * d

                @pl.when((k >= 0) & (k < A))
                def _():
                    for came in (d,) if s else (1, -1):

                        @pl.when(has[-came])
                        def _():
                            z_arrival(k, p, came).wait_recv()
                            part[p, k] = part[p, k] + landing[came][p, k].astype(jnp.float32)

                    if s:
                        zsend[p, k] = part[p, k].astype(jnp.bfloat16)
                        z_copy(k, p, d).start()
                    else:
                        at = slice(p * W, (p + 1) * W)
                        out_ref[:, at] = (hidden_ref[:, at].astype(jnp.float32) + part[p, k]).astype(jnp.bfloat16)

    def finish():
        for s in range(A - 1, 0, -1):
            for d in (1, -1):
                k = a + s * d

                @pl.when((k >= 0) & (k < A))
                def _():
                    for p in range(P):
                        z_copy(k, p, d).wait_send()

        for swap in swaps:
            swap.wait_send()

    return finish


def far_first(A, a):
    low, high = 0, A - 1
    found = []
    for _ in range(A):
        left = (a - low > high - a).astype(jnp.int32)
        found.append(high + left * (low - high))
        low, high = low + left, high - 1 + left
    return found


def feed_phase(
    n, x_ref, gain_ref, gate_ref, up_ref, down_ref, out_ref,
    w_in, sums_in, w_down, act, part,
    xs, cbuf, ysend, yrecv, zsend, zland,
    local, zs, zr, ys, yr, cs, cr, gs, gr, hs, hr, ts, tr,
):
    A = n // 4
    me, a, b, c = place(n)
    across, pair = index_of(a, 1 - b, c), index_of(a, b, 1 - c)
    has, toward = neighbours(n)
    P, W = xs.shape[0], xs.shape[-1]
    rows = x_ref.shape[0]
    units = gate_ref.shape[1]
    split = [(w_in[0], slice(0, units)), (w_in[-1], slice(units, 2 * units) if len(w_in) == 1 else slice(0, units))]
    loads = [
        pltpu.make_async_copy(gate_ref, split[0][0].at[:, split[0][1]], local.at[0]),
        pltpu.make_async_copy(up_ref, split[1][0].at[:, split[1][1]], local.at[1]),
        pltpu.make_async_copy(down_ref, w_down, local.at[2]),
    ]
    for load in loads:
        load.start()
    values = x_ref[...].astype(jnp.float32)
    scale = lax.rsqrt(jnp.mean(values * values, axis=-1, keepdims=True) + epsilon)
    for p in range(P):
        at = slice(p * W, (p + 1) * W)
        xs[p, b, c, a] = (values[:, at] * scale * gain_ref[:, at]).astype(jnp.bfloat16)

    def z_copy(k, p, s, d):
        block = xs.at[p, b, c, k]
        return remote(block, block, zs.at[(0 if d == 1 else A) + s, p], zr.at[k, p], toward[d])

    def y_copy(k, p, bb):
        block = xs.at[p, bb, c, k]
        return remote(block, block, ys.at[k, p], yr.at[k, p], across)

    def c_copy(k, p, bb, cc):
        block = xs.at[p, bb, cc, k]
        return remote(block, block, cs.at[bb * A + k, p], cr.at[bb * A + k, p], pair)

    for p in range(P):
        for d in (1, -1):

            @pl.when(has[d])
            def _():
                z_copy(a, p, 0, d).start()

        y_copy(a, p, b).start()
    for p in range(P):
        c_copy(a, p, b, c).start()

    def pass_on(s, p):
        for d in (1, -1) if s else (1,):
            k = a - s * d

            @pl.when((k >= 0) & (k < A))
            def _():
                y_copy(k, p, 1 - b).wait_recv()
                c_copy(k, p, 1 - b, c).start()

    for s in range(1, A):
        for p in range(P):
            for d in (1, -1):
                k = a - s * d

                @pl.when((k >= 0) & (k < A))
                def _():
                    block = xs.at[p, b, c, k]
                    remote(block, block, zs.at[0, p], zr.at[k, p], toward[-d]).wait_recv()

                    @pl.when(has[d])
                    def _():
                        z_copy(k, p, s, d).start()

                    y_copy(k, p, b).start()
                    c_copy(k, p, b, c).start()

            if s > 1:
                pass_on(s - 2, p)
    for p in range(P):
        pass_on(A - 2, p)
    for load in loads:
        load.wait()

    def contract(p):
        for bb in range(2):
            for k in range(A):
                c_copy(k, p, bb, 1 - c).wait_recv()
        left = xs[p].reshape(n * rows, W)
        for w, sums in zip(w_in, sums_in):
            found = jnp.dot(left, w[p * W : (p + 1) * W, :], preferred_element_type=jnp.float32)
            sums[...] = found if p == 0 else sums[...] + found

    for p in range(P):
        pass_on(A - 1, p)
        if p:
            contract(p - 1)
    contract(P - 1)
    for p in range(P):
        for s in range(A):
            for d in (1, -1):
                k = a - s * d

                @pl.when((k >= 0) & (k < A) & has[d])
                def _():
                    z_copy(k, p, s, d).wait_send()

        for k in range(A):
            y_copy(k, p, b).wait_send()
            for bb in range(2):
                c_copy(k, p, bb, c).wait_send()

    tall = A * rows
    for group in range(4):
        at = slice(group * tall, (group + 1) * tall)
        gate, up = sums_in[0][at, split[0][1]], sums_in[-1][at, split[1][1]]
        act[group] = (jax.nn.gelu(gate, approximate=True) * up).astype(jnp.bfloat16)

    def multiply(i, p, bb, cc):
        found = jnp.dot(act[2 * bb + cc], w_down[:, p * W : (p + 1) * W], preferred_element_type=jnp.float32)
        part[i, p] = found.reshape(A, rows, W)

    def g_copy(side, p):
        return remote(part.at[2 * side, p], cbuf.at[side, p], gs.at[side, p], gr.at[side, p], pair)

    def h_copy(k, p):
        return remote(ysend.at[p, k], yrecv.at[p, k], hs.at[k, p], hr.at[k, p], across)

    def t_copy(k, p, right):
        return remote(
            zsend.at[p, k], zland.at[right, p, k], ts.at[k, p], tr.at[right, k, p], me + 8 * right - 4
        )

    def t_arrival(k, p, right):
        return remote(
            zsend.at[p, k], zland.at[right, p, k], ts.at[k, p], tr.at[right, k, p], me - 8 * right + 4
        )

    order = far_first(A, a)
    for t, k in enumerate(order):
        for p in range(P):
            if t == 0:
                if p == 0:
                    multiply(0, p, 1 - b, 1 - c)
                    g_copy(0, p).start()
                    multiply(1, p, 1 - b, c)
                if p + 1 < P:
                    multiply(0, p + 1, 1 - b, 1 - c)
                    g_copy(0, p + 1).start()
                g_copy(0, p).wait_recv()
            ysend[p, k] = (part[1, p, k] + cbuf[0, p, k]).astype(jnp.bfloat16)
            h_copy(k, p).start()
            if t == 0 and p + 1 < P:
                multiply(1, p + 1, 1 - b, c)
    for p in range(P):
        multiply(2, p, b, 1 - c)
        g_copy(1, p).start()
    for p in range(P):
        multiply(3, p, b, c)
    for t, k in enumerate(order):
        right = (k > a).astype(jnp.int32)
        for p in range(P):
            if t == 0:
                g_copy(1, p).wait_recv()
            h_copy(k, p).wait_recv()
            part[3, p, k] = part[3, p, k] + cbuf[1, p, k] + yrecv[p, k].astype(jnp.float32)
            if t < A - 1:
                comes = ((right == 1) & (a > 0)) | ((right == 0) & (a < A - 1))

                @pl.when(comes)
                def _():
                    t_arrival(k, p, right).wait_recv()
                    part[3, p, k] = part[3, p, k] + zland[right, p, k].astype(jnp.float32)

                zsend[p, k] = part[3, p, k].astype(jnp.bfloat16)
                t_copy(k, p, right).start()
            else:
                for came in (1, -1):

                    @pl.when(has[-came])
                    def _():
                        side = (came + 1) // 2
                        t_arrival(k, p, side).wait_recv()
                        part[3, p, k] = part[3, p, k] + zland[side, p, k].astype(jnp.float32)

                at = slice(p * W, (p + 1) * W)
                out_ref[:, at] = (x_ref[:, at].astype(jnp.float32) + part[3, p, k]).astype(jnp.bfloat16)

    for t, k in enumerate(order):
        right = (k > a).astype(jnp.int32)
        for p in range(P):
            h_copy(k, p).wait_send()
            if t < A - 1:
                t_copy(k, p, right).wait_send()
    for p in range(P):
        g_copy(0, p).wait_send()
        g_copy(1, p).wait_send()


def layer_kernel(n, groups, counts, *refs):
    ends = [sum(counts[: i + 1]) for i in range(len(counts))]
    inputs, (out_ref,), shared, ask, look, out, give = (
        refs[end - count : end] for end, count in zip(ends, counts)
    )
    hidden_ref, gain_ref, wq_ref, kv_ref, cached_ref, lengths_ref, wo_ref, ffn_gain, gate_ref, up_ref, down_ref = inputs
    q_ref, w4, context_ref, residual = shared
    half, full = jnp.bfloat16, jnp.float32
    rows, width = hidden_ref.shape
    requests, positions, across = kv_ref.shape
    heads, units = across // PAD, gate_ref.shape[1]
    P = pieces_of(n, width)
    A, W = n // 4, width // P
    diagonal, arrived, end_query = query_phase(
        n, groups, hidden_ref, gain_ref, wq_ref, wo_ref, q_ref, w4, *ask
    )

    def attending(*own):
        attend_phase(n, diagonal, lengths_ref, q_ref, kv_ref, cached_ref, context_ref, *own, *look)()

    pl.run_scoped(
        attending,
        VM(kv_ref.shape, half),
        VM(cached_ref.shape, half),
        VM((2, heads // 2, 2 * QLEN, positions), full),
        VM((2, heads // 2, 2 * QLEN, positions), half),
        VM((n, QLEN, PAD), full),
    )

    def projecting(part):
        project_phase(n, arrived, context_ref, hidden_ref, residual, w4, part, *out)()

    pl.run_scoped(projecting, VM((P, A, rows, W), full))
    joined = 1 if units % PAD == 0 else 2
    wide = 2 * units // joined

    def feeding(*own):
        feed_phase(
            n, residual, ffn_gain, gate_ref, up_ref, down_ref, out_ref,
            own[:joined], own[joined : 2 * joined], *own[2 * joined :], *give,
        )

    pl.run_scoped(
        feeding,
        *[VM((width, wide), half)] * joined,
        *[VM((n * rows, wide), full)] * joined,
        VM(down_ref.shape, half),
        VM((4, A * rows, units), half),
        VM((4, P, A, rows, W), full),
    )
    end_query()


def layer(n, groups, hidden, gain, w_query, entering_kv, cached_kv, lengths, w_out, ffn_gain, w_gate, w_up, w_down):
    A = n // 4
    rows, width = hidden.shape
    requests, positions, across = entering_kv.shape
    pairs, heads = requests // 2, across // PAD
    assert A > 2 and DH % groups == 0 and pairs % 2 == 0
    assert heads == n and QLEN % rows == 0 and 8 * requests <= PAD
    P = pieces_of(n, width)
    W = width // P
    half, full = jnp.bfloat16, jnp.float32
    piece = (P, A, rows, W)
    inputs = (
        hidden, gain[None, :], w_query.T, entering_kv, cached_kv, lengths, w_out, ffn_gain[None, :],
        w_gate, w_up, w_down,
    )
    spaces = (VM, VM, pl.ANY, pl.ANY, pl.ANY, pltpu.SMEM, pl.ANY, VM, pl.ANY, pl.ANY, pl.ANY)
    shared = [
        VM((2 * A, rows, PAD), half), VM((4,) + w_out.shape, half), VM((n, rows, PAD), half), VM((rows, width), half),
    ]
    ask = [
        VM((P, A, 2, rows, W), half), VM((2, DH, width), half),
        DMA((2,)), DMA((2 * A, P)), DMA((A, P)), DMA((A, P)), DMA((A, P)),
        DMA((2,)), DMA((2,)), DMA((2, groups)), DMA((2, groups)), DMA((2,)), DMA((2,)),
    ]
    look = [
        VM((A, 2, 2, A, rows, PAD), half), VM((2, A, rows, PAD), half),
        VM((n, pairs * QLEN, PAD), half), VM((n, pairs * QLEN, PAD), half),
        VM((n, 8, PAD), full), VM((n, 8, PAD), full),
        DMA((2,)), DMA((A,)), DMA((A,)), DMA((A + 1,)), DMA((A + 1,)), DMA((2 * A,)), DMA((2 * A,)),
        DMA((pairs, n)), DMA((pairs, n)), DMA((n,)), DMA((n,)),
    ]
    out = [VM((3, A, rows, PAD), half), VM((4, A, rows, PAD), half), VM(piece, half), VM(piece, half), VM(piece, half)]
    out += [DMA((3,)), DMA((3,)), DMA((A, P)), DMA((2 * A, P))]
    give = [
        VM((P, 2, 2, A, rows, W), half), VM((2,) + piece, full),
        VM(piece, half), VM(piece, half), VM(piece, half), VM((2,) + piece, half),
        DMA((3,)), DMA((2 * A, P)), DMA((A, P)), DMA((A, P)), DMA((A, P)), DMA((2 * A, P)), DMA((2 * A, P)),
        DMA((2, P)), DMA((2, P)), DMA((A, P)), DMA((A, P)), DMA((A, P)), DMA((2, A, P)),
    ]
    parts = (inputs, (None,), shared, ask, look, out, give)
    return pl.pallas_call(
        functools.partial(layer_kernel, n, groups, tuple(len(part) for part in parts)),
        out_shape=jax.ShapeDtypeStruct((rows, width), half),
        in_specs=[pl.BlockSpec(memory_space=m) for m in spaces],
        out_specs=pl.BlockSpec(memory_space=VM),
        scratch_shapes=shared + ask + look + out + give,
        compiler_params=pltpu.CompilerParams(
            collective_id=0, has_side_effects=True, vmem_limit_bytes=60 * 2**20
        ),
        name="layer",
    )(*inputs)


def solution(mesh):
    placed = (
        P(("groups", "mp"), None),
        P(),
        P(None, "mp"),
        P("groups", "mp", None),
        P("groups", None, "mp"),
        P(None, "groups"),
        P("mp", None),
        P(),
        P(None, "mp"),
        P(None, "mp"),
        P("mp", None),
    )
    return jax.shard_map(
        functools.partial(layer, mesh.shape["mp"], mesh.shape["groups"]),
        mesh=mesh,
        in_specs=placed,
        out_specs=P(("groups", "mp"), None),
        check_vma=False,
    )
```

```python
import functools

import jax
import jax.numpy as jnp
from jax import lax
from jax.experimental import pallas as pl
from jax.experimental.pallas import tpu as pltpu
from jax.sharding import PartitionSpec as P

DH = 64
QLEN = 32
PAD = 2 * DH
MESH = pl.DeviceIdType.MESH
VM = pltpu.VMEM
DMA = pltpu.SemaphoreType.DMA

epsilon = 0.1


def place(n):
    me = lax.axis_index("mp")
    return me, me // 4, (me // 2) % 2, me % 2


def index_of(a, b, c):
    return (a * 2 + b) * 2 + c


def remote(src, dst, send, recv, to):
    return pltpu.make_async_remote_copy(
        src_ref=src, dst_ref=dst, send_sem=send, recv_sem=recv, device_id={"mp": to}, device_id_type=MESH
    )


def greet(to):
    pl.semaphore_signal(pltpu.get_barrier_semaphore(), inc=1, device_id={"mp": to}, device_id_type=MESH)


def pieces_of(n, width):
    return max(1, min(4, 16 // (n // 4), width // 128))


def neighbours(n):
    A = n // 4
    me, a, b, c = place(n)
    has = {1: a < A - 1, -1: a > 0}
    toward = {1: me + 4, -1: me - 4}
    return has, toward


def query_phase(
    n, groups, x_ref, gain_ref, wq_ref, wo_ref, q_ref, w8, xs, w2, local, zs, zr, cs, cr, ys, yr, gs, gr, ps, pr, es, er
):
    A = n // 4
    me, a, b, c = place(n)
    mine = lax.axis_index("groups")
    across, pair = index_of(a, 1 - b, c), index_of(a, b, 1 - c)
    has, toward = neighbours(n)
    P, W = xs.shape[0], xs.shape[-1]
    rows = x_ref.shape[0]
    share = DH // groups
    twins = [lax.rem(mine + i, groups) for i in range(1, groups)]
    for other in range(1, n):
        greet(lax.rem(me + other, n))
    for twin in twins:
        pl.semaphore_signal(
            pltpu.get_barrier_semaphore(), inc=1, device_id={"groups": twin, "mp": me}, device_id_type=MESH
        )
    load_w = pltpu.make_async_copy(wq_ref, w2.at[b], local.at[0])
    load_w.start()
    load_own = pltpu.make_async_copy(wo_ref, w8.at[0], local.at[1])
    load_own.start()
    values = x_ref[...].astype(jnp.float32)
    scale = lax.rsqrt(jnp.mean(values * values, axis=-1, keepdims=True) + epsilon)
    for p in range(P):
        part = slice(p * W, (p + 1) * W)
        xs[p, a, c] = (values[:, part] * scale * gain_ref[:, part]).astype(jnp.bfloat16)
    pl.semaphore_wait(pltpu.get_barrier_semaphore(), n + groups - 2)

    def z_copy(k, p, s, d):
        row = 0 if d == 1 else A
        return remote(xs.at[p, k, c], xs.at[p, k, c], zs.at[row + s, p], zr.at[k, p], toward[d])

    def c_copy(k, p, cc):
        return remote(xs.at[p, k, cc], xs.at[p, k, cc], cs.at[k, p], cr.at[k, p], pair)

    def strip(part):
        return pl.ds(pl.multiple_of(part * share, share), share)

    def landing(which, bb, part):
        return w2.at[bb, strip(part)] if which == 0 else w8.at[2, strip(part)]

    def y_copy(which):
        source = (wq_ref, wo_ref)[which].at[strip(mine)]
        return remote(source, landing(which, b, mine), ys.at[which], yr.at[which], across)

    def y_arrival(which):
        spot = landing(which, 1 - b, mine)
        return remote(spot, spot, ys.at[which], yr.at[which], across)

    def g_copy(which, part, to):
        spot = landing(which, 1 - b, part)
        return pltpu.make_async_remote_copy(
            src_ref=spot, dst_ref=spot, send_sem=gs.at[which, to], recv_sem=gr.at[which, part],
            device_id={"groups": to, "mp": me}, device_id_type=MESH,
        )

    plane_pair = remote(wo_ref, w8.at[1], ps.at[0], pr.at[0], pair)
    plane_diagonal = remote(w8.at[2], w8.at[3], ps.at[1], pr.at[1], pair)
    for p in range(P):
        for d in (1, -1):

            @pl.when(has[d])
            def _():
                z_copy(a, p, 0, d).start()

    for which in range(2):
        y_copy(which).start()
    for p in range(P):
        c_copy(a, p, c).start()
    plane_pair.start()
    for s in range(1, A):
        for p in range(P):
            for d in (1, -1):
                k = a - s * d

                @pl.when((k >= 0) & (k < A))
                def _():
                    remote(xs.at[p, k, c], xs.at[p, k, c], zs.at[0, p], zr.at[k, p], toward[-d]).wait_recv()

                    @pl.when(has[d])
                    def _():
                        z_copy(k, p, s, d).start()

                    c_copy(k, p, c).start()

        if s < 3:
            y_arrival(s - 1).wait_recv()
            for twin in twins:
                g_copy(s - 1, mine, twin).start()
    for twin in twins:
        g_copy(0, twin, mine).wait_recv()
    load_w.wait()
    total = jnp.zeros((2 * A * rows, PAD), jnp.float32)
    for p in range(P):
        for k in range(A):
            c_copy(k, p, 1 - c).wait_recv()
        total = total + lax.dot_general(
            xs[p].reshape(2 * A * rows, W), w2[:, :, p * W : (p + 1) * W].reshape(PAD, W),
            (((1,), (1,)), ((), ())), preferred_element_type=jnp.float32,
        )
    q_ref[...] = total.astype(jnp.bfloat16).reshape(2 * A, rows, PAD)

    def own_strip(slot):
        return w8.at[slot, strip(mine)]

    beyond = remote(wo_ref.at[strip(mine)], own_strip(4), es.at[0], er.at[0], index_of(a + 1 - 2 * (a % 2), b, c))
    beyond_across = remote(own_strip(4), own_strip(6), es.at[1], er.at[1], across)
    beyond_pair = remote(w8.at[4], w8.at[5], es.at[2], er.at[2], pair)
    beyond_diagonal = remote(w8.at[6], w8.at[7], es.at[3], er.at[3], pair)

    def t_copy(i, part, to):
        spot = w8.at[4 + 2 * i, strip(part)]
        return pltpu.make_async_remote_copy(
            src_ref=spot, dst_ref=spot, send_sem=gs.at[2 + i, to], recv_sem=gr.at[2 + i, part],
            device_id={"groups": to, "mp": me}, device_id_type=MESH,
        )

    def share_first():
        beyond.start()

    def share_second():
        for twin in twins:
            g_copy(1, twin, mine).wait_recv()
        plane_diagonal.start()

    def share_third():
        beyond.wait_recv()
        beyond_across.start()
        for twin in twins:
            t_copy(0, mine, twin).start()

    def share_fourth():
        beyond_across.wait_recv()
        for twin in twins:
            t_copy(1, mine, twin).start()
        for twin in twins:
            t_copy(0, twin, mine).wait_recv()
        beyond_pair.start()

    def share_fifth():
        for twin in twins:
            t_copy(1, twin, mine).wait_recv()
        beyond_diagonal.start()

    def share_arrived():
        load_own.wait()
        plane_pair.wait_recv()
        plane_diagonal.wait_recv()
        beyond_pair.wait_recv()
        beyond_diagonal.wait_recv()

    def finish():
        for s in range(A):
            for d in (1, -1):
                k = a - s * d

                @pl.when((k >= 0) & (k < A) & has[d])
                def _():
                    for p in range(P):
                        z_copy(k, p, s, d).wait_send()

        for k in range(A):
            for p in range(P):
                c_copy(k, p, c).wait_send()
        for which in range(2):
            y_copy(which).wait_send()
            for twin in twins:
                g_copy(which, mine, twin).wait_send()
        plane_pair.wait_send()
        plane_diagonal.wait_send()
        for copy in (beyond, beyond_across, beyond_pair, beyond_diagonal):
            copy.wait_send()
        for i in range(2):
            for twin in twins:
                t_copy(i, mine, twin).wait_send()

    return (share_first, share_second, share_third, share_fourth, share_fifth), share_arrived, finish


def attend_phase(
    n, between, lengths_ref, q_ref, kv_ref, cached_ref, context_ref,
    kv, cached, scores, chances, stats,
    q_all, q_cached, o_send, o_recv, st_send, st_recv,
    local, qzs, qzr, qys, qyr, qcs, qcr, os, orr, ss, sr,
):
    A = n // 4
    me, a, b, c = place(n)
    across, pair = index_of(a, 1 - b, c), index_of(a, b, 1 - c)
    requests, positions, width = kv.shape
    pairs, heads = requests // 2, width // PAD
    rows = q_ref.shape[1]
    length = cached.shape[1]
    load_cached = pltpu.make_async_copy(cached_ref, cached, local.at[0])
    load_kv = pltpu.make_async_copy(kv_ref, kv, local.at[1])
    load_cached.start()
    load_kv.start()
    order = sorted(range(1, n), key=lambda s: -min(s, n - s))
    others = [lax.rem(me + s, n) for s in order]
    columns = [lax.rem(a + s, A) for s in range(1, A)]
    entering, flying = pl.ds(0, A), pl.ds(A, A)
    q_all[a, c, b] = q_ref[:A]
    q_cached[b] = q_ref[A:]
    stats[...] = jnp.zeros_like(stats)

    def qz_copy(to, k):
        return remote(q_ref.at[entering], q_all.at[k, c, b], qzs.at[to], qzr.at[k], index_of(to, b, c))

    def qy_copy(k, bb, src=None):
        spot = q_all.at[k, c, bb]
        return remote(spot if src is None else src, spot, qys.at[k], qyr.at[k], across)

    def qc_copy(k, bb, cc, src=None):
        spot = q_all.at[k, cc, bb]
        return remote(spot if src is None else src, spot, qcs.at[bb * A + k], qcr.at[bb * A + k], pair)

    def cached_copy(bb):
        return remote(q_ref.at[flying], q_cached.at[bb], qys.at[A], qyr.at[A], across)

    def o_copy(other, spot, step):
        at = pl.ds(pl.multiple_of(step * QLEN, QLEN), QLEN)
        return remote(
            o_send.at[other, at], o_recv.at[spot, at], os.at[step, other], orr.at[step, spot], other
        )

    def st_copy(other, spot):
        return remote(st_send.at[other], st_recv.at[spot], ss.at[other], sr.at[spot], other)

    for k in columns:
        qz_copy(k, a).start()
    qy_copy(a, b, q_ref.at[entering]).start()
    cached_copy(b).start()
    qc_copy(a, b, c, q_ref.at[entering]).start()
    between[0]()
    lane = lax.broadcasted_iota(jnp.int32, (QLEN, PAD), 1)
    low = lane < DH

    def request_of(r, block):
        per = QLEN // rows
        parts = []
        for i in range(per):
            spot = r * per + i
            parts.append(block((spot // 2) % 2, (spot // 4) * 2 + spot % 2))
        return parts[0] if per == 1 else jnp.concatenate(parts, axis=0)

    def put(r, value):
        per = QLEN // rows
        for i in range(per):
            context_ref[r * per + i] = value[i * rows : (i + 1) * rows].astype(jnp.bfloat16)

    def cached_request(r):
        block = cached[r]
        query = request_of(r, lambda bb, spot: q_cached[bb, spot]).astype(jnp.float32)
        query = jnp.where(b == 0, query, pltpu.roll(query, DH, 1))
        found = lax.dot_general(
            jnp.where(low, query, 0.0).astype(jnp.bfloat16), block, (((1,), (1,)), ((), ())),
            preferred_element_type=jnp.float32,
        )
        usable = lax.broadcasted_iota(jnp.int32, (1, length), 1) < lengths_ref[1, r]
        masked = jnp.where(usable, found, -1e30)
        exponent = jnp.exp(masked - jnp.max(masked, axis=-1, keepdims=True))
        inverse = 1.0 / jnp.sum(exponent, axis=-1, keepdims=True)
        weights = (exponent * inverse).astype(jnp.bfloat16)
        put(requests + r, jnp.dot(weights, block, preferred_element_type=jnp.float32))

    def cached_requests(start, stop):
        def two(i, carry):
            cached_request(start + 2 * i)
            cached_request(start + 2 * i + 1)
            return carry

        lax.fori_loop(0, (stop - start) // 2, two, 0)
        if (stop - start) % 2:
            cached_request(stop - 1)

    at_position = me * positions + lax.broadcasted_iota(jnp.int32, (1, positions), 1)

    def pair_step(step, carry):
        at = pl.ds(pl.multiple_of(step * QLEN, QLEN), QLEN)
        nothing = jnp.zeros((QLEN, PAD), jnp.bfloat16)
        for i in range(2):
            for g in range(heads // 2):
                two = []
                for cc in range(2):
                    packed = request_of(
                        step * 2 + i, lambda bb, spot: q_all[g // 2, cc, bb, spot]
                    ).astype(jnp.float32)
                    packed = packed if g % 2 == 0 else pltpu.roll(packed, DH, 1)
                    two.append(jnp.where(low, packed, 0.0).astype(jnp.bfloat16))
                spread = jnp.concatenate(
                    [
                        jnp.concatenate([two[0], nothing], axis=1),
                        jnp.concatenate([nothing, two[1]], axis=1),
                    ],
                    axis=0,
                )
                scores[i, g] = lax.dot_general(
                    spread, kv[step * 2 + i, :, g * 2 * PAD : (g + 1) * 2 * PAD], (((1,), (1,)), ((), ())),
                    preferred_element_type=jnp.float32,
                )
        for i in range(2):
            r = step * 2 + i
            masked = jnp.where(at_position < lengths_ref[0, r], scores[i], -1e30)
            largest = jnp.max(masked, axis=-1, keepdims=True)
            exponent = jnp.exp(masked - largest)
            total = jnp.sum(exponent, axis=-1, keepdims=True)
            chances[i] = exponent.astype(jnp.bfloat16)
            stats[...] = jnp.where(
                lane == r,
                largest.reshape(heads, QLEN, 1),
                jnp.where(lane == r + requests, total.reshape(heads, QLEN, 1), stats[...]),
            )
        for g in range(heads // 2):
            found = [
                jnp.dot(
                    chances[i, g], kv[step * 2 + i, :, g * 2 * PAD : (g + 1) * 2 * PAD],
                    preferred_element_type=jnp.float32,
                )
                for i in range(2)
            ]
            for e in range(2):
                even, odd = (f[e * QLEN : (e + 1) * QLEN, e * PAD : (e + 1) * PAD] for f in found)
                o_send[2 * g + e, at, :] = jnp.where(low, pltpu.roll(odd, DH, 1), even).astype(jnp.bfloat16)
        for other in others:
            o_copy(other, me, step).start()
        return carry

    def steps(column):
        def one(i, carry):
            return pair_step(2 * i + column, carry)

        lax.fori_loop(0, pairs // 2, one, 0)

    def second_column():
        qy_copy(a, 1 - b).wait_recv()
        qc_copy(a, 1 - b, c).start()
        for k in columns:
            qy_copy(k, 1 - b).wait_recv()
            qc_copy(k, 1 - b, c).start()

    def arrived(bb):
        for k in range(A):
            qc_copy(k, bb, 1 - c).wait_recv()

    for k in columns:
        qz_copy(k, k).wait_recv()
        qy_copy(k, b).start()
        qc_copy(k, b, c).start()
    between[1]()
    cached_copy(1 - b).wait_recv()
    load_cached.wait()
    first, second = requests // 4, requests // 2
    cached_requests(0, first)
    load_kv.wait()
    if rows == QLEN:
        arrived(b)
        steps(b)
        second_column()
    else:
        second_column()
        arrived(b)
        arrived(1 - b)
        steps(b)
    between[2]()
    cached_requests(first, second)
    if rows == QLEN:
        arrived(1 - b)
    steps(1 - b)
    parts = QLEN // 8
    gap = PAD // parts
    folded = stats[:, :8, :].reshape(heads * 8, PAD)
    for g in range(1, parts):
        folded = folded + pltpu.roll(stats[:, 8 * g : 8 * g + 8, :].reshape(heads * 8, PAD), g * gap, 1)
    st_send[...] = folded.reshape(heads, 8, PAD)
    for other in others:
        st_copy(other, me).start()
    o_recv[me] = o_send[me]
    st_recv[me] = st_send[me]
    cached_requests(second, requests)
    between[3]()
    for other in others:
        st_copy(other, other).wait_recv()
    largest = st_recv[...]
    scale = jnp.exp(largest - jnp.max(largest, axis=0, keepdims=True))
    total = jnp.sum(
        scale * pltpu.roll(largest.reshape(n * 8, PAD), PAD - requests, 1).reshape(n, 8, PAD), axis=0, keepdims=True
    )
    st_recv[...] = scale / jnp.where(total > 0.0, total, 1.0)
    short = low[:8]
    for step in range(pairs):
        for other in others:
            o_copy(other, other, step).wait_recv()
        mixed = jnp.zeros((QLEN, PAD), jnp.float32)
        for d in range(n):
            known = st_recv[d]
            share = []
            for g in range(parts):
                lone = g * gap + 2 * step
                share.append(jnp.where(short, known[:, lone + 1 : lone + 2], known[:, lone : lone + 1]))
            share = jnp.concatenate(share, axis=0)
            mixed = mixed + share * o_recv[d, step * QLEN : (step + 1) * QLEN, :].astype(jnp.float32)
        put(2 * step, mixed)
        put(2 * step + 1, pltpu.roll(mixed, DH, 1))

    def finish():
        for k in columns:
            qz_copy(k, a).wait_send()
        cached_copy(b).wait_send()
        for k in range(A):
            qy_copy(k, b).wait_send()
            for bb in range(2):
                qc_copy(k, bb, c).wait_send()
        for other in others:
            st_copy(other, me).wait_send()
            for step in range(pairs):
                o_copy(other, me, step).wait_send()

    return finish


def project_phase(
    n, start, arrived, context_ref, hidden_ref, out_ref, w8, part, c_send, c_recv, zsend, zright, zleft, cs, cr, zs, zr
):
    M = n // 8
    me, a, b, c = place(n)
    m, e = a // 2, a % 2
    has = {1: m < M - 1, -1: m > 0}
    toward = {1: me + 8, -1: me - 8}
    landing = {1: zright, -1: zleft}
    P, _, rows, W = part.shape
    depth = w8.shape[1]

    def peer(j):
        return e + (j // 4) * (1 - 2 * e), b + (j // 2 % 2) * (1 - 2 * b), c + (j % 2) * (1 - 2 * c)

    swaps = []
    for j in range(7, -1, -1):
        ee, bb, cc = peer(j)
        for k in range(M):
            block = context_ref[index_of(2 * k + ee, bb, cc)]
            if j:
                c_send[j - 1, k] = block
            else:
                c_recv[0, k] = block
        if j:
            swap = remote(c_send.at[j - 1], c_recv.at[j], cs.at[j - 1], cr.at[j - 1], index_of(2 * m + ee, bb, cc))
            swap.start()
            swaps.append(swap)
    start()
    for swap in swaps:
        swap.wait_recv()
    low = lax.broadcasted_iota(jnp.int32, (M * rows, PAD), 1) < DH

    def beside(i):
        first = c_recv[i].reshape(M * rows, PAD).astype(jnp.float32)
        second = c_recv[i + 1].reshape(M * rows, PAD).astype(jnp.float32)
        return jnp.where(low, pltpu.roll(first, DH, 1), second).astype(jnp.bfloat16)

    left = jnp.concatenate([beside(i) for i in range(0, 8, 2)], axis=1)
    arrived()

    def z_copy(k, p, d):
        return remote(zsend.at[p, k], landing[d].at[p, k], zs.at[k, p], zr.at[(0 if d == 1 else M) + k, p], toward[d])

    def z_arrival(k, p, d):
        return remote(zsend.at[p, k], landing[d].at[p, k], zs.at[k, p], zr.at[(0 if d == 1 else M) + k, p], toward[-d])

    for s in range(M - 1, -1, -1):
        for p in range(P):
            if s == M - 1:
                w = w8[:, :, p * W : (p + 1) * W].reshape(8 * depth, W)
                found = jnp.dot(left, w, preferred_element_type=jnp.float32)
                part[p] = found.reshape(M, rows, W)
            for d in (1, -1) if s else (1,):
                k = m + s * d

                @pl.when((k >= 0) & (k < M))
                def _():
                    for came in (d,) if s else (1, -1):

                        @pl.when(has[-came])
                        def _():
                            z_arrival(k, p, came).wait_recv()
                            part[p, k] = part[p, k] + landing[came][p, k].astype(jnp.float32)

                    if s:
                        zsend[p, k] = part[p, k].astype(jnp.bfloat16)
                        z_copy(k, p, d).start()
                    else:
                        at = slice(p * W, (p + 1) * W)
                        out_ref[:, at] = (hidden_ref[:, at].astype(jnp.float32) + part[p, k]).astype(jnp.bfloat16)

    def finish():
        for s in range(M - 1, 0, -1):
            for d in (1, -1):
                k = m + s * d

                @pl.when((k >= 0) & (k < M))
                def _():
                    for p in range(P):
                        z_copy(k, p, d).wait_send()

        for swap in swaps:
            swap.wait_send()

    return finish


def far_first(A, a):
    low, high = 0, A - 1
    found = []
    for _ in range(A):
        left = (a - low > high - a).astype(jnp.int32)
        found.append(high + left * (low - high))
        low, high = low + left, high - 1 + left
    return found


def feed_phase(
    n, x_ref, gain_ref, gate_ref, up_ref, down_ref, out_ref,
    w_in, sums_in, w_down, act, part,
    xs, cbuf, ysend, yrecv, zsend, zland,
    local, zs, zr, ys, yr, cs, cr, gs, gr, hs, hr, ts, tr,
):
    A = n // 4
    me, a, b, c = place(n)
    across, pair = index_of(a, 1 - b, c), index_of(a, b, 1 - c)
    has, toward = neighbours(n)
    P, W = xs.shape[0], xs.shape[-1]
    rows = x_ref.shape[0]
    units = gate_ref.shape[1]
    split = [(w_in[0], slice(0, units)), (w_in[-1], slice(units, 2 * units) if len(w_in) == 1 else slice(0, units))]
    loads = [
        pltpu.make_async_copy(gate_ref, split[0][0].at[:, split[0][1]], local.at[0]),
        pltpu.make_async_copy(up_ref, split[1][0].at[:, split[1][1]], local.at[1]),
        pltpu.make_async_copy(down_ref, w_down, local.at[2]),
    ]
    for load in loads:
        load.start()
    values = x_ref[...].astype(jnp.float32)
    scale = lax.rsqrt(jnp.mean(values * values, axis=-1, keepdims=True) + epsilon)
    for p in range(P):
        at = slice(p * W, (p + 1) * W)
        xs[p, b, c, a] = (values[:, at] * scale * gain_ref[:, at]).astype(jnp.bfloat16)

    def z_copy(k, p, s, d):
        block = xs.at[p, b, c, k]
        return remote(block, block, zs.at[(0 if d == 1 else A) + s, p], zr.at[k, p], toward[d])

    def y_copy(k, p, bb):
        block = xs.at[p, bb, c, k]
        return remote(block, block, ys.at[k, p], yr.at[k, p], across)

    def c_copy(k, p, bb, cc):
        block = xs.at[p, bb, cc, k]
        return remote(block, block, cs.at[bb * A + k, p], cr.at[bb * A + k, p], pair)

    for p in range(P):
        for d in (1, -1):

            @pl.when(has[d])
            def _():
                z_copy(a, p, 0, d).start()

        y_copy(a, p, b).start()
    for p in range(P):
        c_copy(a, p, b, c).start()

    def pass_on(s, p):
        for d in (1, -1) if s else (1,):
            k = a - s * d

            @pl.when((k >= 0) & (k < A))
            def _():
                y_copy(k, p, 1 - b).wait_recv()
                c_copy(k, p, 1 - b, c).start()

    for s in range(1, A):
        for p in range(P):
            for d in (1, -1):
                k = a - s * d

                @pl.when((k >= 0) & (k < A))
                def _():
                    block = xs.at[p, b, c, k]
                    remote(block, block, zs.at[0, p], zr.at[k, p], toward[-d]).wait_recv()

                    @pl.when(has[d])
                    def _():
                        z_copy(k, p, s, d).start()

                    y_copy(k, p, b).start()
                    c_copy(k, p, b, c).start()

            if s > 1:
                pass_on(s - 2, p)
    for p in range(P):
        pass_on(A - 2, p)
    for load in loads:
        load.wait()

    def contract(p):
        for bb in range(2):
            for k in range(A):
                c_copy(k, p, bb, 1 - c).wait_recv()
        left = xs[p].reshape(n * rows, W)
        for w, sums in zip(w_in, sums_in):
            found = jnp.dot(left, w[p * W : (p + 1) * W, :], preferred_element_type=jnp.float32)
            sums[...] = found if p == 0 else sums[...] + found

    for p in range(P):
        pass_on(A - 1, p)
        if p:
            contract(p - 1)
    contract(P - 1)
    for p in range(P):
        for s in range(A):
            for d in (1, -1):
                k = a - s * d

                @pl.when((k >= 0) & (k < A) & has[d])
                def _():
                    z_copy(k, p, s, d).wait_send()

        for k in range(A):
            y_copy(k, p, b).wait_send()
            for bb in range(2):
                c_copy(k, p, bb, c).wait_send()

    tall = A * rows
    for group in range(4):
        at = slice(group * tall, (group + 1) * tall)
        gate, up = sums_in[0][at, split[0][1]], sums_in[-1][at, split[1][1]]
        act[group] = (jax.nn.gelu(gate, approximate=True) * up).astype(jnp.bfloat16)

    def multiply(i, p, bb, cc):
        found = jnp.dot(act[2 * bb + cc], w_down[:, p * W : (p + 1) * W], preferred_element_type=jnp.float32)
        part[i, p] = found.reshape(A, rows, W)

    def g_copy(side, p):
        return remote(part.at[2 * side, p], cbuf.at[side, p], gs.at[side, p], gr.at[side, p], pair)

    def h_copy(k, p):
        return remote(ysend.at[p, k], yrecv.at[p, k], hs.at[k, p], hr.at[k, p], across)

    def t_copy(k, p, right):
        return remote(
            zsend.at[p, k], zland.at[right, p, k], ts.at[k, p], tr.at[right, k, p], me + 8 * right - 4
        )

    def t_arrival(k, p, right):
        return remote(
            zsend.at[p, k], zland.at[right, p, k], ts.at[k, p], tr.at[right, k, p], me - 8 * right + 4
        )

    order = far_first(A, a)
    for t, k in enumerate(order):
        for p in range(P):
            if t == 0:
                if p == 0:
                    multiply(0, p, 1 - b, 1 - c)
                    g_copy(0, p).start()
                    multiply(1, p, 1 - b, c)
                if p + 1 < P:
                    multiply(0, p + 1, 1 - b, 1 - c)
                    g_copy(0, p + 1).start()
                g_copy(0, p).wait_recv()
            ysend[p, k] = (part[1, p, k] + cbuf[0, p, k]).astype(jnp.bfloat16)
            h_copy(k, p).start()
            if t == 0 and p + 1 < P:
                multiply(1, p + 1, 1 - b, c)
    for p in range(P):
        multiply(2, p, b, 1 - c)
        g_copy(1, p).start()
    for p in range(P):
        multiply(3, p, b, c)
    for t, k in enumerate(order):
        right = (k > a).astype(jnp.int32)
        for p in range(P):
            if t == 0:
                g_copy(1, p).wait_recv()
            h_copy(k, p).wait_recv()
            part[3, p, k] = part[3, p, k] + cbuf[1, p, k] + yrecv[p, k].astype(jnp.float32)
            if t < A - 1:
                comes = ((right == 1) & (a > 0)) | ((right == 0) & (a < A - 1))

                @pl.when(comes)
                def _():
                    t_arrival(k, p, right).wait_recv()
                    part[3, p, k] = part[3, p, k] + zland[right, p, k].astype(jnp.float32)

                zsend[p, k] = part[3, p, k].astype(jnp.bfloat16)
                t_copy(k, p, right).start()
            else:
                for came in (1, -1):

                    @pl.when(has[-came])
                    def _():
                        side = (came + 1) // 2
                        t_arrival(k, p, side).wait_recv()
                        part[3, p, k] = part[3, p, k] + zland[side, p, k].astype(jnp.float32)

                at = slice(p * W, (p + 1) * W)
                out_ref[:, at] = (x_ref[:, at].astype(jnp.float32) + part[3, p, k]).astype(jnp.bfloat16)

    for t, k in enumerate(order):
        right = (k > a).astype(jnp.int32)
        for p in range(P):
            h_copy(k, p).wait_send()
            if t < A - 1:
                t_copy(k, p, right).wait_send()
    for p in range(P):
        g_copy(0, p).wait_send()
        g_copy(1, p).wait_send()


def layer_kernel(n, groups, counts, *refs):
    ends = [sum(counts[: i + 1]) for i in range(len(counts))]
    inputs, (out_ref,), shared, ask, look, out, give = (
        refs[end - count : end] for end, count in zip(ends, counts)
    )
    hidden_ref, gain_ref, wq_ref, kv_ref, cached_ref, lengths_ref, wo_ref, ffn_gain, gate_ref, up_ref, down_ref = inputs
    q_ref, w8, context_ref, residual = shared
    half, full = jnp.bfloat16, jnp.float32
    rows, width = hidden_ref.shape
    requests, positions, across = kv_ref.shape
    heads, units = across // PAD, gate_ref.shape[1]
    P = pieces_of(n, width)
    A, W = n // 4, width // P
    shares, arrived, end_query = query_phase(
        n, groups, hidden_ref, gain_ref, wq_ref, wo_ref, q_ref, w8, *ask
    )

    def attending(*own):
        attend_phase(n, shares, lengths_ref, q_ref, kv_ref, cached_ref, context_ref, *own, *look)()

    pl.run_scoped(
        attending,
        VM(kv_ref.shape, half),
        VM(cached_ref.shape, half),
        VM((2, heads // 2, 2 * QLEN, positions), full),
        VM((2, heads // 2, 2 * QLEN, positions), half),
        VM((n, QLEN, PAD), full),
    )

    def projecting(part):
        project_phase(n, shares[4], arrived, context_ref, hidden_ref, residual, w8, part, *out)()

    pl.run_scoped(projecting, VM((P, A // 2, rows, W), full))
    joined = 1 if units % PAD == 0 else 2
    wide = 2 * units // joined

    def feeding(*own):
        feed_phase(
            n, residual, ffn_gain, gate_ref, up_ref, down_ref, out_ref,
            own[:joined], own[joined : 2 * joined], *own[2 * joined :], *give,
        )

    pl.run_scoped(
        feeding,
        *[VM((width, wide), half)] * joined,
        *[VM((n * rows, wide), full)] * joined,
        VM(down_ref.shape, half),
        VM((4, A * rows, units), half),
        VM((4, P, A, rows, W), full),
    )
    end_query()


def layer(n, groups, hidden, gain, w_query, entering_kv, cached_kv, lengths, w_out, ffn_gain, w_gate, w_up, w_down):
    A = n // 4
    rows, width = hidden.shape
    requests, positions, across = entering_kv.shape
    pairs, heads = requests // 2, across // PAD
    assert A > 2 and A % 2 == 0 and DH % groups == 0 and pairs % 2 == 0
    assert heads == n and QLEN % rows == 0 and 8 * requests <= PAD
    P = pieces_of(n, width)
    W = width // P
    half, full = jnp.bfloat16, jnp.float32
    piece = (P, A, rows, W)
    inputs = (
        hidden, gain[None, :], w_query.T, entering_kv, cached_kv, lengths, w_out, ffn_gain[None, :],
        w_gate, w_up, w_down,
    )
    spaces = (VM, VM, pl.ANY, pl.ANY, pl.ANY, pltpu.SMEM, pl.ANY, VM, pl.ANY, pl.ANY, pl.ANY)
    shared = [
        VM((2 * A, rows, PAD), half), VM((8,) + w_out.shape, half), VM((n, rows, PAD), half), VM((rows, width), half),
    ]
    ask = [
        VM((P, A, 2, rows, W), half), VM((2, DH, width), half),
        DMA((2,)), DMA((2 * A, P)), DMA((A, P)), DMA((A, P)), DMA((A, P)),
        DMA((2,)), DMA((2,)), DMA((4, groups)), DMA((4, groups)), DMA((2,)), DMA((2,)), DMA((4,)), DMA((4,)),
    ]
    look = [
        VM((A, 2, 2, A, rows, PAD), half), VM((2, A, rows, PAD), half),
        VM((n, pairs * QLEN, PAD), half), VM((n, pairs * QLEN, PAD), half),
        VM((n, 8, PAD), full), VM((n, 8, PAD), full),
        DMA((2,)), DMA((A,)), DMA((A,)), DMA((A + 1,)), DMA((A + 1,)), DMA((2 * A,)), DMA((2 * A,)),
        DMA((pairs, n)), DMA((pairs, n)), DMA((n,)), DMA((n,)),
    ]
    M = A // 2
    half_piece = (P, M, rows, W)
    out = [VM((7, M, rows, PAD), half), VM((8, M, rows, PAD), half)] + [VM(half_piece, half)] * 3
    out += [DMA((7,)), DMA((7,)), DMA((M, P)), DMA((2 * M, P))]
    give = [
        VM((P, 2, 2, A, rows, W), half), VM((2,) + piece, full),
        VM(piece, half), VM(piece, half), VM(piece, half), VM((2,) + piece, half),
        DMA((3,)), DMA((2 * A, P)), DMA((A, P)), DMA((A, P)), DMA((A, P)), DMA((2 * A, P)), DMA((2 * A, P)),
        DMA((2, P)), DMA((2, P)), DMA((A, P)), DMA((A, P)), DMA((A, P)), DMA((2, A, P)),
    ]
    parts = (inputs, (None,), shared, ask, look, out, give)
    return pl.pallas_call(
        functools.partial(layer_kernel, n, groups, tuple(len(part) for part in parts)),
        out_shape=jax.ShapeDtypeStruct((rows, width), half),
        in_specs=[pl.BlockSpec(memory_space=m) for m in spaces],
        out_specs=pl.BlockSpec(memory_space=VM),
        scratch_shapes=shared + ask + look + out + give,
        compiler_params=pltpu.CompilerParams(
            collective_id=0, has_side_effects=True, vmem_limit_bytes=60 * 2**20
        ),
        name="layer",
    )(*inputs)


def solution(mesh):
    placed = (
        P(("groups", "mp"), None),
        P(),
        P(None, "mp"),
        P("groups", "mp", None),
        P("groups", None, "mp"),
        P(None, "groups"),
        P("mp", None),
        P(),
        P(None, "mp"),
        P(None, "mp"),
        P("mp", None),
    )
    return jax.shard_map(
        functools.partial(layer, mesh.shape["mp"], mesh.shape["groups"]),
        mesh=mesh,
        in_specs=placed,
        out_specs=P(("groups", "mp"), None),
        check_vma=False,
    )
```

```python
import functools

import jax
import jax.numpy as jnp
from jax import lax
from jax.experimental import pallas as pl
from jax.experimental.pallas import tpu as pltpu
from jax.sharding import PartitionSpec as P

DH = 64
QLEN = 32
PAD = 2 * DH
MESH = pl.DeviceIdType.MESH
VM = pltpu.VMEM
DMA = pltpu.SemaphoreType.DMA

epsilon = 0.1


def place(n):
    me = lax.axis_index("mp")
    return me, me // 4, (me // 2) % 2, me % 2


def index_of(a, b, c):
    return (a * 2 + b) * 2 + c


def remote(src, dst, send, recv, to):
    return pltpu.make_async_remote_copy(
        src_ref=src, dst_ref=dst, send_sem=send, recv_sem=recv, device_id={"mp": to}, device_id_type=MESH
    )


def greet(to):
    pl.semaphore_signal(pltpu.get_barrier_semaphore(), inc=1, device_id={"mp": to}, device_id_type=MESH)


def pieces_of(n, width):
    return max(1, min(4, 16 // (n // 4), width // 128))


def neighbours(n):
    A = n // 4
    me, a, b, c = place(n)
    has = {1: a < A - 1, -1: a > 0}
    toward = {1: me + 4, -1: me - 4}
    return has, toward


def far_first(A, a):
    low, high = 0, A - 1
    found = []
    for _ in range(A):
        left = (a - low > high - a).astype(jnp.int32)
        found.append(high + left * (low - high))
        low, high = low + left, high - 1 + left
    return found


def query_phase(
    n, groups, x_ref, gain_ref, wq_ref, wo_ref, q_ref, w8, xs, w2, local, zs, zr, cs, cr, ys, yr, gs, gr, ps, pr, es, er
):
    A = n // 4
    me, a, b, c = place(n)
    mine = lax.axis_index("groups")
    across, pair = index_of(a, 1 - b, c), index_of(a, b, 1 - c)
    has, toward = neighbours(n)
    P, W = xs.shape[0], xs.shape[-1]
    rows = x_ref.shape[0]
    share = DH // groups
    twins = [lax.rem(mine + i, groups) for i in range(1, groups)]
    for other in range(1, n):
        greet(lax.rem(me + other, n))
    for twin in twins:
        pl.semaphore_signal(
            pltpu.get_barrier_semaphore(), inc=1, device_id={"groups": twin, "mp": me}, device_id_type=MESH
        )
    load_w = pltpu.make_async_copy(wq_ref, w2.at[b], local.at[0])
    load_w.start()
    load_own = pltpu.make_async_copy(wo_ref, w8.at[0], local.at[1])
    load_own.start()
    values = x_ref[...].astype(jnp.float32)
    scale = lax.rsqrt(jnp.mean(values * values, axis=-1, keepdims=True) + epsilon)
    for p in range(P):
        part = slice(p * W, (p + 1) * W)
        xs[p, a, c] = (values[:, part] * scale * gain_ref[:, part]).astype(jnp.bfloat16)
    pl.semaphore_wait(pltpu.get_barrier_semaphore(), n + groups - 2)

    def z_copy(k, p, s, d):
        row = 0 if d == 1 else A
        return remote(xs.at[p, k, c], xs.at[p, k, c], zs.at[row + s, p], zr.at[k, p], toward[d])

    def c_copy(k, p, cc):
        return remote(xs.at[p, k, cc], xs.at[p, k, cc], cs.at[k, p], cr.at[k, p], pair)

    def strip(part):
        return pl.ds(pl.multiple_of(part * share, share), share)

    def landing(which, bb, part):
        return w2.at[bb, strip(part)] if which == 0 else w8.at[2, strip(part)]

    def y_copy(which):
        source = (wq_ref, wo_ref)[which].at[strip(mine)]
        return remote(source, landing(which, b, mine), ys.at[which], yr.at[which], across)

    def y_arrival(which):
        spot = landing(which, 1 - b, mine)
        return remote(spot, spot, ys.at[which], yr.at[which], across)

    def g_copy(which, part, to):
        spot = landing(which, 1 - b, part)
        return pltpu.make_async_remote_copy(
            src_ref=spot, dst_ref=spot, send_sem=gs.at[which, to], recv_sem=gr.at[which, part],
            device_id={"groups": to, "mp": me}, device_id_type=MESH,
        )

    plane_pair = remote(wo_ref, w8.at[1], ps.at[0], pr.at[0], pair)
    plane_diagonal = remote(w8.at[2], w8.at[3], ps.at[1], pr.at[1], pair)
    for p in range(P):
        for d in (1, -1):

            @pl.when(has[d])
            def _():
                z_copy(a, p, 0, d).start()

    for which in range(2):
        y_copy(which).start()
    for p in range(P):
        c_copy(a, p, c).start()
    plane_pair.start()
    for s in range(1, A):
        for p in range(P):
            for d in (1, -1):
                k = a - s * d

                @pl.when((k >= 0) & (k < A))
                def _():
                    remote(xs.at[p, k, c], xs.at[p, k, c], zs.at[0, p], zr.at[k, p], toward[-d]).wait_recv()

                    @pl.when(has[d])
                    def _():
                        z_copy(k, p, s, d).start()

                    c_copy(k, p, c).start()

        if s < 3:
            y_arrival(s - 1).wait_recv()
            for twin in twins:
                g_copy(s - 1, mine, twin).start()
    for twin in twins:
        g_copy(0, twin, mine).wait_recv()
    load_w.wait()
    total = jnp.zeros((2 * A * rows, PAD), jnp.float32)
    for p in range(P):
        for k in range(A):
            c_copy(k, p, 1 - c).wait_recv()
        total = total + lax.dot_general(
            xs[p].reshape(2 * A * rows, W), w2[:, :, p * W : (p + 1) * W].reshape(PAD, W),
            (((1,), (1,)), ((), ())), preferred_element_type=jnp.float32,
        )
    q_ref[...] = total.astype(jnp.bfloat16).reshape(2 * A, rows, PAD)

    def own_strip(slot):
        return w8.at[slot, strip(mine)]

    beyond = remote(wo_ref.at[strip(mine)], own_strip(4), es.at[0], er.at[0], index_of(a + 1 - 2 * (a % 2), b, c))
    beyond_across = remote(own_strip(4), own_strip(6), es.at[1], er.at[1], across)
    beyond_pair = remote(w8.at[4], w8.at[5], es.at[2], er.at[2], pair)
    beyond_diagonal = remote(w8.at[6], w8.at[7], es.at[3], er.at[3], pair)

    def t_copy(i, part, to):
        spot = w8.at[4 + 2 * i, strip(part)]
        return pltpu.make_async_remote_copy(
            src_ref=spot, dst_ref=spot, send_sem=gs.at[2 + i, to], recv_sem=gr.at[2 + i, part],
            device_id={"groups": to, "mp": me}, device_id_type=MESH,
        )

    def share_first():
        beyond.start()

    def share_second():
        for twin in twins:
            g_copy(1, twin, mine).wait_recv()
        plane_diagonal.start()

    def share_third():
        beyond.wait_recv()
        beyond_across.start()
        for twin in twins:
            t_copy(0, mine, twin).start()

    def share_fourth():
        beyond_across.wait_recv()
        for twin in twins:
            t_copy(1, mine, twin).start()
        for twin in twins:
            t_copy(0, twin, mine).wait_recv()
        beyond_pair.start()

    def share_fifth():
        for twin in twins:
            t_copy(1, twin, mine).wait_recv()
        beyond_diagonal.start()

    def share_arrived():
        load_own.wait()
        plane_pair.wait_recv()
        plane_diagonal.wait_recv()
        beyond_pair.wait_recv()
        beyond_diagonal.wait_recv()

    def finish():
        for s in range(A):
            for d in (1, -1):
                k = a - s * d

                @pl.when((k >= 0) & (k < A) & has[d])
                def _():
                    for p in range(P):
                        z_copy(k, p, s, d).wait_send()

        for k in range(A):
            for p in range(P):
                c_copy(k, p, c).wait_send()
        for which in range(2):
            y_copy(which).wait_send()
            for twin in twins:
                g_copy(which, mine, twin).wait_send()
        plane_pair.wait_send()
        plane_diagonal.wait_send()
        for copy in (beyond, beyond_across, beyond_pair, beyond_diagonal):
            copy.wait_send()
        for i in range(2):
            for twin in twins:
                t_copy(i, mine, twin).wait_send()

    return (share_first, share_second, share_third, share_fourth, share_fifth), share_arrived, finish


def attend_phase(
    n, between, lengths_ref, q_ref, kv_ref, cached_ref, context_ref,
    kv, cached, scores, chances, stats,
    q_all, q_cached, o_send, o_recv, st_send, st_recv,
    local, qzs, qzr, qys, qyr, qcs, qcr, os, orr, ss, sr,
):
    A = n // 4
    me, a, b, c = place(n)
    across, pair = index_of(a, 1 - b, c), index_of(a, b, 1 - c)
    requests, positions, width = kv.shape
    pairs, heads = requests // 2, width // PAD
    rows = q_ref.shape[1]
    length = cached.shape[1]
    load_cached = pltpu.make_async_copy(cached_ref, cached, local.at[0])
    load_kv = pltpu.make_async_copy(kv_ref, kv, local.at[1])
    load_cached.start()
    load_kv.start()
    *far, _ = far_first(A, a)
    others = [index_of(k, bb, cc) for k in far for bb in (b, 1 - b) for cc in (c, 1 - c)]
    others += [index_of(a, 1 - b, 1 - c), across, pair]
    columns = far
    entering, flying = pl.ds(0, A), pl.ds(A, A)
    q_all[a, c, b] = q_ref[:A]
    q_cached[b] = q_ref[A:]
    stats[...] = jnp.zeros_like(stats)

    def qz_copy(to, k):
        return remote(q_ref.at[entering], q_all.at[k, c, b], qzs.at[to], qzr.at[k], index_of(to, b, c))

    def qy_copy(k, bb, src=None):
        spot = q_all.at[k, c, bb]
        return remote(spot if src is None else src, spot, qys.at[k], qyr.at[k], across)

    def qc_copy(k, bb, cc, src=None):
        spot = q_all.at[k, cc, bb]
        return remote(spot if src is None else src, spot, qcs.at[bb * A + k], qcr.at[bb * A + k], pair)

    def cached_copy(bb):
        return remote(q_ref.at[flying], q_cached.at[bb], qys.at[A], qyr.at[A], across)

    def o_copy(other, spot, step):
        at = pl.ds(pl.multiple_of(step * QLEN, QLEN), QLEN)
        return remote(
            o_send.at[other, at], o_recv.at[spot, at], os.at[step, other], orr.at[step, spot], other
        )

    def st_copy(other, spot):
        return remote(st_send.at[other], st_recv.at[spot], ss.at[other], sr.at[spot], other)

    for k in columns:
        qz_copy(k, a).start()
    qy_copy(a, b, q_ref.at[entering]).start()
    cached_copy(b).start()
    qc_copy(a, b, c, q_ref.at[entering]).start()
    between[0]()
    lane = lax.broadcasted_iota(jnp.int32, (QLEN, PAD), 1)
    low = lane < DH

    def request_of(r, block):
        per = QLEN // rows
        parts = []
        for i in range(per):
            spot = r * per + i
            parts.append(block((spot // 2) % 2, (spot // 4) * 2 + spot % 2))
        return parts[0] if per == 1 else jnp.concatenate(parts, axis=0)

    def put(r, value):
        per = QLEN // rows
        for i in range(per):
            context_ref[r * per + i] = value[i * rows : (i + 1) * rows].astype(jnp.bfloat16)

    def cached_request(r):
        block = cached[r]
        query = request_of(r, lambda bb, spot: q_cached[bb, spot]).astype(jnp.float32)
        query = jnp.where(b == 0, query, pltpu.roll(query, DH, 1))
        found = lax.dot_general(
            jnp.where(low, query, 0.0).astype(jnp.bfloat16), block, (((1,), (1,)), ((), ())),
            preferred_element_type=jnp.float32,
        )
        usable = lax.broadcasted_iota(jnp.int32, (1, length), 1) < lengths_ref[1, r]
        masked = jnp.where(usable, found, -1e30)
        exponent = jnp.exp(masked - jnp.max(masked, axis=-1, keepdims=True))
        inverse = 1.0 / jnp.sum(exponent, axis=-1, keepdims=True)
        weights = (exponent * inverse).astype(jnp.bfloat16)
        put(requests + r, jnp.dot(weights, block, preferred_element_type=jnp.float32))

    def cached_requests(start, stop):
        def two(i, carry):
            cached_request(start + 2 * i)
            cached_request(start + 2 * i + 1)
            return carry

        lax.fori_loop(0, (stop - start) // 2, two, 0)
        if (stop - start) % 2:
            cached_request(stop - 1)

    at_position = me * positions + lax.broadcasted_iota(jnp.int32, (1, positions), 1)

    def pair_step(step, carry):
        at = pl.ds(pl.multiple_of(step * QLEN, QLEN), QLEN)
        nothing = jnp.zeros((QLEN, PAD), jnp.bfloat16)
        for i in range(2):
            for g in range(heads // 2):
                two = []
                for cc in range(2):
                    packed = request_of(
                        step * 2 + i, lambda bb, spot: q_all[g // 2, cc, bb, spot]
                    ).astype(jnp.float32)
                    packed = packed if g % 2 == 0 else pltpu.roll(packed, DH, 1)
                    two.append(jnp.where(low, packed, 0.0).astype(jnp.bfloat16))
                spread = jnp.concatenate(
                    [
                        jnp.concatenate([two[0], nothing], axis=1),
                        jnp.concatenate([nothing, two[1]], axis=1),
                    ],
                    axis=0,
                )
                scores[i, g] = lax.dot_general(
                    spread, kv[step * 2 + i, :, g * 2 * PAD : (g + 1) * 2 * PAD], (((1,), (1,)), ((), ())),
                    preferred_element_type=jnp.float32,
                )
        for i in range(2):
            r = step * 2 + i
            masked = jnp.where(at_position < lengths_ref[0, r], scores[i], -1e30)
            largest = jnp.max(masked, axis=-1, keepdims=True)
            exponent = jnp.exp(masked - largest)
            total = jnp.sum(exponent, axis=-1, keepdims=True)
            chances[i] = exponent.astype(jnp.bfloat16)
            stats[...] = jnp.where(
                lane == r,
                largest.reshape(heads, QLEN, 1),
                jnp.where(lane == r + requests, total.reshape(heads, QLEN, 1), stats[...]),
            )
        for g in range(heads // 2):
            found = [
                jnp.dot(
                    chances[i, g], kv[step * 2 + i, :, g * 2 * PAD : (g + 1) * 2 * PAD],
                    preferred_element_type=jnp.float32,
                )
                for i in range(2)
            ]
            for e in range(2):
                even, odd = (f[e * QLEN : (e + 1) * QLEN, e * PAD : (e + 1) * PAD] for f in found)
                o_send[2 * g + e, at, :] = jnp.where(low, pltpu.roll(odd, DH, 1), even).astype(jnp.bfloat16)
        for other in others:
            o_copy(other, me, step).start()
        return carry

    def steps(column):
        def one(i, carry):
            return pair_step(2 * i + column, carry)

        lax.fori_loop(0, pairs // 2, one, 0)

    def second_column():
        qy_copy(a, 1 - b).wait_recv()
        qc_copy(a, 1 - b, c).start()
        for k in columns:
            qy_copy(k, 1 - b).wait_recv()
            qc_copy(k, 1 - b, c).start()

    def arrived(bb):
        for k in range(A):
            qc_copy(k, bb, 1 - c).wait_recv()

    for k in columns:
        qz_copy(k, k).wait_recv()
        qy_copy(k, b).start()
        qc_copy(k, b, c).start()
    between[1]()
    cached_copy(1 - b).wait_recv()
    load_cached.wait()
    first, second = requests // 4, requests // 2
    cached_requests(0, first)
    load_kv.wait()
    if rows == QLEN:
        arrived(b)
        steps(b)
        second_column()
    else:
        second_column()
        arrived(b)
        arrived(1 - b)
        steps(b)
    between[2]()
    cached_requests(first, second)
    if rows == QLEN:
        arrived(1 - b)
    steps(1 - b)
    parts = QLEN // 8
    gap = PAD // parts
    folded = stats[:, :8, :].reshape(heads * 8, PAD)
    for g in range(1, parts):
        folded = folded + pltpu.roll(stats[:, 8 * g : 8 * g + 8, :].reshape(heads * 8, PAD), g * gap, 1)
    st_send[...] = folded.reshape(heads, 8, PAD)
    for other in others:
        st_copy(other, me).start()
    o_recv[me] = o_send[me]
    st_recv[me] = st_send[me]
    cached_requests(second, requests)
    between[3]()
    for other in others:
        st_copy(other, other).wait_recv()
    largest = st_recv[...]
    scale = jnp.exp(largest - jnp.max(largest, axis=0, keepdims=True))
    total = jnp.sum(
        scale * pltpu.roll(largest.reshape(n * 8, PAD), PAD - requests, 1).reshape(n, 8, PAD), axis=0, keepdims=True
    )
    st_recv[...] = scale / jnp.where(total > 0.0, total, 1.0)
    short = low[:8]
    for step in range(pairs):
        for other in others:
            o_copy(other, other, step).wait_recv()
        mixed = jnp.zeros((QLEN, PAD), jnp.float32)
        for d in range(n):
            known = st_recv[d]
            share = []
            for g in range(parts):
                lone = g * gap + 2 * step
                share.append(jnp.where(short, known[:, lone + 1 : lone + 2], known[:, lone : lone + 1]))
            share = jnp.concatenate(share, axis=0)
            mixed = mixed + share * o_recv[d, step * QLEN : (step + 1) * QLEN, :].astype(jnp.float32)
        put(2 * step, mixed)
        put(2 * step + 1, pltpu.roll(mixed, DH, 1))

    def finish():
        for k in columns:
            qz_copy(k, a).wait_send()
        cached_copy(b).wait_send()
        for k in range(A):
            qy_copy(k, b).wait_send()
            for bb in range(2):
                qc_copy(k, bb, c).wait_send()
        for other in others:
            st_copy(other, me).wait_send()
            for step in range(pairs):
                o_copy(other, me, step).wait_send()

    return finish


def project_phase(
    n, start, arrived, context_ref, hidden_ref, out_ref, w8, part, c_send, c_recv, zsend, zright, zleft, cs, cr, zs, zr
):
    M = n // 8
    me, a, b, c = place(n)
    m, e = a // 2, a % 2
    has = {1: m < M - 1, -1: m > 0}
    toward = {1: me + 8, -1: me - 8}
    landing = {1: zright, -1: zleft}
    P, _, rows, W = part.shape
    depth = w8.shape[1]

    def peer(j):
        return e + (j // 4) * (1 - 2 * e), b + (j // 2 % 2) * (1 - 2 * b), c + (j % 2) * (1 - 2 * c)

    swaps = []
    for j in range(7, -1, -1):
        ee, bb, cc = peer(j)
        for k in range(M):
            block = context_ref[index_of(2 * k + ee, bb, cc)]
            if j:
                c_send[j - 1, k] = block
            else:
                c_recv[0, k] = block
        if j:
            swap = remote(c_send.at[j - 1], c_recv.at[j], cs.at[j - 1], cr.at[j - 1], index_of(2 * m + ee, bb, cc))
            swap.start()
            swaps.append(swap)
    start()
    for swap in swaps:
        swap.wait_recv()
    low = lax.broadcasted_iota(jnp.int32, (M * rows, PAD), 1) < DH

    def beside(i):
        first = c_recv[i].reshape(M * rows, PAD).astype(jnp.float32)
        second = c_recv[i + 1].reshape(M * rows, PAD).astype(jnp.float32)
        return jnp.where(low, pltpu.roll(first, DH, 1), second).astype(jnp.bfloat16)

    left = jnp.concatenate([beside(i) for i in range(0, 8, 2)], axis=1)
    arrived()

    def z_copy(k, p, d):
        return remote(zsend.at[p, k], landing[d].at[p, k], zs.at[k, p], zr.at[(0 if d == 1 else M) + k, p], toward[d])

    def z_arrival(k, p, d):
        return remote(zsend.at[p, k], landing[d].at[p, k], zs.at[k, p], zr.at[(0 if d == 1 else M) + k, p], toward[-d])

    for s in range(M - 1, -1, -1):
        for p in range(P):
            if s == M - 1:
                w = w8[:, :, p * W : (p + 1) * W].reshape(8 * depth, W)
                found = jnp.dot(left, w, preferred_element_type=jnp.float32)
                part[p] = found.reshape(M, rows, W)
            for d in (1, -1) if s else (1,):
                k = m + s * d

                @pl.when((k >= 0) & (k < M))
                def _():
                    for came in (d,) if s else (1, -1):

                        @pl.when(has[-came])
                        def _():
                            z_arrival(k, p, came).wait_recv()
                            part[p, k] = part[p, k] + landing[came][p, k].astype(jnp.float32)

                    if s:
                        zsend[p, k] = part[p, k].astype(jnp.bfloat16)
                        z_copy(k, p, d).start()
                    else:
                        at = slice(p * W, (p + 1) * W)
                        out_ref[:, at] = (hidden_ref[:, at].astype(jnp.float32) + part[p, k]).astype(jnp.bfloat16)

    def finish():
        for s in range(M - 1, 0, -1):
            for d in (1, -1):
                k = m + s * d

                @pl.when((k >= 0) & (k < M))
                def _():
                    for p in range(P):
                        z_copy(k, p, d).wait_send()

        for swap in swaps:
            swap.wait_send()

    return finish


def feed_phase(
    n, x_ref, gain_ref, gate_ref, up_ref, down_ref, out_ref,
    w_in, sums_in, w_down, act, part,
    xs, cbuf, ysend, yrecv, zsend, zland,
    local, zs, zr, ys, yr, cs, cr, gs, gr, hs, hr, ts, tr,
):
    A = n // 4
    me, a, b, c = place(n)
    across, pair = index_of(a, 1 - b, c), index_of(a, b, 1 - c)
    has, toward = neighbours(n)
    P, W = xs.shape[0], xs.shape[-1]
    rows = x_ref.shape[0]
    units = gate_ref.shape[1]
    split = [(w_in[0], slice(0, units)), (w_in[-1], slice(units, 2 * units) if len(w_in) == 1 else slice(0, units))]
    loads = [
        pltpu.make_async_copy(gate_ref, split[0][0].at[:, split[0][1]], local.at[0]),
        pltpu.make_async_copy(up_ref, split[1][0].at[:, split[1][1]], local.at[1]),
        pltpu.make_async_copy(down_ref, w_down, local.at[2]),
    ]
    for load in loads:
        load.start()
    values = x_ref[...].astype(jnp.float32)
    scale = lax.rsqrt(jnp.mean(values * values, axis=-1, keepdims=True) + epsilon)
    for p in range(P):
        at = slice(p * W, (p + 1) * W)
        xs[p, a, b, c] = (values[:, at] * scale * gain_ref[:, at]).astype(jnp.bfloat16)

    def z_copy(k, p, s, d):
        block = xs.at[p, k, b, c]
        return remote(block, block, zs.at[(0 if d == 1 else A) + s, p], zr.at[k, p], toward[d])

    def y_copy(k, p, bb):
        block = xs.at[p, k, bb, c]
        return remote(block, block, ys.at[k, p], yr.at[k, p], across)

    def c_copy(k, p, bb, cc):
        block = xs.at[p, k, bb, cc]
        return remote(block, block, cs.at[bb * A + k, p], cr.at[bb * A + k, p], pair)

    for p in range(P):
        for d in (1, -1):

            @pl.when(has[d])
            def _():
                z_copy(a, p, 0, d).start()

        y_copy(a, p, b).start()
    for p in range(P):
        c_copy(a, p, b, c).start()

    def pass_on(s, p):
        for d in (1, -1) if s else (1,):
            k = a - s * d

            @pl.when((k >= 0) & (k < A))
            def _():
                y_copy(k, p, 1 - b).wait_recv()
                c_copy(k, p, 1 - b, c).start()

    for sums in sums_in:
        sums[...] = jnp.zeros_like(sums)
    tall = 4 * rows

    def hop(s, p):
        for d in (1, -1):
            k = a - s * d

            @pl.when((k >= 0) & (k < A))
            def _():
                block = xs.at[p, k, b, c]
                remote(block, block, zs.at[0, p], zr.at[k, p], toward[-d]).wait_recv()

                @pl.when(has[d])
                def _():
                    z_copy(k, p, s, d).start()

                y_copy(k, p, b).start()
                c_copy(k, p, b, c).start()

    def contract(s, p):
        for d in (1, -1) if s else (1,):
            k = a - s * d

            @pl.when((k >= 0) & (k < A))
            def _():
                for bb in range(2):
                    c_copy(k, p, bb, 1 - c).wait_recv()
                left = xs[p, k].reshape(tall, W)
                at = pl.ds(pl.multiple_of(k * tall, tall), tall)
                taken = pl.ds(pl.multiple_of(p * W, W), W)
                for w, sums in zip(w_in, sums_in):
                    sums[at, :] += jnp.dot(left, w[taken, :], preferred_element_type=jnp.float32)

    def each(visit):
        def one(p, carry):
            visit(p)
            return carry

        lax.fori_loop(0, P, one, 0)

    each(lambda p: hop(1, p))
    for s in range(2, A + 1):
        if s == 3 or A < 3:
            for load in loads:
                load.wait()

        def stage(p, s=s):
            if s < A:
                hop(s, p)
            pass_on(s - 2, p)
            if s > 2:
                contract(s - 3, p)

        each(stage)

    def last(p):
        pass_on(A - 1, p)
        contract(A - 2, p)

        @pl.when(p > 0)
        def _():
            contract(A - 1, p - 1)

    each(last)
    contract(A - 1, P - 1)

    def activate(bb, cc):
        found = []
        for k in range(A):
            at = pl.ds(pl.multiple_of((4 * k + 2 * bb + cc) * rows, rows), rows)
            gate, up = sums_in[0][at, split[0][1]], sums_in[-1][at, split[1][1]]
            found.append(jax.nn.gelu(gate, approximate=True) * up)
        act[2 * bb + cc] = jnp.concatenate(found, axis=0).astype(jnp.bfloat16)

    activate(1 - b, 1 - c)

    def finish_gather():
        for p in range(P):
            gathered_sends(p)

    def gathered_sends(p):
        for s in range(A):
            for d in (1, -1):
                k = a - s * d

                @pl.when((k >= 0) & (k < A) & has[d])
                def _():
                    z_copy(k, p, s, d).wait_send()

        for k in range(A):
            y_copy(k, p, b).wait_send()
            for bb in range(2):
                c_copy(k, p, bb, c).wait_send()

    def multiply(i, p, bb, cc):
        found = jnp.dot(act[2 * bb + cc], w_down[:, p * W : (p + 1) * W], preferred_element_type=jnp.float32)
        part[i, p] = found.reshape(A, rows, W)

    def g_copy(side, p):
        return remote(part.at[2 * side, p], cbuf.at[side, p], gs.at[side, p], gr.at[side, p], pair)

    def h_copy(k, p):
        return remote(ysend.at[p, k], yrecv.at[p, k], hs.at[k, p], hr.at[k, p], across)

    def t_copy(k, p, right):
        return remote(
            zsend.at[p, k], zland.at[right, p, k], ts.at[k, p], tr.at[right, k, p], me + 8 * right - 4
        )

    def t_arrival(k, p, right):
        return remote(
            zsend.at[p, k], zland.at[right, p, k], ts.at[k, p], tr.at[right, k, p], me - 8 * right + 4
        )

    order = far_first(A, a)
    for t, k in enumerate(order):
        for p in range(P):
            if t == 0:
                if p == 0:
                    multiply(0, p, 1 - b, 1 - c)
                    g_copy(0, p).start()
                    activate(1 - b, c)
                    multiply(1, p, 1 - b, c)
                if p + 1 < P:
                    multiply(0, p + 1, 1 - b, 1 - c)
                    g_copy(0, p + 1).start()
                g_copy(0, p).wait_recv()
            ysend[p, k] = (part[1, p, k] + cbuf[0, p, k]).astype(jnp.bfloat16)
            h_copy(k, p).start()
            if t == 0 and p + 1 < P:
                multiply(1, p + 1, 1 - b, c)
    activate(b, 1 - c)
    activate(b, c)
    for p in range(P):
        multiply(2, p, b, 1 - c)
        g_copy(1, p).start()
    for p in range(P):
        multiply(3, p, b, c)
    for t, k in enumerate(order):
        right = (k > a).astype(jnp.int32)
        for p in range(P):
            if t == 0:
                g_copy(1, p).wait_recv()
            h_copy(k, p).wait_recv()
            part[3, p, k] = part[3, p, k] + cbuf[1, p, k] + yrecv[p, k].astype(jnp.float32)
            if t < A - 1:
                comes = ((right == 1) & (a > 0)) | ((right == 0) & (a < A - 1))

                @pl.when(comes)
                def _():
                    t_arrival(k, p, right).wait_recv()
                    part[3, p, k] = part[3, p, k] + zland[right, p, k].astype(jnp.float32)

                zsend[p, k] = part[3, p, k].astype(jnp.bfloat16)
                t_copy(k, p, right).start()
            else:
                for came in (1, -1):

                    @pl.when(has[-came])
                    def _():
                        side = (came + 1) // 2
                        t_arrival(k, p, side).wait_recv()
                        part[3, p, k] = part[3, p, k] + zland[side, p, k].astype(jnp.float32)

                at = slice(p * W, (p + 1) * W)
                out_ref[:, at] = (x_ref[:, at].astype(jnp.float32) + part[3, p, k]).astype(jnp.bfloat16)

    finish_gather()
    for t, k in enumerate(order):
        right = (k > a).astype(jnp.int32)
        for p in range(P):
            h_copy(k, p).wait_send()
            if t < A - 1:
                t_copy(k, p, right).wait_send()
    for p in range(P):
        g_copy(0, p).wait_send()
        g_copy(1, p).wait_send()


def layer_kernel(n, groups, counts, *refs):
    ends = [sum(counts[: i + 1]) for i in range(len(counts))]
    inputs, (out_ref,), shared, ask, look, out, give = (
        refs[end - count : end] for end, count in zip(ends, counts)
    )
    hidden_ref, gain_ref, wq_ref, kv_ref, cached_ref, lengths_ref, wo_ref, ffn_gain, gate_ref, up_ref, down_ref = inputs
    q_ref, w8, context_ref, residual = shared
    half, full = jnp.bfloat16, jnp.float32
    rows, width = hidden_ref.shape
    requests, positions, across = kv_ref.shape
    heads, units = across // PAD, gate_ref.shape[1]
    P = pieces_of(n, width)
    A, W = n // 4, width // P
    shares, arrived, end_query = query_phase(
        n, groups, hidden_ref, gain_ref, wq_ref, wo_ref, q_ref, w8, *ask
    )

    def attending(*own):
        attend_phase(n, shares, lengths_ref, q_ref, kv_ref, cached_ref, context_ref, *own, *look)()

    pl.run_scoped(
        attending,
        VM(kv_ref.shape, half),
        VM(cached_ref.shape, half),
        VM((2, heads // 2, 2 * QLEN, positions), full),
        VM((2, heads // 2, 2 * QLEN, positions), half),
        VM((n, QLEN, PAD), full),
    )

    def projecting(part):
        project_phase(n, shares[4], arrived, context_ref, hidden_ref, residual, w8, part, *out)()

    pl.run_scoped(projecting, VM((P, A // 2, rows, W), full))
    joined = 1 if units % PAD == 0 else 2
    wide = 2 * units // joined

    def feeding(*own):
        feed_phase(
            n, residual, ffn_gain, gate_ref, up_ref, down_ref, out_ref,
            own[:joined], own[joined : 2 * joined], *own[2 * joined :], *give,
        )

    pl.run_scoped(
        feeding,
        *[VM((width, wide), half)] * joined,
        *[VM((n * rows, wide), full)] * joined,
        VM(down_ref.shape, half),
        VM((4, A * rows, units), half),
        VM((4, P, A, rows, W), full),
    )
    end_query()


def layer(n, groups, hidden, gain, w_query, entering_kv, cached_kv, lengths, w_out, ffn_gain, w_gate, w_up, w_down):
    A = n // 4
    rows, width = hidden.shape
    requests, positions, across = entering_kv.shape
    pairs, heads = requests // 2, across // PAD
    assert A > 2 and A % 2 == 0 and DH % groups == 0 and pairs % 2 == 0
    assert heads == n and QLEN % rows == 0 and 8 * requests <= PAD
    P = pieces_of(n, width)
    W = width // P
    half, full = jnp.bfloat16, jnp.float32
    piece = (P, A, rows, W)
    inputs = (
        hidden, gain[None, :], w_query.T, entering_kv, cached_kv, lengths, w_out, ffn_gain[None, :],
        w_gate, w_up, w_down,
    )
    spaces = (VM, VM, pl.ANY, pl.ANY, pl.ANY, pltpu.SMEM, pl.ANY, VM, pl.ANY, pl.ANY, pl.ANY)
    shared = [
        VM((2 * A, rows, PAD), half), VM((8,) + w_out.shape, half), VM((n, rows, PAD), half), VM((rows, width), half),
    ]
    ask = [
        VM((P, A, 2, rows, W), half), VM((2, DH, width), half),
        DMA((2,)), DMA((2 * A, P)), DMA((A, P)), DMA((A, P)), DMA((A, P)),
        DMA((2,)), DMA((2,)), DMA((4, groups)), DMA((4, groups)), DMA((2,)), DMA((2,)), DMA((4,)), DMA((4,)),
    ]
    look = [
        VM((A, 2, 2, A, rows, PAD), half), VM((2, A, rows, PAD), half),
        VM((n, pairs * QLEN, PAD), half), VM((n, pairs * QLEN, PAD), half),
        VM((n, 8, PAD), full), VM((n, 8, PAD), full),
        DMA((2,)), DMA((A,)), DMA((A,)), DMA((A + 1,)), DMA((A + 1,)), DMA((2 * A,)), DMA((2 * A,)),
        DMA((pairs, n)), DMA((pairs, n)), DMA((n,)), DMA((n,)),
    ]
    M = A // 2
    half_piece = (P, M, rows, W)
    out = [VM((7, M, rows, PAD), half), VM((8, M, rows, PAD), half)] + [VM(half_piece, half)] * 3
    out += [DMA((7,)), DMA((7,)), DMA((M, P)), DMA((2 * M, P))]
    give = [
        VM((P, A, 2, 2, rows, W), half), VM((2,) + piece, full),
        VM(piece, half), VM(piece, half), VM(piece, half), VM((2,) + piece, half),
        DMA((3,)), DMA((2 * A, P)), DMA((A, P)), DMA((A, P)), DMA((A, P)), DMA((2 * A, P)), DMA((2 * A, P)),
        DMA((2, P)), DMA((2, P)), DMA((A, P)), DMA((A, P)), DMA((A, P)), DMA((2, A, P)),
    ]
    parts = (inputs, (None,), shared, ask, look, out, give)
    return pl.pallas_call(
        functools.partial(layer_kernel, n, groups, tuple(len(part) for part in parts)),
        out_shape=jax.ShapeDtypeStruct((rows, width), half),
        in_specs=[pl.BlockSpec(memory_space=m) for m in spaces],
        out_specs=pl.BlockSpec(memory_space=VM),
        scratch_shapes=shared + ask + look + out + give,
        compiler_params=pltpu.CompilerParams(
            collective_id=0, has_side_effects=True, vmem_limit_bytes=60 * 2**20
        ),
        name="layer",
    )(*inputs)


def solution(mesh):
    placed = (
        P(("groups", "mp"), None),
        P(),
        P(None, "mp"),
        P("groups", "mp", None),
        P("groups", None, "mp"),
        P(None, "groups"),
        P("mp", None),
        P(),
        P(None, "mp"),
        P(None, "mp"),
        P("mp", None),
    )
    return jax.shard_map(
        functools.partial(layer, mesh.shape["mp"], mesh.shape["groups"]),
        mesh=mesh,
        in_specs=placed,
        out_specs=P(("groups", "mp"), None),
        check_vma=False,
    )
```

```python
import functools

import jax
import jax.numpy as jnp
from jax import lax
from jax.experimental import pallas as pl
from jax.experimental.pallas import tpu as pltpu
from jax.sharding import PartitionSpec as P

DH = 64
QLEN = 32
PAD = 2 * DH
MESH = pl.DeviceIdType.MESH
VM = pltpu.VMEM
DMA = pltpu.SemaphoreType.DMA

epsilon = 0.1


def place(n):
    me = lax.axis_index("mp")
    return me, me // 4, (me // 2) % 2, me % 2


def index_of(a, b, c):
    return (a * 2 + b) * 2 + c


def remote(src, dst, send, recv, to):
    return pltpu.make_async_remote_copy(
        src_ref=src, dst_ref=dst, send_sem=send, recv_sem=recv, device_id={"mp": to}, device_id_type=MESH
    )


def greet(to):
    pl.semaphore_signal(pltpu.get_barrier_semaphore(), inc=1, device_id={"mp": to}, device_id_type=MESH)


def pieces_of(n, width):
    return max(1, min(4, 16 // (n // 4), width // 128))


def neighbours(n):
    A = n // 4
    me, a, b, c = place(n)
    has = {1: a < A - 1, -1: a > 0}
    toward = {1: me + 4, -1: me - 4}
    return has, toward


def far_first(A, a):
    low, high = 0, A - 1
    found = []
    for _ in range(A):
        left = (a - low > high - a).astype(jnp.int32)
        found.append(high + left * (low - high))
        low, high = low + left, high - 1 + left
    return found


def query_phase(
    n, groups, x_ref, gain_ref, wq_ref, wo_ref, q_ref, w8, xs, w2, local, zs, zr, cs, cr, ys, yr, gs, gr, ps, pr, es, er
):
    A = n // 4
    me, a, b, c = place(n)
    mine = lax.axis_index("groups")
    across, pair = index_of(a, 1 - b, c), index_of(a, b, 1 - c)
    has, toward = neighbours(n)
    P, W = xs.shape[0], xs.shape[-1]
    rows = x_ref.shape[0]
    share = DH // groups
    twins = [lax.rem(mine + i, groups) for i in range(1, groups)]
    for other in range(1, n):
        greet(lax.rem(me + other, n))
    for twin in twins:
        pl.semaphore_signal(
            pltpu.get_barrier_semaphore(), inc=1, device_id={"groups": twin, "mp": me}, device_id_type=MESH
        )
    load_w = pltpu.make_async_copy(wq_ref, w2.at[b], local.at[0])
    load_w.start()
    load_own = pltpu.make_async_copy(wo_ref, w8.at[0], local.at[1])
    load_own.start()
    values = x_ref[...].astype(jnp.float32)
    scale = lax.rsqrt(jnp.mean(values * values, axis=-1, keepdims=True) + epsilon)
    for p in range(P):
        part = slice(p * W, (p + 1) * W)
        xs[p, a, c] = (values[:, part] * scale * gain_ref[:, part]).astype(jnp.bfloat16)
    pl.semaphore_wait(pltpu.get_barrier_semaphore(), n + groups - 2)

    def z_copy(k, p, s, d):
        row = 0 if d == 1 else A
        return remote(xs.at[p, k, c], xs.at[p, k, c], zs.at[row + s, p], zr.at[k, p], toward[d])

    def c_copy(k, p, cc):
        return remote(xs.at[p, k, cc], xs.at[p, k, cc], cs.at[k, p], cr.at[k, p], pair)

    def strip(part):
        return pl.ds(pl.multiple_of(part * share, share), share)

    def landing(which, bb, part):
        return w2.at[bb, strip(part)] if which == 0 else w8.at[2, strip(part)]

    def y_copy(which):
        source = (wq_ref, wo_ref)[which].at[strip(mine)]
        return remote(source, landing(which, b, mine), ys.at[which], yr.at[which], across)

    def y_arrival(which):
        spot = landing(which, 1 - b, mine)
        return remote(spot, spot, ys.at[which], yr.at[which], across)

    def g_copy(which, part, to):
        spot = landing(which, 1 - b, part)
        return pltpu.make_async_remote_copy(
            src_ref=spot, dst_ref=spot, send_sem=gs.at[which, to], recv_sem=gr.at[which, part],
            device_id={"groups": to, "mp": me}, device_id_type=MESH,
        )

    plane_pair = remote(wo_ref, w8.at[1], ps.at[0], pr.at[0], pair)
    plane_diagonal = remote(w8.at[2], w8.at[3], ps.at[1], pr.at[1], pair)
    for p in range(P):
        for d in (1, -1):

            @pl.when(has[d])
            def _():
                z_copy(a, p, 0, d).start()

    for which in range(2):
        y_copy(which).start()
    for p in range(P):
        c_copy(a, p, c).start()
    plane_pair.start()
    for s in range(1, A):
        for p in range(P):
            for d in (1, -1):
                k = a - s * d

                @pl.when((k >= 0) & (k < A))
                def _():
                    remote(xs.at[p, k, c], xs.at[p, k, c], zs.at[0, p], zr.at[k, p], toward[-d]).wait_recv()

                    @pl.when(has[d])
                    def _():
                        z_copy(k, p, s, d).start()

                    c_copy(k, p, c).start()

        if s < 3:
            y_arrival(s - 1).wait_recv()
            for twin in twins:
                g_copy(s - 1, mine, twin).start()
    for twin in twins:
        g_copy(0, twin, mine).wait_recv()
    load_w.wait()
    total = jnp.zeros((2 * A * rows, PAD), jnp.float32)
    for p in range(P):
        for k in range(A):
            c_copy(k, p, 1 - c).wait_recv()
        total = total + lax.dot_general(
            xs[p].reshape(2 * A * rows, W), w2[:, :, p * W : (p + 1) * W].reshape(PAD, W),
            (((1,), (1,)), ((), ())), preferred_element_type=jnp.float32,
        )
    q_ref[...] = total.astype(jnp.bfloat16).reshape(2 * A, rows, PAD)

    def own_strip(slot):
        return w8.at[slot, strip(mine)]

    beyond = remote(wo_ref.at[strip(mine)], own_strip(4), es.at[0], er.at[0], index_of(a + 1 - 2 * (a % 2), b, c))
    beyond_across = remote(own_strip(4), own_strip(6), es.at[1], er.at[1], across)
    beyond_pair = remote(w8.at[4], w8.at[5], es.at[2], er.at[2], pair)
    beyond_diagonal = remote(w8.at[6], w8.at[7], es.at[3], er.at[3], pair)

    def t_copy(i, part, to):
        spot = w8.at[4 + 2 * i, strip(part)]
        return pltpu.make_async_remote_copy(
            src_ref=spot, dst_ref=spot, send_sem=gs.at[2 + i, to], recv_sem=gr.at[2 + i, part],
            device_id={"groups": to, "mp": me}, device_id_type=MESH,
        )

    def share_first():
        beyond.start()

    def share_second():
        for twin in twins:
            g_copy(1, twin, mine).wait_recv()
        plane_diagonal.start()

    def share_third():
        beyond.wait_recv()
        beyond_across.start()
        for twin in twins:
            t_copy(0, mine, twin).start()

    def share_fourth():
        beyond_across.wait_recv()
        for twin in twins:
            t_copy(1, mine, twin).start()
        for twin in twins:
            t_copy(0, twin, mine).wait_recv()
        beyond_pair.start()

    def share_fifth():
        for twin in twins:
            t_copy(1, twin, mine).wait_recv()
        beyond_diagonal.start()

    def share_arrived():
        load_own.wait()
        plane_pair.wait_recv()
        plane_diagonal.wait_recv()
        beyond_pair.wait_recv()
        beyond_diagonal.wait_recv()

    def finish():
        for s in range(A):
            for d in (1, -1):
                k = a - s * d

                @pl.when((k >= 0) & (k < A) & has[d])
                def _():
                    for p in range(P):
                        z_copy(k, p, s, d).wait_send()

        for k in range(A):
            for p in range(P):
                c_copy(k, p, c).wait_send()
        for which in range(2):
            y_copy(which).wait_send()
            for twin in twins:
                g_copy(which, mine, twin).wait_send()
        plane_pair.wait_send()
        plane_diagonal.wait_send()
        for copy in (beyond, beyond_across, beyond_pair, beyond_diagonal):
            copy.wait_send()
        for i in range(2):
            for twin in twins:
                t_copy(i, mine, twin).wait_send()

    return (share_first, share_second, share_third, share_fourth, share_fifth), share_arrived, finish


def attend_phase(
    n, between, lengths_ref, q_ref, kv_ref, cached_ref, context_ref,
    kv, cached, scores, chances, stats,
    q_all, q_cached, o_send, o_recv, st_send, st_recv,
    local, qzs, qzr, qys, qyr, qcs, qcr, os, orr, ss, sr,
):
    A = n // 4
    me, a, b, c = place(n)
    across, pair = index_of(a, 1 - b, c), index_of(a, b, 1 - c)
    requests, positions, width = kv.shape
    pairs, heads = requests // 2, width // PAD
    rows = q_ref.shape[1]
    length = cached.shape[1]
    load_cached = pltpu.make_async_copy(cached_ref, cached, local.at[0])
    load_kv = pltpu.make_async_copy(kv_ref, kv, local.at[1])
    load_cached.start()
    load_kv.start()
    *far, _ = far_first(A, a)
    others = [index_of(k, bb, cc) for k in far for bb in (b, 1 - b) for cc in (c, 1 - c)]
    others += [index_of(a, 1 - b, 1 - c), across, pair]
    columns = far
    entering, flying = pl.ds(0, A), pl.ds(A, A)
    q_all[a, c, b] = q_ref[:A]
    q_cached[b] = q_ref[A:]
    stats[...] = jnp.zeros_like(stats)

    def qz_copy(to, k):
        return remote(q_ref.at[entering], q_all.at[k, c, b], qzs.at[to], qzr.at[k], index_of(to, b, c))

    def qy_copy(k, bb, src=None):
        spot = q_all.at[k, c, bb]
        return remote(spot if src is None else src, spot, qys.at[k], qyr.at[k], across)

    def qc_copy(k, bb, cc, src=None):
        spot = q_all.at[k, cc, bb]
        return remote(spot if src is None else src, spot, qcs.at[bb * A + k], qcr.at[bb * A + k], pair)

    def cached_copy(bb):
        return remote(q_ref.at[flying], q_cached.at[bb], qys.at[A], qyr.at[A], across)

    def o_copy(other, spot, column):
        tall = pairs // 2 * QLEN
        at = pl.ds(pl.multiple_of(column * tall, tall), tall)
        return remote(
            o_send.at[other, at], o_recv.at[spot, at], os.at[column, other], orr.at[column, spot], other
        )

    def st_copy(other, spot):
        return remote(st_send.at[other], st_recv.at[spot], ss.at[other], sr.at[spot], other)

    for k in columns:
        qz_copy(k, a).start()
    qy_copy(a, b, q_ref.at[entering]).start()
    cached_copy(b).start()
    qc_copy(a, b, c, q_ref.at[entering]).start()
    between[0]()
    lane = lax.broadcasted_iota(jnp.int32, (QLEN, PAD), 1)
    low = lane < DH

    def request_of(r, block):
        per = QLEN // rows
        parts = []
        for i in range(per):
            spot = r * per + i
            parts.append(block((spot // 2) % 2, (spot // 4) * 2 + spot % 2))
        return parts[0] if per == 1 else jnp.concatenate(parts, axis=0)

    def put(r, value):
        per = QLEN // rows
        for i in range(per):
            context_ref[r * per + i] = value[i * rows : (i + 1) * rows].astype(jnp.bfloat16)

    def cached_request(r):
        block = cached[r]
        query = request_of(r, lambda bb, spot: q_cached[bb, spot]).astype(jnp.float32)
        query = jnp.where(b == 0, query, pltpu.roll(query, DH, 1))
        found = lax.dot_general(
            jnp.where(low, query, 0.0).astype(jnp.bfloat16), block, (((1,), (1,)), ((), ())),
            preferred_element_type=jnp.float32,
        )
        usable = lax.broadcasted_iota(jnp.int32, (1, length), 1) < lengths_ref[1, r]
        masked = jnp.where(usable, found, -1e30)
        exponent = jnp.exp(masked - jnp.max(masked, axis=-1, keepdims=True))
        inverse = 1.0 / jnp.sum(exponent, axis=-1, keepdims=True)
        weights = (exponent * inverse).astype(jnp.bfloat16)
        put(requests + r, jnp.dot(weights, block, preferred_element_type=jnp.float32))

    def cached_requests(start, stop):
        def two(i, carry):
            cached_request(start + 2 * i)
            cached_request(start + 2 * i + 1)
            return carry

        lax.fori_loop(0, (stop - start) // 2, two, 0)
        if (stop - start) % 2:
            cached_request(stop - 1)

    at_position = me * positions + lax.broadcasted_iota(jnp.int32, (1, positions), 1)

    def pair_step(step, spot):
        at = pl.ds(pl.multiple_of(spot * QLEN, QLEN), QLEN)
        nothing = jnp.zeros((QLEN, PAD), jnp.bfloat16)
        for i in range(2):
            for g in range(heads // 2):
                two = []
                for cc in range(2):
                    packed = request_of(
                        step * 2 + i, lambda bb, spot: q_all[g // 2, cc, bb, spot]
                    ).astype(jnp.float32)
                    packed = packed if g % 2 == 0 else pltpu.roll(packed, DH, 1)
                    two.append(jnp.where(low, packed, 0.0).astype(jnp.bfloat16))
                spread = jnp.concatenate(
                    [
                        jnp.concatenate([two[0], nothing], axis=1),
                        jnp.concatenate([nothing, two[1]], axis=1),
                    ],
                    axis=0,
                )
                scores[i, g] = lax.dot_general(
                    spread, kv[step * 2 + i, :, g * 2 * PAD : (g + 1) * 2 * PAD], (((1,), (1,)), ((), ())),
                    preferred_element_type=jnp.float32,
                )
        for i in range(2):
            r = step * 2 + i
            masked = jnp.where(at_position < lengths_ref[0, r], scores[i], -1e30)
            largest = jnp.max(masked, axis=-1, keepdims=True)
            exponent = jnp.exp(masked - largest)
            total = jnp.sum(exponent, axis=-1, keepdims=True)
            chances[i] = exponent.astype(jnp.bfloat16)
            stats[...] = jnp.where(
                lane == r,
                largest.reshape(heads, QLEN, 1),
                jnp.where(lane == r + requests, total.reshape(heads, QLEN, 1), stats[...]),
            )
        for g in range(heads // 2):
            found = [
                jnp.dot(
                    chances[i, g], kv[step * 2 + i, :, g * 2 * PAD : (g + 1) * 2 * PAD],
                    preferred_element_type=jnp.float32,
                )
                for i in range(2)
            ]
            for e in range(2):
                even, odd = (f[e * QLEN : (e + 1) * QLEN, e * PAD : (e + 1) * PAD] for f in found)
                o_send[2 * g + e, at, :] = jnp.where(low, pltpu.roll(odd, DH, 1), even).astype(jnp.bfloat16)

    def steps(column):
        def one(i, carry):
            pair_step(2 * i + column, column * (pairs // 2) + i)
            return carry

        lax.fori_loop(0, pairs // 2, one, 0)
        for other in others:
            o_copy(other, me, column).start()

    def second_column():
        qy_copy(a, 1 - b).wait_recv()
        qc_copy(a, 1 - b, c).start()
        for k in columns:
            qy_copy(k, 1 - b).wait_recv()
            qc_copy(k, 1 - b, c).start()

    def arrived(bb):
        for k in range(A):
            qc_copy(k, bb, 1 - c).wait_recv()

    for k in columns:
        qz_copy(k, k).wait_recv()
        qy_copy(k, b).start()
        qc_copy(k, b, c).start()
    between[1]()
    cached_copy(1 - b).wait_recv()
    load_cached.wait()
    second = requests // 4
    load_kv.wait()
    if rows == QLEN:
        arrived(b)
        steps(b)
        second_column()
    else:
        second_column()
        arrived(b)
        arrived(1 - b)
        steps(b)
    between[2]()
    cached_requests(0, second)
    if rows == QLEN:
        arrived(1 - b)
    steps(1 - b)
    parts = QLEN // 8
    gap = PAD // parts
    folded = stats[:, :8, :].reshape(heads * 8, PAD)
    for g in range(1, parts):
        folded = folded + pltpu.roll(stats[:, 8 * g : 8 * g + 8, :].reshape(heads * 8, PAD), g * gap, 1)
    st_send[...] = folded.reshape(heads, 8, PAD)
    for other in others:
        st_copy(other, me).start()
    o_recv[me] = o_send[me]
    st_recv[me] = st_send[me]
    cached_requests(second, requests)
    between[3]()
    for other in others:
        st_copy(other, other).wait_recv()
    largest = st_recv[...]
    scale = jnp.exp(largest - jnp.max(largest, axis=0, keepdims=True))
    total = jnp.sum(
        scale * pltpu.roll(largest.reshape(n * 8, PAD), PAD - requests, 1).reshape(n, 8, PAD), axis=0, keepdims=True
    )
    st_recv[...] = scale / jnp.where(total > 0.0, total, 1.0)
    short = low[:8]
    for column in range(2):
        for other in others:
            o_copy(other, other, column).wait_recv()
    for step in range(pairs):
        spot = step % 2 * (pairs // 2) + step // 2
        mixed = jnp.zeros((QLEN, PAD), jnp.float32)
        for d in range(n):
            known = st_recv[d]
            share = []
            for g in range(parts):
                lone = g * gap + 2 * step
                share.append(jnp.where(short, known[:, lone + 1 : lone + 2], known[:, lone : lone + 1]))
            share = jnp.concatenate(share, axis=0)
            mixed = mixed + share * o_recv[d, spot * QLEN : (spot + 1) * QLEN, :].astype(jnp.float32)
        put(2 * step, mixed)
        put(2 * step + 1, pltpu.roll(mixed, DH, 1))

    def finish():
        for k in columns:
            qz_copy(k, a).wait_send()
        cached_copy(b).wait_send()
        for k in range(A):
            qy_copy(k, b).wait_send()
            for bb in range(2):
                qc_copy(k, bb, c).wait_send()
        for other in others:
            st_copy(other, me).wait_send()
            for column in range(2):
                o_copy(other, me, column).wait_send()

    return finish


def project_phase(
    n, start, arrived, context_ref, hidden_ref, out_ref, w8, part, c_send, c_recv, zsend, zright, zleft, cs, cr, zs, zr
):
    M = n // 8
    me, a, b, c = place(n)
    m, e = a // 2, a % 2
    has = {1: m < M - 1, -1: m > 0}
    toward = {1: me + 8, -1: me - 8}
    landing = {1: zright, -1: zleft}
    P, _, rows, W = part.shape
    depth = w8.shape[1]

    def peer(j):
        return e + (j // 4) * (1 - 2 * e), b + (j // 2 % 2) * (1 - 2 * b), c + (j % 2) * (1 - 2 * c)

    swaps = []
    for j in range(7, -1, -1):
        ee, bb, cc = peer(j)
        for k in range(M):
            block = context_ref[index_of(2 * k + ee, bb, cc)]
            if j:
                c_send[j - 1, k] = block
            else:
                c_recv[0, k] = block
        if j:
            swap = remote(c_send.at[j - 1], c_recv.at[j], cs.at[j - 1], cr.at[j - 1], index_of(2 * m + ee, bb, cc))
            swap.start()
            swaps.append(swap)
    start()
    for swap in swaps:
        swap.wait_recv()
    low = lax.broadcasted_iota(jnp.int32, (M * rows, PAD), 1) < DH

    def beside(i):
        first = c_recv[i].reshape(M * rows, PAD).astype(jnp.float32)
        second = c_recv[i + 1].reshape(M * rows, PAD).astype(jnp.float32)
        return jnp.where(low, pltpu.roll(first, DH, 1), second).astype(jnp.bfloat16)

    left = jnp.concatenate([beside(i) for i in range(0, 8, 2)], axis=1)
    arrived()

    def z_copy(k, p, d):
        return remote(zsend.at[p, k], landing[d].at[p, k], zs.at[k, p], zr.at[(0 if d == 1 else M) + k, p], toward[d])

    def z_arrival(k, p, d):
        return remote(zsend.at[p, k], landing[d].at[p, k], zs.at[k, p], zr.at[(0 if d == 1 else M) + k, p], toward[-d])

    for s in range(M - 1, -1, -1):
        for p in range(P):
            if s == M - 1:
                w = w8[:, :, p * W : (p + 1) * W].reshape(8 * depth, W)
                found = jnp.dot(left, w, preferred_element_type=jnp.float32)
                part[p] = found.reshape(M, rows, W)
            for d in (1, -1) if s else (1,):
                k = m + s * d

                @pl.when((k >= 0) & (k < M))
                def _():
                    for came in (d,) if s else (1, -1):

                        @pl.when(has[-came])
                        def _():
                            z_arrival(k, p, came).wait_recv()
                            part[p, k] = part[p, k] + landing[came][p, k].astype(jnp.float32)

                    if s:
                        zsend[p, k] = part[p, k].astype(jnp.bfloat16)
                        z_copy(k, p, d).start()
                    else:
                        at = slice(p * W, (p + 1) * W)
                        out_ref[:, at] = (hidden_ref[:, at].astype(jnp.float32) + part[p, k]).astype(jnp.bfloat16)

    def finish():
        for s in range(M - 1, 0, -1):
            for d in (1, -1):
                k = m + s * d

                @pl.when((k >= 0) & (k < M))
                def _():
                    for p in range(P):
                        z_copy(k, p, d).wait_send()

        for swap in swaps:
            swap.wait_send()

    return finish


def feed_phase(
    n, x_ref, gain_ref, gate_ref, up_ref, down_ref, out_ref,
    w_in, sums_in, w_down, act, part,
    xs, cbuf, ysend, yrecv, zsend, zland,
    local, zs, zr, ys, yr, cs, cr, gs, gr, hs, hr, ts, tr,
):
    A = n // 4
    me, a, b, c = place(n)
    across, pair = index_of(a, 1 - b, c), index_of(a, b, 1 - c)
    has, toward = neighbours(n)
    P, W = xs.shape[0], xs.shape[-1]
    rows = x_ref.shape[0]
    units = gate_ref.shape[1]
    split = [(w_in[0], slice(0, units)), (w_in[-1], slice(units, 2 * units) if len(w_in) == 1 else slice(0, units))]
    loads = [
        pltpu.make_async_copy(gate_ref, split[0][0].at[:, split[0][1]], local.at[0]),
        pltpu.make_async_copy(up_ref, split[1][0].at[:, split[1][1]], local.at[1]),
        pltpu.make_async_copy(down_ref, w_down, local.at[2]),
    ]
    for load in loads:
        load.start()
    values = x_ref[...].astype(jnp.float32)
    scale = lax.rsqrt(jnp.mean(values * values, axis=-1, keepdims=True) + epsilon)
    for p in range(P):
        at = slice(p * W, (p + 1) * W)
        xs[p, a, b, c] = (values[:, at] * scale * gain_ref[:, at]).astype(jnp.bfloat16)

    def z_copy(k, p, s, d):
        block = xs.at[p, k, b, c]
        return remote(block, block, zs.at[(0 if d == 1 else A) + s, p], zr.at[k, p], toward[d])

    def y_copy(k, p, bb):
        block = xs.at[p, k, bb, c]
        return remote(block, block, ys.at[k, p], yr.at[k, p], across)

    def c_copy(k, p, bb, cc):
        block = xs.at[p, k, bb, cc]
        return remote(block, block, cs.at[bb * A + k, p], cr.at[bb * A + k, p], pair)

    for p in range(P):
        for d in (1, -1):

            @pl.when(has[d])
            def _():
                z_copy(a, p, 0, d).start()

        y_copy(a, p, b).start()
    for p in range(P):
        c_copy(a, p, b, c).start()

    def pass_on(s, p):
        for d in (1, -1) if s else (1,):
            k = a - s * d

            @pl.when((k >= 0) & (k < A))
            def _():
                y_copy(k, p, 1 - b).wait_recv()
                c_copy(k, p, 1 - b, c).start()

    for sums in sums_in:
        sums[...] = jnp.zeros_like(sums)
    tall = 4 * rows

    def hop(s, p):
        for d in (1, -1):
            k = a - s * d

            @pl.when((k >= 0) & (k < A))
            def _():
                block = xs.at[p, k, b, c]
                remote(block, block, zs.at[0, p], zr.at[k, p], toward[-d]).wait_recv()

                @pl.when(has[d])
                def _():
                    z_copy(k, p, s, d).start()

                y_copy(k, p, b).start()
                c_copy(k, p, b, c).start()

    def contract(s, p):
        for d in (1, -1) if s else (1,):
            k = a - s * d

            @pl.when((k >= 0) & (k < A))
            def _():
                for bb in range(2):
                    c_copy(k, p, bb, 1 - c).wait_recv()
                left = xs[p, k].reshape(tall, W)
                at = pl.ds(pl.multiple_of(k * tall, tall), tall)
                taken = pl.ds(pl.multiple_of(p * W, W), W)
                for w, sums in zip(w_in, sums_in):
                    sums[at, :] += jnp.dot(left, w[taken, :], preferred_element_type=jnp.float32)

    def each(visit):
        def one(p, carry):
            visit(p)
            return carry

        lax.fori_loop(0, P, one, 0)

    each(lambda p: hop(1, p))
    for s in range(2, A + 1):
        if s == 3 or A < 3:
            for load in loads:
                load.wait()

        def stage(p, s=s):
            if s < A:
                hop(s, p)
            pass_on(s - 2, p)
            if s > 2:
                contract(s - 3, p)

        each(stage)

    def last(p):
        pass_on(A - 1, p)
        contract(A - 2, p)

        @pl.when(p > 0)
        def _():
            contract(A - 1, p - 1)

    each(last)
    contract(A - 1, P - 1)

    def activate(bb, cc):
        found = []
        for k in range(A):
            at = pl.ds(pl.multiple_of((4 * k + 2 * bb + cc) * rows, rows), rows)
            gate, up = sums_in[0][at, split[0][1]], sums_in[-1][at, split[1][1]]
            found.append(jax.nn.gelu(gate, approximate=True) * up)
        act[2 * bb + cc] = jnp.concatenate(found, axis=0).astype(jnp.bfloat16)

    activate(1 - b, 1 - c)

    def finish_gather():
        for p in range(P):
            gathered_sends(p)

    def gathered_sends(p):
        for s in range(A):
            for d in (1, -1):
                k = a - s * d

                @pl.when((k >= 0) & (k < A) & has[d])
                def _():
                    z_copy(k, p, s, d).wait_send()

        for k in range(A):
            y_copy(k, p, b).wait_send()
            for bb in range(2):
                c_copy(k, p, bb, c).wait_send()

    def multiply(i, p, bb, cc):
        found = jnp.dot(act[2 * bb + cc], w_down[:, p * W : (p + 1) * W], preferred_element_type=jnp.float32)
        part[i, p] = found.reshape(A, rows, W)

    def g_copy(side, p):
        return remote(part.at[2 * side, p], cbuf.at[side, p], gs.at[side, p], gr.at[side, p], pair)

    def h_copy(k, p):
        return remote(ysend.at[p, k], yrecv.at[p, k], hs.at[k, p], hr.at[k, p], across)

    def t_copy(k, p, right):
        return remote(
            zsend.at[p, k], zland.at[right, p, k], ts.at[k, p], tr.at[right, k, p], me + 8 * right - 4
        )

    def t_arrival(k, p, right):
        return remote(
            zsend.at[p, k], zland.at[right, p, k], ts.at[k, p], tr.at[right, k, p], me - 8 * right + 4
        )

    order = far_first(A, a)
    for t, k in enumerate(order):
        for p in range(P):
            if t == 0:
                if p == 0:
                    multiply(0, p, 1 - b, 1 - c)
                    g_copy(0, p).start()
                    activate(1 - b, c)
                    multiply(1, p, 1 - b, c)
                if p + 1 < P:
                    multiply(0, p + 1, 1 - b, 1 - c)
                    g_copy(0, p + 1).start()
                g_copy(0, p).wait_recv()
            ysend[p, k] = (part[1, p, k] + cbuf[0, p, k]).astype(jnp.bfloat16)
            h_copy(k, p).start()
            if t == 0 and p + 1 < P:
                multiply(1, p + 1, 1 - b, c)
    activate(b, 1 - c)
    activate(b, c)
    for p in range(P):
        multiply(2, p, b, 1 - c)
        g_copy(1, p).start()
    for p in range(P):
        multiply(3, p, b, c)
    for t, k in enumerate(order):
        right = (k > a).astype(jnp.int32)
        for p in range(P):
            if t == 0:
                g_copy(1, p).wait_recv()
            h_copy(k, p).wait_recv()
            part[3, p, k] = part[3, p, k] + cbuf[1, p, k] + yrecv[p, k].astype(jnp.float32)
            if t < A - 1:
                comes = ((right == 1) & (a > 0)) | ((right == 0) & (a < A - 1))

                @pl.when(comes)
                def _():
                    t_arrival(k, p, right).wait_recv()
                    part[3, p, k] = part[3, p, k] + zland[right, p, k].astype(jnp.float32)

                zsend[p, k] = part[3, p, k].astype(jnp.bfloat16)
                t_copy(k, p, right).start()
            else:
                for came in (1, -1):

                    @pl.when(has[-came])
                    def _():
                        side = (came + 1) // 2
                        t_arrival(k, p, side).wait_recv()
                        part[3, p, k] = part[3, p, k] + zland[side, p, k].astype(jnp.float32)

                at = slice(p * W, (p + 1) * W)
                out_ref[:, at] = (x_ref[:, at].astype(jnp.float32) + part[3, p, k]).astype(jnp.bfloat16)

    finish_gather()
    for t, k in enumerate(order):
        right = (k > a).astype(jnp.int32)
        for p in range(P):
            h_copy(k, p).wait_send()
            if t < A - 1:
                t_copy(k, p, right).wait_send()
    for p in range(P):
        g_copy(0, p).wait_send()
        g_copy(1, p).wait_send()


def layer_kernel(n, groups, counts, *refs):
    ends = [sum(counts[: i + 1]) for i in range(len(counts))]
    inputs, (out_ref,), shared, ask, look, out, give = (
        refs[end - count : end] for end, count in zip(ends, counts)
    )
    hidden_ref, gain_ref, wq_ref, kv_ref, cached_ref, lengths_ref, wo_ref, ffn_gain, gate_ref, up_ref, down_ref = inputs
    q_ref, w8, context_ref, residual = shared
    half, full = jnp.bfloat16, jnp.float32
    rows, width = hidden_ref.shape
    requests, positions, across = kv_ref.shape
    heads, units = across // PAD, gate_ref.shape[1]
    P = pieces_of(n, width)
    A, W = n // 4, width // P
    shares, arrived, end_query = query_phase(
        n, groups, hidden_ref, gain_ref, wq_ref, wo_ref, q_ref, w8, *ask
    )

    def attending(*own):
        attend_phase(n, shares, lengths_ref, q_ref, kv_ref, cached_ref, context_ref, *own, *look)()

    pl.run_scoped(
        attending,
        VM(kv_ref.shape, half),
        VM(cached_ref.shape, half),
        VM((2, heads // 2, 2 * QLEN, positions), full),
        VM((2, heads // 2, 2 * QLEN, positions), half),
        VM((n, QLEN, PAD), full),
    )

    def projecting(part):
        project_phase(n, shares[4], arrived, context_ref, hidden_ref, residual, w8, part, *out)()

    pl.run_scoped(projecting, VM((P, A // 2, rows, W), full))
    joined = 1 if units % PAD == 0 else 2
    wide = 2 * units // joined

    def feeding(*own):
        feed_phase(
            n, residual, ffn_gain, gate_ref, up_ref, down_ref, out_ref,
            own[:joined], own[joined : 2 * joined], *own[2 * joined :], *give,
        )

    pl.run_scoped(
        feeding,
        *[VM((width, wide), half)] * joined,
        *[VM((n * rows, wide), full)] * joined,
        VM(down_ref.shape, half),
        VM((4, A * rows, units), half),
        VM((4, P, A, rows, W), full),
    )
    end_query()


def layer(n, groups, hidden, gain, w_query, entering_kv, cached_kv, lengths, w_out, ffn_gain, w_gate, w_up, w_down):
    A = n // 4
    rows, width = hidden.shape
    requests, positions, across = entering_kv.shape
    pairs, heads = requests // 2, across // PAD
    assert A > 2 and A % 2 == 0 and DH % groups == 0 and pairs % 2 == 0
    assert heads == n and QLEN % rows == 0 and 8 * requests <= PAD
    P = pieces_of(n, width)
    W = width // P
    half, full = jnp.bfloat16, jnp.float32
    piece = (P, A, rows, W)
    inputs = (
        hidden, gain[None, :], w_query.T, entering_kv, cached_kv, lengths, w_out, ffn_gain[None, :],
        w_gate, w_up, w_down,
    )
    spaces = (VM, VM, pl.ANY, pl.ANY, pl.ANY, pltpu.SMEM, pl.ANY, VM, pl.ANY, pl.ANY, pl.ANY)
    shared = [
        VM((2 * A, rows, PAD), half), VM((8,) + w_out.shape, half), VM((n, rows, PAD), half), VM((rows, width), half),
    ]
    ask = [
        VM((P, A, 2, rows, W), half), VM((2, DH, width), half),
        DMA((2,)), DMA((2 * A, P)), DMA((A, P)), DMA((A, P)), DMA((A, P)),
        DMA((2,)), DMA((2,)), DMA((4, groups)), DMA((4, groups)), DMA((2,)), DMA((2,)), DMA((4,)), DMA((4,)),
    ]
    look = [
        VM((A, 2, 2, A, rows, PAD), half), VM((2, A, rows, PAD), half),
        VM((n, pairs * QLEN, PAD), half), VM((n, pairs * QLEN, PAD), half),
        VM((n, 8, PAD), full), VM((n, 8, PAD), full),
        DMA((2,)), DMA((A,)), DMA((A,)), DMA((A + 1,)), DMA((A + 1,)), DMA((2 * A,)), DMA((2 * A,)),
        DMA((2, n)), DMA((2, n)), DMA((n,)), DMA((n,)),
    ]
    M = A // 2
    half_piece = (P, M, rows, W)
    out = [VM((7, M, rows, PAD), half), VM((8, M, rows, PAD), half)] + [VM(half_piece, half)] * 3
    out += [DMA((7,)), DMA((7,)), DMA((M, P)), DMA((2 * M, P))]
    give = [
        VM((P, A, 2, 2, rows, W), half), VM((2,) + piece, full),
        VM(piece, half), VM(piece, half), VM(piece, half), VM((2,) + piece, half),
        DMA((3,)), DMA((2 * A, P)), DMA((A, P)), DMA((A, P)), DMA((A, P)), DMA((2 * A, P)), DMA((2 * A, P)),
        DMA((2, P)), DMA((2, P)), DMA((A, P)), DMA((A, P)), DMA((A, P)), DMA((2, A, P)),
    ]
    parts = (inputs, (None,), shared, ask, look, out, give)
    return pl.pallas_call(
        functools.partial(layer_kernel, n, groups, tuple(len(part) for part in parts)),
        out_shape=jax.ShapeDtypeStruct((rows, width), half),
        in_specs=[pl.BlockSpec(memory_space=m) for m in spaces],
        out_specs=pl.BlockSpec(memory_space=VM),
        scratch_shapes=shared + ask + look + out + give,
        compiler_params=pltpu.CompilerParams(
            collective_id=0, has_side_effects=True, vmem_limit_bytes=60 * 2**20
        ),
        name="layer",
    )(*inputs)


def solution(mesh):
    placed = (
        P(("groups", "mp"), None),
        P(),
        P(None, "mp"),
        P("groups", "mp", None),
        P("groups", None, "mp"),
        P(None, "groups"),
        P("mp", None),
        P(),
        P(None, "mp"),
        P(None, "mp"),
        P("mp", None),
    )
    return jax.shard_map(
        functools.partial(layer, mesh.shape["mp"], mesh.shape["groups"]),
        mesh=mesh,
        in_specs=placed,
        out_specs=P(("groups", "mp"), None),
        check_vma=False,
    )
```

```python
import functools

import jax
import jax.numpy as jnp
from jax import lax
from jax.experimental import pallas as pl
from jax.experimental.pallas import tpu as pltpu
from jax.sharding import PartitionSpec as P

DH = 64
QLEN = 32
PAD = 2 * DH
MESH = pl.DeviceIdType.MESH
VM = pltpu.VMEM
DMA = pltpu.SemaphoreType.DMA

epsilon = 0.1


def place(n):
    me = lax.axis_index("mp")
    return me, me // 4, (me // 2) % 2, me % 2


def index_of(a, b, c):
    return (a * 2 + b) * 2 + c


def remote(src, dst, send, recv, to):
    return pltpu.make_async_remote_copy(
        src_ref=src, dst_ref=dst, send_sem=send, recv_sem=recv, device_id={"mp": to}, device_id_type=MESH
    )


def greet(to):
    pl.semaphore_signal(pltpu.get_barrier_semaphore(), inc=1, device_id={"mp": to}, device_id_type=MESH)


def pieces_of(n, width):
    return max(1, min(4, 16 // (n // 4), width // 128))


def neighbours(n):
    A = n // 4
    me, a, b, c = place(n)
    has = {1: a < A - 1, -1: a > 0}
    toward = {1: me + 4, -1: me - 4}
    return has, toward


def far_first(A, a):
    low, high = 0, A - 1
    found = []
    for _ in range(A):
        left = (a - low > high - a).astype(jnp.int32)
        found.append(high + left * (low - high))
        low, high = low + left, high - 1 + left
    return found


def query_phase(
    n, groups, x_ref, gain_ref, wq_ref, wo_ref, q_ref, w8, xs, w2, local, zs, zr, cs, cr, ys, yr, gs, gr, ps, pr, es, er
):
    A = n // 4
    me, a, b, c = place(n)
    mine = lax.axis_index("groups")
    across, pair = index_of(a, 1 - b, c), index_of(a, b, 1 - c)
    has, toward = neighbours(n)
    P, W = xs.shape[0], xs.shape[-1]
    rows = x_ref.shape[0]
    share = DH // groups
    twins = [lax.rem(mine + i, groups) for i in range(1, groups)]
    for other in range(1, n):
        greet(lax.rem(me + other, n))
    for twin in twins:
        pl.semaphore_signal(
            pltpu.get_barrier_semaphore(), inc=1, device_id={"groups": twin, "mp": me}, device_id_type=MESH
        )
    load_w = pltpu.make_async_copy(wq_ref, w2.at[b], local.at[0])
    load_w.start()
    load_own = pltpu.make_async_copy(wo_ref, w8.at[0], local.at[1])
    load_own.start()
    values = x_ref[...].astype(jnp.float32)
    scale = lax.rsqrt(jnp.mean(values * values, axis=-1, keepdims=True) + epsilon)
    for p in range(P):
        part = slice(p * W, (p + 1) * W)
        xs[p, a, c] = (values[:, part] * scale * gain_ref[:, part]).astype(jnp.bfloat16)
    pl.semaphore_wait(pltpu.get_barrier_semaphore(), n + groups - 2)

    def z_copy(k, p, s, d):
        row = 0 if d == 1 else A
        return remote(xs.at[p, k, c], xs.at[p, k, c], zs.at[row + s, p], zr.at[k, p], toward[d])

    def c_copy(k, p, cc):
        return remote(xs.at[p, k, cc], xs.at[p, k, cc], cs.at[k, p], cr.at[k, p], pair)

    def strip(part):
        return pl.ds(pl.multiple_of(part * share, share), share)

    def landing(which, bb, part):
        return w2.at[bb, strip(part)] if which == 0 else w8.at[2, strip(part)]

    def y_copy(which):
        source = (wq_ref, wo_ref)[which].at[strip(mine)]
        return remote(source, landing(which, b, mine), ys.at[which], yr.at[which], across)

    def y_arrival(which):
        spot = landing(which, 1 - b, mine)
        return remote(spot, spot, ys.at[which], yr.at[which], across)

    def g_copy(which, part, to):
        spot = landing(which, 1 - b, part)
        return pltpu.make_async_remote_copy(
            src_ref=spot, dst_ref=spot, send_sem=gs.at[which, to], recv_sem=gr.at[which, part],
            device_id={"groups": to, "mp": me}, device_id_type=MESH,
        )

    plane_pair = remote(wo_ref, w8.at[1], ps.at[0], pr.at[0], pair)
    plane_diagonal = remote(w8.at[2], w8.at[3], ps.at[1], pr.at[1], pair)
    for p in range(P):
        for d in (1, -1):

            @pl.when(has[d])
            def _():
                z_copy(a, p, 0, d).start()

    for which in range(2):
        y_copy(which).start()
    for p in range(P):
        c_copy(a, p, c).start()
    plane_pair.start()
    for s in range(1, A):
        for p in range(P):
            for d in (1, -1):
                k = a - s * d

                @pl.when((k >= 0) & (k < A))
                def _():
                    remote(xs.at[p, k, c], xs.at[p, k, c], zs.at[0, p], zr.at[k, p], toward[-d]).wait_recv()

                    @pl.when(has[d])
                    def _():
                        z_copy(k, p, s, d).start()

                    c_copy(k, p, c).start()

            if s in (2, 3) and p == min(1, P - 1):
                y_arrival(s - 2).wait_recv()
                for twin in twins:
                    g_copy(s - 2, mine, twin).start()

    for twin in twins:
        g_copy(0, twin, mine).wait_recv()
    load_w.wait()
    total = jnp.zeros((2 * A * rows, PAD), jnp.float32)
    for p in range(P):
        for k in range(A):
            c_copy(k, p, 1 - c).wait_recv()
        total = total + lax.dot_general(
            xs[p].reshape(2 * A * rows, W), w2[:, :, p * W : (p + 1) * W].reshape(PAD, W),
            (((1,), (1,)), ((), ())), preferred_element_type=jnp.float32,
        )
    q_ref[...] = total.astype(jnp.bfloat16).reshape(2 * A, rows, PAD)

    def own_strip(slot):
        return w8.at[slot, strip(mine)]

    beyond = remote(wo_ref.at[strip(mine)], own_strip(4), es.at[0], er.at[0], index_of(a + 1 - 2 * (a % 2), b, c))
    beyond_across = remote(own_strip(4), own_strip(6), es.at[1], er.at[1], across)
    beyond_pair = remote(w8.at[4], w8.at[5], es.at[2], er.at[2], pair)
    beyond_diagonal = remote(w8.at[6], w8.at[7], es.at[3], er.at[3], pair)

    def t_copy(i, part, to):
        spot = w8.at[4 + 2 * i, strip(part)]
        return pltpu.make_async_remote_copy(
            src_ref=spot, dst_ref=spot, send_sem=gs.at[2 + i, to], recv_sem=gr.at[2 + i, part],
            device_id={"groups": to, "mp": me}, device_id_type=MESH,
        )

    def share_first():
        beyond.start()

    def share_second():
        for twin in twins:
            g_copy(1, twin, mine).wait_recv()
        plane_diagonal.start()

    def share_third():
        beyond.wait_recv()
        beyond_across.start()
        for twin in twins:
            t_copy(0, mine, twin).start()

    def share_fourth():
        beyond_across.wait_recv()
        for twin in twins:
            t_copy(1, mine, twin).start()
        for twin in twins:
            t_copy(0, twin, mine).wait_recv()
        beyond_pair.start()

    def share_fifth():
        for twin in twins:
            t_copy(1, twin, mine).wait_recv()
        beyond_diagonal.start()

    def share_arrived():
        load_own.wait()
        plane_pair.wait_recv()
        plane_diagonal.wait_recv()
        beyond_pair.wait_recv()
        beyond_diagonal.wait_recv()

    def finish():
        for s in range(A):
            for d in (1, -1):
                k = a - s * d

                @pl.when((k >= 0) & (k < A) & has[d])
                def _():
                    for p in range(P):
                        z_copy(k, p, s, d).wait_send()

        for k in range(A):
            for p in range(P):
                c_copy(k, p, c).wait_send()
        for which in range(2):
            y_copy(which).wait_send()
            for twin in twins:
                g_copy(which, mine, twin).wait_send()
        plane_pair.wait_send()
        plane_diagonal.wait_send()
        for copy in (beyond, beyond_across, beyond_pair, beyond_diagonal):
            copy.wait_send()
        for i in range(2):
            for twin in twins:
                t_copy(i, mine, twin).wait_send()

    return (share_first, share_second, share_third, share_fourth, share_fifth), share_arrived, finish


def attend_phase(
    n, between, lengths_ref, q_ref, kv_ref, cached_ref, context_ref,
    kv, cached, scores, chances, stats,
    q_all, q_cached, o_send, o_recv, st_send, st_recv,
    local, qzs, qzr, qys, qyr, qcs, qcr, os, orr, ss, sr,
):
    A = n // 4
    me, a, b, c = place(n)
    across, pair = index_of(a, 1 - b, c), index_of(a, b, 1 - c)
    requests, positions, width = kv.shape
    pairs, heads = requests // 2, width // PAD
    rows = q_ref.shape[1]
    length = cached.shape[1]
    load_cached = pltpu.make_async_copy(cached_ref, cached, local.at[0])
    load_kv = pltpu.make_async_copy(kv_ref, kv, local.at[1])
    load_cached.start()
    load_kv.start()
    *far, _ = far_first(A, a)
    others = [index_of(k, bb, cc) for k in far for bb in (b, 1 - b) for cc in (c, 1 - c)]
    others += [index_of(a, 1 - b, 1 - c), across, pair]
    columns = far
    entering, flying = pl.ds(0, A), pl.ds(A, A)
    q_all[a, c, b] = q_ref[:A]
    q_cached[b] = q_ref[A:]
    stats[...] = jnp.zeros_like(stats)

    def qz_copy(to, k):
        return remote(q_ref.at[entering], q_all.at[k, c, b], qzs.at[to], qzr.at[k], index_of(to, b, c))

    def qy_copy(k, bb, src=None):
        spot = q_all.at[k, c, bb]
        return remote(spot if src is None else src, spot, qys.at[k], qyr.at[k], across)

    def qc_copy(k, bb, cc, src=None):
        spot = q_all.at[k, cc, bb]
        return remote(spot if src is None else src, spot, qcs.at[bb * A + k], qcr.at[bb * A + k], pair)

    def cached_copy(bb):
        return remote(q_ref.at[flying], q_cached.at[bb], qys.at[A], qyr.at[A], across)

    def o_copy(other, spot, column):
        tall = pairs // 2 * QLEN
        at = pl.ds(pl.multiple_of(column * tall, tall), tall)
        return remote(
            o_send.at[other, at], o_recv.at[spot, at], os.at[column, other], orr.at[column, spot], other
        )

    def st_copy(other, spot):
        return remote(st_send.at[other], st_recv.at[spot], ss.at[other], sr.at[spot], other)

    for k in columns:
        qz_copy(k, a).start()
    qy_copy(a, b, q_ref.at[entering]).start()
    cached_copy(b).start()
    qc_copy(a, b, c, q_ref.at[entering]).start()
    between[0]()
    lane = lax.broadcasted_iota(jnp.int32, (QLEN, PAD), 1)
    low = lane < DH

    def request_of(r, block):
        per = QLEN // rows
        parts = []
        for i in range(per):
            spot = r * per + i
            parts.append(block((spot // 2) % 2, (spot // 4) * 2 + spot % 2))
        return parts[0] if per == 1 else jnp.concatenate(parts, axis=0)

    def put(r, value):
        per = QLEN // rows
        for i in range(per):
            context_ref[r * per + i] = value[i * rows : (i + 1) * rows].astype(jnp.bfloat16)

    def cached_request(r):
        block = cached[r]
        query = request_of(r, lambda bb, spot: q_cached[bb, spot]).astype(jnp.float32)
        query = jnp.where(b == 0, query, pltpu.roll(query, DH, 1))
        found = lax.dot_general(
            jnp.where(low, query, 0.0).astype(jnp.bfloat16), block, (((1,), (1,)), ((), ())),
            preferred_element_type=jnp.float32,
        )
        usable = lax.broadcasted_iota(jnp.int32, (1, length), 1) < lengths_ref[1, r]
        masked = jnp.where(usable, found, -1e30)
        exponent = jnp.exp(masked - jnp.max(masked, axis=-1, keepdims=True))
        inverse = 1.0 / jnp.sum(exponent, axis=-1, keepdims=True)
        weights = (exponent * inverse).astype(jnp.bfloat16)
        put(requests + r, jnp.dot(weights, block, preferred_element_type=jnp.float32))

    def cached_requests(start, stop):
        def two(i, carry):
            cached_request(start + 2 * i)
            cached_request(start + 2 * i + 1)
            return carry

        lax.fori_loop(0, (stop - start) // 2, two, 0)
        if (stop - start) % 2:
            cached_request(stop - 1)

    at_position = me * positions + lax.broadcasted_iota(jnp.int32, (1, positions), 1)

    def pair_step(step, spot):
        at = pl.ds(pl.multiple_of(spot * QLEN, QLEN), QLEN)
        nothing = jnp.zeros((QLEN, PAD), jnp.bfloat16)
        for i in range(2):
            for g in range(heads // 2):
                two = []
                for cc in range(2):
                    packed = request_of(
                        step * 2 + i, lambda bb, spot: q_all[g // 2, cc, bb, spot]
                    ).astype(jnp.float32)
                    packed = packed if g % 2 == 0 else pltpu.roll(packed, DH, 1)
                    two.append(jnp.where(low, packed, 0.0).astype(jnp.bfloat16))
                spread = jnp.concatenate(
                    [
                        jnp.concatenate([two[0], nothing], axis=1),
                        jnp.concatenate([nothing, two[1]], axis=1),
                    ],
                    axis=0,
                )
                scores[i, g] = lax.dot_general(
                    spread, kv[step * 2 + i, :, g * 2 * PAD : (g + 1) * 2 * PAD], (((1,), (1,)), ((), ())),
                    preferred_element_type=jnp.float32,
                )
        for i in range(2):
            r = step * 2 + i
            masked = jnp.where(at_position < lengths_ref[0, r], scores[i], -1e30)
            largest = jnp.max(masked, axis=-1, keepdims=True)
            exponent = jnp.exp(masked - largest)
            total = jnp.sum(exponent, axis=-1, keepdims=True)
            chances[i] = exponent.astype(jnp.bfloat16)
            stats[...] = jnp.where(
                lane == r,
                largest.reshape(heads, QLEN, 1),
                jnp.where(lane == r + requests, total.reshape(heads, QLEN, 1), stats[...]),
            )
        for g in range(heads // 2):
            found = [
                jnp.dot(
                    chances[i, g], kv[step * 2 + i, :, g * 2 * PAD : (g + 1) * 2 * PAD],
                    preferred_element_type=jnp.float32,
                )
                for i in range(2)
            ]
            for e in range(2):
                even, odd = (f[e * QLEN : (e + 1) * QLEN, e * PAD : (e + 1) * PAD] for f in found)
                o_send[2 * g + e, at, :] = jnp.where(low, pltpu.roll(odd, DH, 1), even).astype(jnp.bfloat16)

    def steps(column):
        def one(i, carry):
            pair_step(2 * i + column, column * (pairs // 2) + i)
            return carry

        lax.fori_loop(0, pairs // 2, one, 0)
        for other in others:
            o_copy(other, me, column).start()

    def second_column():
        qy_copy(a, 1 - b).wait_recv()
        qc_copy(a, 1 - b, c).start()
        for k in columns:
            qy_copy(k, 1 - b).wait_recv()
            qc_copy(k, 1 - b, c).start()

    def arrived(bb):
        for k in range(A):
            qc_copy(k, bb, 1 - c).wait_recv()

    for k in columns:
        qz_copy(k, k).wait_recv()
        qy_copy(k, b).start()
        qc_copy(k, b, c).start()
    between[1]()
    cached_copy(1 - b).wait_recv()
    load_cached.wait()
    second = requests // 4
    load_kv.wait()
    if rows == QLEN:
        arrived(b)
        steps(b)
        second_column()
    else:
        second_column()
        arrived(b)
        arrived(1 - b)
        steps(b)
    between[2]()
    cached_requests(0, second)
    if rows == QLEN:
        arrived(1 - b)
    steps(1 - b)
    parts = QLEN // 8
    gap = PAD // parts
    folded = stats[:, :8, :].reshape(heads * 8, PAD)
    for g in range(1, parts):
        folded = folded + pltpu.roll(stats[:, 8 * g : 8 * g + 8, :].reshape(heads * 8, PAD), g * gap, 1)
    st_send[...] = folded.reshape(heads, 8, PAD)
    for other in others:
        st_copy(other, me).start()
    o_recv[me] = o_send[me]
    st_recv[me] = st_send[me]
    cached_requests(second, requests)
    between[3]()
    for other in others:
        st_copy(other, other).wait_recv()
    largest = st_recv[...]
    scale = jnp.exp(largest - jnp.max(largest, axis=0, keepdims=True))
    total = jnp.sum(
        scale * pltpu.roll(largest.reshape(n * 8, PAD), PAD - requests, 1).reshape(n, 8, PAD), axis=0, keepdims=True
    )
    st_recv[...] = scale / jnp.where(total > 0.0, total, 1.0)
    short = low[:8]
    for column in range(2):
        for other in others:
            o_copy(other, other, column).wait_recv()
    for step in range(pairs):
        spot = step % 2 * (pairs // 2) + step // 2
        mixed = jnp.zeros((QLEN, PAD), jnp.float32)
        for d in range(n):
            known = st_recv[d]
            share = []
            for g in range(parts):
                lone = g * gap + 2 * step
                share.append(jnp.where(short, known[:, lone + 1 : lone + 2], known[:, lone : lone + 1]))
            share = jnp.concatenate(share, axis=0)
            mixed = mixed + share * o_recv[d, spot * QLEN : (spot + 1) * QLEN, :].astype(jnp.float32)
        put(2 * step, mixed)
        put(2 * step + 1, pltpu.roll(mixed, DH, 1))

    def finish():
        for k in columns:
            qz_copy(k, a).wait_send()
        cached_copy(b).wait_send()
        for k in range(A):
            qy_copy(k, b).wait_send()
            for bb in range(2):
                qc_copy(k, bb, c).wait_send()
        for other in others:
            st_copy(other, me).wait_send()
            for column in range(2):
                o_copy(other, me, column).wait_send()

    return finish


def project_phase(
    n, start, arrived, context_ref, hidden_ref, out_ref, w8, part, c_send, c_recv, zsend, zright, zleft, cs, cr, zs, zr
):
    M = n // 8
    me, a, b, c = place(n)
    m, e = a // 2, a % 2
    has = {1: m < M - 1, -1: m > 0}
    toward = {1: me + 8, -1: me - 8}
    landing = {1: zright, -1: zleft}
    P, _, rows, W = part.shape
    depth = w8.shape[1]

    def peer(j):
        return e + (j // 4) * (1 - 2 * e), b + (j // 2 % 2) * (1 - 2 * b), c + (j % 2) * (1 - 2 * c)

    swaps = []
    for j in range(7, -1, -1):
        ee, bb, cc = peer(j)
        for k in range(M):
            block = context_ref[index_of(2 * k + ee, bb, cc)]
            if j:
                c_send[j - 1, k] = block
            else:
                c_recv[0, k] = block
        if j:
            swap = remote(c_send.at[j - 1], c_recv.at[j], cs.at[j - 1], cr.at[j - 1], index_of(2 * m + ee, bb, cc))
            swap.start()
            swaps.append(swap)
    start()
    for swap in swaps:
        swap.wait_recv()
    low = lax.broadcasted_iota(jnp.int32, (M * rows, PAD), 1) < DH

    def beside(i):
        first = c_recv[i].reshape(M * rows, PAD).astype(jnp.float32)
        second = c_recv[i + 1].reshape(M * rows, PAD).astype(jnp.float32)
        return jnp.where(low, pltpu.roll(first, DH, 1), second).astype(jnp.bfloat16)

    left = jnp.concatenate([beside(i) for i in range(0, 8, 2)], axis=1)
    arrived()

    def z_copy(k, p, d):
        return remote(zsend.at[p, k], landing[d].at[p, k], zs.at[k, p], zr.at[(0 if d == 1 else M) + k, p], toward[d])

    def z_arrival(k, p, d):
        return remote(zsend.at[p, k], landing[d].at[p, k], zs.at[k, p], zr.at[(0 if d == 1 else M) + k, p], toward[-d])

    for s in range(M - 1, -1, -1):
        for p in range(P):
            if s == M - 1:
                w = w8[:, :, p * W : (p + 1) * W].reshape(8 * depth, W)
                found = jnp.dot(left, w, preferred_element_type=jnp.float32)
                part[p] = found.reshape(M, rows, W)
            for d in (1, -1) if s else (1,):
                k = m + s * d

                @pl.when((k >= 0) & (k < M))
                def _():
                    for came in (d,) if s else (1, -1):

                        @pl.when(has[-came])
                        def _():
                            z_arrival(k, p, came).wait_recv()
                            part[p, k] = part[p, k] + landing[came][p, k].astype(jnp.float32)

                    if s:
                        zsend[p, k] = part[p, k].astype(jnp.bfloat16)
                        z_copy(k, p, d).start()
                    else:
                        at = slice(p * W, (p + 1) * W)
                        out_ref[:, at] = (hidden_ref[:, at].astype(jnp.float32) + part[p, k]).astype(jnp.bfloat16)

    def finish():
        for s in range(M - 1, 0, -1):
            for d in (1, -1):
                k = m + s * d

                @pl.when((k >= 0) & (k < M))
                def _():
                    for p in range(P):
                        z_copy(k, p, d).wait_send()

        for swap in swaps:
            swap.wait_send()

    return finish


def feed_phase(
    n, x_ref, gain_ref, gate_ref, up_ref, down_ref, out_ref,
    w_in, sums_in, w_down, act, part,
    xs, cbuf, ysend, yrecv, zsend, zland,
    local, zs, zr, ys, yr, cs, cr, gs, gr, hs, hr, ts, tr,
):
    A = n // 4
    me, a, b, c = place(n)
    across, pair = index_of(a, 1 - b, c), index_of(a, b, 1 - c)
    has, toward = neighbours(n)
    P, W = xs.shape[0], xs.shape[-1]
    rows = x_ref.shape[0]
    units = gate_ref.shape[1]
    split = [(w_in[0], slice(0, units)), (w_in[-1], slice(units, 2 * units) if len(w_in) == 1 else slice(0, units))]
    loads = [
        pltpu.make_async_copy(gate_ref, split[0][0].at[:, split[0][1]], local.at[0]),
        pltpu.make_async_copy(up_ref, split[1][0].at[:, split[1][1]], local.at[1]),
        pltpu.make_async_copy(down_ref, w_down, local.at[2]),
    ]
    for load in loads:
        load.start()
    values = x_ref[...].astype(jnp.float32)
    scale = lax.rsqrt(jnp.mean(values * values, axis=-1, keepdims=True) + epsilon)
    for p in range(P):
        at = slice(p * W, (p + 1) * W)
        xs[p, a, b, c] = (values[:, at] * scale * gain_ref[:, at]).astype(jnp.bfloat16)

    def z_copy(k, p, s, d):
        block = xs.at[p, k, b, c]
        return remote(block, block, zs.at[(0 if d == 1 else A) + s, p], zr.at[k, p], toward[d])

    def y_copy(k, p, bb):
        block = xs.at[p, k, bb, c]
        return remote(block, block, ys.at[k, p], yr.at[k, p], across)

    def c_copy(k, p, bb, cc):
        block = xs.at[p, k, bb, cc]
        return remote(block, block, cs.at[bb * A + k, p], cr.at[bb * A + k, p], pair)

    for p in range(P):
        for d in (1, -1):

            @pl.when(has[d])
            def _():
                z_copy(a, p, 0, d).start()

        y_copy(a, p, b).start()
    for p in range(P):
        c_copy(a, p, b, c).start()

    def pass_on(s, p):
        for d in (1, -1) if s else (1,):
            k = a - s * d

            @pl.when((k >= 0) & (k < A))
            def _():
                y_copy(k, p, 1 - b).wait_recv()
                c_copy(k, p, 1 - b, c).start()

    for sums in sums_in:
        sums[...] = jnp.zeros_like(sums)
    tall = 4 * rows

    def hop(s, p):
        for d in (1, -1):
            k = a - s * d

            @pl.when((k >= 0) & (k < A))
            def _():
                block = xs.at[p, k, b, c]
                remote(block, block, zs.at[0, p], zr.at[k, p], toward[-d]).wait_recv()

                @pl.when(has[d])
                def _():
                    z_copy(k, p, s, d).start()

                y_copy(k, p, b).start()
                c_copy(k, p, b, c).start()

    def contract(s, p):
        for d in (1, -1) if s else (1,):
            k = a - s * d

            @pl.when((k >= 0) & (k < A))
            def _():
                for bb in range(2):
                    c_copy(k, p, bb, 1 - c).wait_recv()
                left = xs[p, k].reshape(tall, W)
                at = pl.ds(pl.multiple_of(k * tall, tall), tall)
                taken = pl.ds(pl.multiple_of(p * W, W), W)
                for w, sums in zip(w_in, sums_in):
                    sums[at, :] += jnp.dot(left, w[taken, :], preferred_element_type=jnp.float32)

    def each(visit):
        def one(p, carry):
            visit(p)
            return carry

        lax.fori_loop(0, P, one, 0)

    each(lambda p: hop(1, p))
    for s in range(2, A + 1):
        if s == 3 or A < 3:
            for load in loads:
                load.wait()

        def stage(p, s=s):
            if s < A:
                hop(s, p)
            pass_on(s - 2, p)
            if s > 2:
                contract(s - 3, p)

        each(stage)

    def last(p):
        pass_on(A - 1, p)
        contract(A - 2, p)

        @pl.when(p > 0)
        def _():
            contract(A - 1, p - 1)

    each(last)
    contract(A - 1, P - 1)

    def activate(bb, cc):
        found = []
        for k in range(A):
            at = pl.ds(pl.multiple_of((4 * k + 2 * bb + cc) * rows, rows), rows)
            gate, up = sums_in[0][at, split[0][1]], sums_in[-1][at, split[1][1]]
            found.append(jax.nn.gelu(gate, approximate=True) * up)
        act[2 * bb + cc] = jnp.concatenate(found, axis=0).astype(jnp.bfloat16)

    activate(1 - b, 1 - c)

    def finish_gather():
        for p in range(P):
            gathered_sends(p)

    def gathered_sends(p):
        for s in range(A):
            for d in (1, -1):
                k = a - s * d

                @pl.when((k >= 0) & (k < A) & has[d])
                def _():
                    z_copy(k, p, s, d).wait_send()

        for k in range(A):
            y_copy(k, p, b).wait_send()
            for bb in range(2):
                c_copy(k, p, bb, c).wait_send()

    def multiply(i, p, bb, cc):
        found = jnp.dot(act[2 * bb + cc], w_down[:, p * W : (p + 1) * W], preferred_element_type=jnp.float32)
        part[i, p] = found.reshape(A, rows, W)

    def g_copy(side, p):
        return remote(part.at[2 * side, p], cbuf.at[side, p], gs.at[side, p], gr.at[side, p], pair)

    def h_copy(k, p):
        return remote(ysend.at[p, k], yrecv.at[p, k], hs.at[k, p], hr.at[k, p], across)

    def t_copy(k, p, right):
        return remote(
            zsend.at[p, k], zland.at[right, p, k], ts.at[k, p], tr.at[right, k, p], me + 8 * right - 4
        )

    def t_arrival(k, p, right):
        return remote(
            zsend.at[p, k], zland.at[right, p, k], ts.at[k, p], tr.at[right, k, p], me - 8 * right + 4
        )

    order = far_first(A, a)
    for t, k in enumerate(order):
        for p in range(P):
            if t == 0:
                if p == 0:
                    multiply(0, p, 1 - b, 1 - c)
                    g_copy(0, p).start()
                    activate(1 - b, c)
                    multiply(1, p, 1 - b, c)
                if p + 1 < P:
                    multiply(0, p + 1, 1 - b, 1 - c)
                    g_copy(0, p + 1).start()
                g_copy(0, p).wait_recv()
            ysend[p, k] = (part[1, p, k] + cbuf[0, p, k]).astype(jnp.bfloat16)
            h_copy(k, p).start()
            if t == 0 and p + 1 < P:
                multiply(1, p + 1, 1 - b, c)
    activate(b, 1 - c)
    activate(b, c)
    for p in range(P):
        multiply(2, p, b, 1 - c)
        g_copy(1, p).start()
    for p in range(P):
        multiply(3, p, b, c)
    for t, k in enumerate(order):
        right = (k > a).astype(jnp.int32)
        for p in range(P):
            if t == 0:
                g_copy(1, p).wait_recv()
            h_copy(k, p).wait_recv()
            part[3, p, k] = part[3, p, k] + cbuf[1, p, k] + yrecv[p, k].astype(jnp.float32)
            if t < A - 1:
                comes = ((right == 1) & (a > 0)) | ((right == 0) & (a < A - 1))

                @pl.when(comes)
                def _():
                    t_arrival(k, p, right).wait_recv()
                    part[3, p, k] = part[3, p, k] + zland[right, p, k].astype(jnp.float32)

                zsend[p, k] = part[3, p, k].astype(jnp.bfloat16)
                t_copy(k, p, right).start()
            else:
                for came in (1, -1):

                    @pl.when(has[-came])
                    def _():
                        side = (came + 1) // 2
                        t_arrival(k, p, side).wait_recv()
                        part[3, p, k] = part[3, p, k] + zland[side, p, k].astype(jnp.float32)

                at = slice(p * W, (p + 1) * W)
                out_ref[:, at] = (x_ref[:, at].astype(jnp.float32) + part[3, p, k]).astype(jnp.bfloat16)

    finish_gather()
    for t, k in enumerate(order):
        right = (k > a).astype(jnp.int32)
        for p in range(P):
            h_copy(k, p).wait_send()
            if t < A - 1:
                t_copy(k, p, right).wait_send()
    for p in range(P):
        g_copy(0, p).wait_send()
        g_copy(1, p).wait_send()


def layer_kernel(n, groups, counts, *refs):
    ends = [sum(counts[: i + 1]) for i in range(len(counts))]
    inputs, (out_ref,), shared, ask, look, out, give = (
        refs[end - count : end] for end, count in zip(ends, counts)
    )
    hidden_ref, gain_ref, wq_ref, kv_ref, cached_ref, lengths_ref, wo_ref, ffn_gain, gate_ref, up_ref, down_ref = inputs
    q_ref, w8, context_ref, residual = shared
    half, full = jnp.bfloat16, jnp.float32
    rows, width = hidden_ref.shape
    requests, positions, across = kv_ref.shape
    heads, units = across // PAD, gate_ref.shape[1]
    P = pieces_of(n, width)
    A, W = n // 4, width // P
    shares, arrived, end_query = query_phase(
        n, groups, hidden_ref, gain_ref, wq_ref, wo_ref, q_ref, w8, *ask
    )

    def attending(*own):
        attend_phase(n, shares, lengths_ref, q_ref, kv_ref, cached_ref, context_ref, *own, *look)()

    pl.run_scoped(
        attending,
        VM(kv_ref.shape, half),
        VM(cached_ref.shape, half),
        VM((2, heads // 2, 2 * QLEN, positions), full),
        VM((2, heads // 2, 2 * QLEN, positions), half),
        VM((n, QLEN, PAD), full),
    )

    def projecting(part):
        project_phase(n, shares[4], arrived, context_ref, hidden_ref, residual, w8, part, *out)()

    pl.run_scoped(projecting, VM((P, A // 2, rows, W), full))
    joined = 1 if units % PAD == 0 else 2
    wide = 2 * units // joined

    def feeding(*own):
        feed_phase(
            n, residual, ffn_gain, gate_ref, up_ref, down_ref, out_ref,
            own[:joined], own[joined : 2 * joined], *own[2 * joined :], *give,
        )

    pl.run_scoped(
        feeding,
        *[VM((width, wide), half)] * joined,
        *[VM((n * rows, wide), full)] * joined,
        VM(down_ref.shape, half),
        VM((4, A * rows, units), half),
        VM((4, P, A, rows, W), full),
    )
    end_query()


def layer(n, groups, hidden, gain, w_query, entering_kv, cached_kv, lengths, w_out, ffn_gain, w_gate, w_up, w_down):
    A = n // 4
    rows, width = hidden.shape
    requests, positions, across = entering_kv.shape
    pairs, heads = requests // 2, across // PAD
    assert A > 3 and A % 2 == 0 and DH % groups == 0 and pairs % 2 == 0
    assert heads == n and QLEN % rows == 0 and 8 * requests <= PAD
    P = pieces_of(n, width)
    W = width // P
    half, full = jnp.bfloat16, jnp.float32
    piece = (P, A, rows, W)
    inputs = (
        hidden, gain[None, :], w_query.T, entering_kv, cached_kv, lengths, w_out, ffn_gain[None, :],
        w_gate, w_up, w_down,
    )
    spaces = (VM, VM, pl.ANY, pl.ANY, pl.ANY, pltpu.SMEM, pl.ANY, VM, pl.ANY, pl.ANY, pl.ANY)
    shared = [
        VM((2 * A, rows, PAD), half), VM((8,) + w_out.shape, half), VM((n, rows, PAD), half), VM((rows, width), half),
    ]
    ask = [
        VM((P, A, 2, rows, W), half), VM((2, DH, width), half),
        DMA((2,)), DMA((2 * A, P)), DMA((A, P)), DMA((A, P)), DMA((A, P)),
        DMA((2,)), DMA((2,)), DMA((4, groups)), DMA((4, groups)), DMA((2,)), DMA((2,)), DMA((4,)), DMA((4,)),
    ]
    look = [
        VM((A, 2, 2, A, rows, PAD), half), VM((2, A, rows, PAD), half),
        VM((n, pairs * QLEN, PAD), half), VM((n, pairs * QLEN, PAD), half),
        VM((n, 8, PAD), full), VM((n, 8, PAD), full),
        DMA((2,)), DMA((A,)), DMA((A,)), DMA((A + 1,)), DMA((A + 1,)), DMA((2 * A,)), DMA((2 * A,)),
        DMA((2, n)), DMA((2, n)), DMA((n,)), DMA((n,)),
    ]
    M = A // 2
    half_piece = (P, M, rows, W)
    out = [VM((7, M, rows, PAD), half), VM((8, M, rows, PAD), half)] + [VM(half_piece, half)] * 3
    out += [DMA((7,)), DMA((7,)), DMA((M, P)), DMA((2 * M, P))]
    give = [
        VM((P, A, 2, 2, rows, W), half), VM((2,) + piece, full),
        VM(piece, half), VM(piece, half), VM(piece, half), VM((2,) + piece, half),
        DMA((3,)), DMA((2 * A, P)), DMA((A, P)), DMA((A, P)), DMA((A, P)), DMA((2 * A, P)), DMA((2 * A, P)),
        DMA((2, P)), DMA((2, P)), DMA((A, P)), DMA((A, P)), DMA((A, P)), DMA((2, A, P)),
    ]
    parts = (inputs, (None,), shared, ask, look, out, give)
    return pl.pallas_call(
        functools.partial(layer_kernel, n, groups, tuple(len(part) for part in parts)),
        out_shape=jax.ShapeDtypeStruct((rows, width), half),
        in_specs=[pl.BlockSpec(memory_space=m) for m in spaces],
        out_specs=pl.BlockSpec(memory_space=VM),
        scratch_shapes=shared + ask + look + out + give,
        compiler_params=pltpu.CompilerParams(
            collective_id=0, has_side_effects=True, vmem_limit_bytes=60 * 2**20
        ),
        name="layer",
    )(*inputs)


def solution(mesh):
    placed = (
        P(("groups", "mp"), None),
        P(),
        P(None, "mp"),
        P("groups", "mp", None),
        P("groups", None, "mp"),
        P(None, "groups"),
        P("mp", None),
        P(),
        P(None, "mp"),
        P(None, "mp"),
        P("mp", None),
    )
    return jax.shard_map(
        functools.partial(layer, mesh.shape["mp"], mesh.shape["groups"]),
        mesh=mesh,
        in_specs=placed,
        out_specs=P(("groups", "mp"), None),
        check_vma=False,
    )
```
